8 devices in a mesh: dp: 1 (over z), tp: 2 (over y), ep: 4 (over x, core).
Axes of the slice: x: 2, y: 2, z: 1, core: 2. Of those that a mesh axis runs over, the one named last changes fastest.
Arguments:
- resid_in: bfloat16 [512, 7168], P(('dp', 'ep'))
- norm_scale: bfloat16 [7168], replicated
- w_router: bfloat16 [7168, 128], replicated
- w_gate: bfloat16 [128, 7168, 256], P('ep', None, 'tp')
- w_up: bfloat16 [128, 7168, 256], P('ep', None, 'tp')
- w_down: bfloat16 [128, 256, 7168], P('ep', 'tp')
- choice: int32 [512, 2], P(('dp', 'ep'))
Outputs:
- output: bfloat16 [512, 7168], P(('dp', 'ep'))
All inputs are finite; a program needn't handle non-finite values.
Results may differ from the reference program's by a relative error of at most 0.00572865.
Values are sent between devices in bfloat16 or wider.
A program may use at most 1 GiB of HBM per device.

```python
import jax
import jax.numpy as jnp
from jax import lax

D_MODEL = 7168
EXPERTS = 128
TOP_K = 2
TOK_DEV = 128
FF_SHARD = 128
EP_GROUPS = 4
TP_SHARDS = 2

TOKENS = EP_GROUPS * TOK_DEV
FF_WIDTH = TP_SHARDS * FF_SHARD
CAPACITY = (2 * TOK_DEV * TOP_K + EXPERTS - 1) // EXPERTS
NUM_SLOTS = EXPERTS * EP_GROUPS * CAPACITY
NORM_EPS = 1e-5


def draw_choice(choice_key):
    base_key, bias_key = jax.random.split(choice_key)
    base_score = jax.random.randint(base_key, (TOKENS, EXPERTS), 0, 65536, dtype=jnp.int32)
    expert_bias = jax.random.randint(bias_key, (EXPERTS,), 0, 16384, dtype=jnp.int32)
    scores = (base_score + expert_bias[None, :]) * EXPERTS + jnp.arange(EXPERTS, dtype=jnp.int32)[None, :]
    return lax.top_k(scores, TOP_K)[1].astype(jnp.int32)


def setup_inputs(seed: int = 0, part: int = 0) -> dict:
    root_key = jax.random.key(seed)
    sub_keys = jax.random.split(root_key, 7)
    resid_in = jax.random.normal(jax.random.fold_in(sub_keys[0], part), (TOKENS, D_MODEL), jnp.float32)
    norm_scale = 1.0 + 0.3 * jax.random.normal(sub_keys[1], (D_MODEL,), jnp.float32)
    w_router = jax.random.normal(sub_keys[2], (D_MODEL, EXPERTS), jnp.float32) * D_MODEL ** -0.5
    w_gate = jax.random.normal(sub_keys[3], (EXPERTS, D_MODEL, FF_WIDTH), jnp.float32) * D_MODEL ** -0.5
    w_up = jax.random.normal(sub_keys[4], (EXPERTS, D_MODEL, FF_WIDTH), jnp.float32) * D_MODEL ** -0.5
    w_down = jax.random.normal(sub_keys[5], (EXPERTS, FF_WIDTH, D_MODEL), jnp.float32) * (2.0 * FF_WIDTH ** -0.5)
    choice = draw_choice(jax.random.fold_in(sub_keys[6], part))
    return {'resid_in': resid_in.astype(jnp.bfloat16), 'norm_scale': norm_scale.astype(jnp.bfloat16), 'w_router': w_router.astype(jnp.bfloat16), 'w_gate': w_gate.astype(jnp.bfloat16), 'w_up': w_up.astype(jnp.bfloat16), 'w_down': w_down.astype(jnp.bfloat16), 'choice': choice}


def norm_route(resid_rows, norm_scale, w_router, choice_rows):
    rows_f32 = resid_rows.astype(jnp.float32)
    centered = rows_f32 - jnp.mean(rows_f32, axis=-1, keepdims=True)
    variance = jnp.mean(centered * centered, axis=-1, keepdims=True)
    normed = (centered * lax.rsqrt(variance + NORM_EPS) * norm_scale.astype(jnp.float32)).astype(jnp.bfloat16)
    logits = jnp.dot(normed, w_router, preferred_element_type=jnp.float32)
    router_probs = jax.nn.softmax(logits, axis=-1)
    expert_ids = jnp.arange(w_router.shape[1], dtype=jnp.int32)
    picked = jnp.sum(jnp.where(choice_rows[:, :, None] == expert_ids[None, None, :], router_probs[:, None, :], 0.0), axis=-1)
    gate_vals = picked / jnp.sum(picked, axis=-1, keepdims=True)
    return normed, gate_vals


def expert_glu(rows_in, w_gate_e, w_up_e, w_down_e):
    gate_act = jnp.dot(rows_in, w_gate_e, preferred_element_type=jnp.float32)
    up_act = jnp.dot(rows_in, w_up_e, preferred_element_type=jnp.float32)
    hidden = (jax.nn.silu(gate_act) * up_act).astype(jnp.bfloat16)
    hidden_split = hidden.reshape(rows_in.shape[0], TP_SHARDS, FF_SHARD).astype(jnp.float32)
    down_split = w_down_e.reshape(TP_SHARDS, FF_SHARD, D_MODEL).astype(jnp.float32)
    partial_out = jnp.einsum('stf,tfd->tsd', hidden_split, down_split).astype(jnp.bfloat16)
    return jnp.sum(partial_out.astype(jnp.float32), axis=0)


def reference(resid_in, norm_scale, w_router, w_gate, w_up, w_down, choice):
    normed, gate_vals = norm_route(resid_in, norm_scale, w_router, choice)
    group_choice = choice.reshape(EP_GROUPS, TOK_DEV * TOP_K)
    onehot = (group_choice[:, :, None] == jnp.arange(EXPERTS, dtype=jnp.int32)[None, None, :]).astype(jnp.int32)
    earlier = jnp.cumsum(onehot, axis=1) - onehot
    position = jnp.sum(earlier * onehot, axis=2)
    is_kept = (position < CAPACITY).reshape(-1)
    group_ids = jnp.arange(EP_GROUPS, dtype=jnp.int32)[:, None]
    slot_ids = (group_choice * (EP_GROUPS * CAPACITY) + group_ids * CAPACITY + position).reshape(-1)
    target = jnp.where(is_kept, slot_ids, NUM_SLOTS)
    token_rows = (group_ids * TOK_DEV + jnp.arange(TOK_DEV * TOP_K, dtype=jnp.int32)[None, :] // TOP_K).reshape(-1)
    source_row = jnp.zeros((NUM_SLOTS + 1,), jnp.int32).at[target].set(token_rows)[:NUM_SLOTS]
    kept_gate = jnp.where(is_kept, gate_vals.reshape(-1), 0.0)
    slot_gate = jnp.zeros((NUM_SLOTS + 1,), jnp.float32).at[target].set(kept_gate)[:NUM_SLOTS]

    def expert_step(mixed_sum, expert_in):
        rows_idx, gate_col, w_gate_e, w_up_e, w_down_e = expert_in
        y_rows = expert_glu(normed[rows_idx], w_gate_e, w_up_e, w_down_e)
        return mixed_sum.at[rows_idx].add(gate_col[:, None] * y_rows), None

    mixed_sum, unused = lax.scan(expert_step, jnp.zeros((TOKENS, D_MODEL), jnp.float32), (source_row.reshape(EXPERTS, EP_GROUPS * CAPACITY), slot_gate.reshape(EXPERTS, EP_GROUPS * CAPACITY), w_gate, w_up, w_down))
    return (resid_in.astype(jnp.float32) + mixed_sum).astype(jnp.bfloat16)
```

```python
import functools

import jax
import jax.numpy as jnp
from jax import lax
from jax.experimental import pallas as pl
from jax.experimental.pallas import tpu as pltpu
from jax.sharding import PartitionSpec as P

NORM_EPS = 1e-5
MESH = pl.DeviceIdType.MESH
F32 = jnp.float32
BF16 = jnp.bfloat16
CAP = 4
GROUPS = 4
UP_STEPS = 14
UP_BUFS = 4
DOWN_STEPS = 7
DOWN_BUFS = 3
VMEM_LIMIT = 62 * 1024 * 1024


def remote(src, dst, send_sem, recv_sem, device):
    return pltpu.make_async_remote_copy(src_ref=src, dst_ref=dst, send_sem=send_sem, recv_sem=recv_sem, device_id=device, device_id_type=MESH)


def place():
    dp, tp, ep = lax.axis_index('dp'), lax.axis_index('tp'), lax.axis_index('ep')
    return dp, tp, ep, ep // 2, ep % 2


def up_kernel(x_ref, g_ref, wr_hbm, wg_hbm, wu_hbm, tok_ref, choice_ref, hid_ref, gate_ref,
              u_ref, xs_ref, pick_ref, acc_ref, wbuf, wr_ref, logit_ref,
              w_sem, wr_sem, own_s, own_r, x_s, x_r, y_s, y_r, dx_s, dx_r, dy_s, dy_r):
    dp, tp, ep, cx, core = place()
    local = wg_hbm.shape[0]
    tok, d_model = x_ref.shape
    half = d_model // 2
    steps = UP_STEPS
    cw = half // steps
    twin = (dp, tp, cx * 2 + (1 - core))
    across = (dp, tp, (1 - cx) * 2 + core)
    other_tp = (dp, 1 - tp, ep)
    far = (1 - cx) * 2 + core

    barrier = pltpu.get_barrier_semaphore()
    for peer in (twin, across, other_tp):
        pl.semaphore_signal(barrier, inc=1, device_id=peer, device_id_type=MESH)

    def weight_copies(step, slot):
        out = []
        for h in range(2):
            rows = pl.ds(pl.multiple_of(h * half + step * cw, cw), cw)
            for m, w in enumerate((wg_hbm, wu_hbm)):
                out.append(pltpu.make_async_copy(w.at[:, rows, :], wbuf.at[slot, :, h * cw:(h + 1) * cw, m * 128:(m + 1) * 128], w_sem.at[slot, h * 2 + m]))
        return out

    wr_copy = pltpu.make_async_copy(wr_hbm, wr_ref, wr_sem)
    for c in weight_copies(0, 0):
        c.start()
    wr_copy.start()
    for b in range(1, UP_BUFS):
        for c in weight_copies(b, b):
            c.start()

    def norm_rows(r, carry):
        rows = pl.ds(pl.multiple_of(r * 16, 16), 16)
        xb = x_ref[rows, :].astype(F32)
        cen = xb - jnp.mean(xb, axis=-1, keepdims=True)
        var = jnp.mean(cen * cen, axis=-1, keepdims=True)
        u = (cen * lax.rsqrt(var + NORM_EPS) * g_ref[...].astype(F32)).astype(BF16)
        for j in range(steps):
            for h in range(2):
                u_ref[j, h, ep, rows, :] = u[:, h * half + j * cw:h * half + (j + 1) * cw]
        return carry

    lax.fori_loop(0, tok // 16, norm_rows, 0)
    slots = tok_ref.shape[0]
    pick_ref[...] = jnp.where(tok_ref[...] == lax.broadcasted_iota(jnp.int32, (slots, GROUPS * tok), 1), 1.0, 0.0).astype(BF16)
    acc_ref[...] = jnp.zeros_like(acc_ref)
    logit_ref[...] = jnp.zeros_like(logit_ref)
    pl.semaphore_wait(barrier, 3)

    def own_copy(j):
        return remote(u_ref.at[j, :, ep], u_ref.at[j, :, ep], own_s.at[j], own_r.at[j], twin)

    def x_copy(j):
        return remote(u_ref.at[j, tp, ep], u_ref.at[j, tp, ep], x_s.at[j], x_r.at[j], across)

    def y_copy(j):
        return remote(u_ref.at[j, tp, far], u_ref.at[j, tp, far], y_s.at[j], y_r.at[j], other_tp)

    def dx_copy(j):
        return remote(u_ref.at[j, tp, far], u_ref.at[j, tp, far], dx_s.at[j], dx_r.at[j], twin)

    def dy_copy(j):
        return remote(u_ref.at[j, 1 - tp, far], u_ref.at[j, 1 - tp, far], dy_s.at[j], dy_r.at[j], twin)

    def first_sends(j, carry):
        x_copy(j).start()
        own_copy(j).start()
        return carry

    lax.fori_loop(0, steps, first_sends, 0)
    wr_copy.wait()

    def main(i, carry):
        @pl.when(i < steps)
        def _():
            x_copy(i).wait_recv()
            y_copy(i).start()
            dx_copy(i).start()

        @pl.when((i >= 1) & (i < steps + 1))
        def _():
            j = i - 1
            y_copy(j).wait_recv()
            dy_copy(j).start()

        @pl.when(i >= 2)
        def _():
            j = i - 2
            slot = lax.rem(j, UP_BUFS)
            for h in range(2):
                kr = pl.ds(pl.multiple_of(h * half + j * cw, cw), cw)
                logit_ref[...] += jnp.dot(u_ref[j, h, ep], wr_ref[kr, :], preferred_element_type=F32)
            own_copy(j).wait_recv()
            dx_copy(j).wait_recv()
            dy_copy(j).wait_recv()
            for h in range(2):
                block = u_ref[j, h].reshape(GROUPS * tok, cw)
                xs_ref[:, h * cw:(h + 1) * cw] = jnp.dot(pick_ref[...], block, preferred_element_type=F32).astype(BF16)
            for c in weight_copies(j, slot):
                c.wait()

            def experts(t, carry2):
                for z in range(4):
                    e = t * 4 + z
                    rows = pl.ds(pl.multiple_of(e * 16, 16), 16)
                    acc_ref[rows, :] += jnp.dot(xs_ref[rows, :], wbuf[slot, e], preferred_element_type=F32)
                return carry2

            lax.fori_loop(0, local // 4, experts, 0)

            @pl.when(j + UP_BUFS < steps)
            def _():
                for c in weight_copies(j + UP_BUFS, slot):
                    c.start()
        return carry

    lax.fori_loop(0, steps + 2, main, 0)

    gate_act = acc_ref[:, :128]
    hid_ref[...] = (gate_act * jax.nn.sigmoid(gate_act) * acc_ref[:, 128:]).astype(BF16)
    logits = logit_ref[...]
    ex = jnp.exp(logits - jnp.max(logits, axis=-1, keepdims=True))
    probs = ex / jnp.sum(ex, axis=-1, keepdims=True)
    ids = lax.broadcasted_iota(jnp.int32, probs.shape, 1)
    p0 = jnp.sum(jnp.where(choice_ref[:, 0:1] == ids, probs, 0.0), axis=-1, keepdims=True)
    p1 = jnp.sum(jnp.where(choice_ref[:, 1:2] == ids, probs, 0.0), axis=-1, keepdims=True)
    gate_ref[:, 0:1] = p0 / (p0 + p1)
    gate_ref[:, 1:2] = p1 / (p0 + p1)

    def last_waits(j, carry):
        x_copy(j).wait_send()
        own_copy(j).wait_send()
        y_copy(j).wait_send()
        dx_copy(j).wait_send()
        dy_copy(j).wait_send()
        return carry

    lax.fori_loop(0, steps, last_waits, 0)


def down_kernel(rows_c, rows_n, hid_ref, x_ref, gate_ref, slotkey_ref, keycol_ref, keyrow_ref, nkey_ref, poskey_ref, npos_ref, wd_hbm, out_ref,
                send_ref, land_ref, fwd_ref, yland_ref, qs_ref, w2buf, p_ref, s_ref, a_ref, b_ref,
                w_sem, q_s, q_r, f_s, f_r, o_s, o_r):
    dp, tp, ep, cx, core = place()
    local = wd_hbm.shape[0]
    tok, d_model = x_ref.shape
    half = d_model // 2
    steps = DOWN_STEPS
    cw = half // steps
    peers = [(1 - cx) * 2 + core, (1 - cx) * 2 + (1 - core), cx * 2 + (1 - core)]
    other_tp = (dp, 1 - tp, ep)

    barrier = pltpu.get_barrier_semaphore()
    for g in peers:
        pl.semaphore_signal(barrier, inc=1, device_id=(dp, tp, g), device_id_type=MESH)
    pl.semaphore_signal(barrier, inc=1, device_id=other_tp, device_id_type=MESH)

    def weight_copies(step, slot):
        out = []
        for h in range(2):
            cols = pl.ds(pl.multiple_of(h * half + step * cw, 128), cw)
            out.append(pltpu.make_async_copy(wd_hbm.at[:, :, cols], w2buf.at[slot, :, :, h * cw:(h + 1) * cw], w_sem.at[slot, h]))
        return out

    for b in range(DOWN_BUFS):
        for c in weight_copies(b, b):
            c.start()

    p_ref[...] = jnp.where(keycol_ref[...] == slotkey_ref[...], 1.0, 0.0).astype(BF16)
    s_ref[...] = jnp.where(lax.broadcasted_iota(jnp.int32, s_ref.shape, 0) == nkey_ref[...], 1.0, 0.0).astype(BF16)

    def split_gates(keys, pos, dst):
        mat = jnp.where(pos[:, 0:1] == keys, gate_ref[:, 0:1], 0.0) + jnp.where(pos[:, 1:2] == keys, gate_ref[:, 1:2], 0.0)
        for z in range(3):
            part = mat.astype(BF16)
            dst[z] = part
            mat = mat - part.astype(F32)

    split_gates(keyrow_ref[...], poskey_ref[...], a_ref)
    split_gates(lax.broadcasted_iota(jnp.int32, (tok, rows_n), 1), npos_ref[...], b_ref)
    pl.semaphore_wait(barrier, 4)

    def q_copy(k, n):
        return remote(send_ref.at[k, :, peers[n]], land_ref.at[k, :, ep], q_s.at[k, n], q_r.at[k, n], (dp, tp, peers[n]))

    def f_copy(k):
        return remote(fwd_ref.at[k], yland_ref.at[k], f_s.at[k], f_r.at[k], other_tp)

    def o_copy(k):
        cols = pl.ds(pl.multiple_of(tp * half + k * cw, 128), cw)
        return remote(out_ref.at[:, cols], out_ref.at[:, cols], o_s.at[k], o_r.at[k], other_tp)

    def main(i, carry):
        @pl.when(i < steps)
        def _():
            slot = lax.rem(i, DOWN_BUFS)
            for c in weight_copies(i, slot):
                c.wait()

            def experts(t, carry2):
                for z in range(4):
                    e = t * 4 + z
                    rows = pl.ds(pl.multiple_of(e * 16, 16), 16)
                    qs_ref[rows, :] = jnp.dot(hid_ref[rows, :], w2buf[slot, e], preferred_element_type=F32).astype(BF16)
                return carry2

            lax.fori_loop(0, local // 4, experts, 0)
            for h in range(2):
                send_ref[i, h] = jnp.dot(p_ref[...], qs_ref[:, h * cw:(h + 1) * cw], preferred_element_type=F32).astype(BF16).reshape(GROUPS, rows_c, cw)
            land_ref[i, :, ep] = send_ref[i, :, ep]

            @pl.when(i + DOWN_BUFS < steps)
            def _():
                for c in weight_copies(i + DOWN_BUFS, slot):
                    c.start()
            for n in range(3):
                q_copy(i, n).start()

        @pl.when((i >= 1) & (i < steps + 1))
        def _():
            k = i - 1
            for n in range(3):
                q_copy(k, n).wait_recv()
            block = land_ref[k, 1 - tp].reshape(GROUPS * rows_c, cw)
            fwd_ref[k] = jnp.dot(s_ref[...], block, preferred_element_type=F32).astype(BF16)
            f_copy(k).start()

        @pl.when(i >= 2)
        def _():
            k = i - 2
            mine = land_ref[k, tp].reshape(GROUPS * rows_c, cw)
            mix = jnp.dot(a_ref[2], mine, preferred_element_type=F32)
            mix += jnp.dot(a_ref[1], mine, preferred_element_type=F32)
            mix += jnp.dot(a_ref[0], mine, preferred_element_type=F32)
            f_copy(k).wait_recv()
            theirs = yland_ref[k]
            for z in (2, 1, 0):
                mix += jnp.dot(b_ref[z], theirs, preferred_element_type=F32)
            cols = pl.ds(pl.multiple_of(tp * half + k * cw, 128), cw)
            out_ref[:, cols] = (x_ref[:, cols].astype(F32) + mix).astype(BF16)
            o_copy(k).start()
        return carry

    lax.fori_loop(0, steps + 2, main, 0)

    def last_waits(k, carry):
        for n in range(3):
            q_copy(k, n).wait_send()
        f_copy(k).wait_send()
        o_copy(k).wait_send()
        cols = pl.ds(pl.multiple_of((1 - tp) * half + k * cw, 128), cw)
        remote(out_ref.at[:, cols], out_ref.at[:, cols], o_s.at[k], o_r.at[k], other_tp).wait_recv()
        return carry

    lax.fori_loop(0, steps, last_waits, 0)


def routing(choice):
    ep = lax.axis_index('ep')
    pairs = choice.shape[0] * choice.shape[1]
    ids = lax.all_gather(choice, 'ep', tiled=True).reshape(GROUPS, pairs)
    onehot = (ids[:, :, None] == jnp.arange(128, dtype=jnp.int32)).astype(BF16)
    order = jnp.arange(pairs, dtype=jnp.int32)
    tri = (order[:, None] > order[None, :]).astype(BF16)
    earlier = jnp.einsum('pq,gqe->gpe', tri, onehot, preferred_element_type=F32)
    position = jnp.sum(earlier * onehot.astype(F32), axis=-1).astype(jnp.int32)
    kept = position < CAP
    owner = ids // 32
    hot = ((owner[:, :, None] == jnp.arange(GROUPS, dtype=jnp.int32)) & kept[:, :, None])
    hot = jnp.concatenate([hot, kept[:, :, None]], axis=-1).astype(BF16)
    before = jnp.einsum('pq,gqe->gpe', tri, hot, preferred_element_type=F32)
    rank = jnp.sum((before * hot.astype(F32))[:, :, :GROUPS], axis=-1).astype(jnp.int32)
    nrank = before[:, :, GROUPS].astype(jnp.int32)
    count = jnp.sum(hot.astype(F32), axis=1).astype(jnp.int32)
    max_c = jnp.max(count[:, :GROUPS])
    max_n = jnp.max(count[:, GROUPS])
    group = jnp.arange(GROUPS, dtype=jnp.int32)[:, None]
    slot = jnp.where(kept & (owner == ep), (ids - ep * 32) * 16 + group * CAP + position, -1).reshape(-1)
    token = (group * (pairs // 2) + order[None, :] // 2).reshape(-1)
    match = slot[None, :] == jnp.arange(512, dtype=jnp.int32)[:, None]
    tok_of = jnp.max(jnp.where(match, token[None, :], -1), axis=1)
    slotkey = jnp.max(jnp.where(match, (group * 128 + rank).reshape(-1)[None, :], -1), axis=1)
    key = jnp.where(kept, owner * 128 + rank, -1)
    npos = jnp.where(kept, nrank, -1)
    my_key = lax.dynamic_index_in_dim(key, ep, 0, keepdims=False)
    my_n = lax.dynamic_index_in_dim(npos, ep, 0, keepdims=False)
    nkey = jnp.max(jnp.where(my_key[None, :] == jnp.arange(512, dtype=jnp.int32)[:, None], my_n[None, :], -1), axis=1)
    return tok_of[:, None], slotkey[None, :], my_key.reshape(-1, 2), my_n.reshape(-1, 2), nkey.reshape(GROUPS, 128), max_c, max_n


def run_up(x, g, wr, wg, wu, tok_of, choice):
    tok, d_model = x.shape
    local = wg.shape[0]
    cw = d_model // 2 // UP_STEPS
    slots = tok_of.shape[0]
    vm = pl.BlockSpec(memory_space=pltpu.VMEM)
    hbm = pl.BlockSpec(memory_space=pl.ANY)
    sem = pltpu.SemaphoreType.DMA
    return pl.pallas_call(
        up_kernel,
        out_shape=(jax.ShapeDtypeStruct((slots, 128), BF16), jax.ShapeDtypeStruct((tok, 2), F32)),
        in_specs=[vm, vm, hbm, hbm, hbm, vm, vm],
        out_specs=(vm, vm),
        scratch_shapes=[
            pltpu.VMEM((UP_STEPS, 2, GROUPS, tok, cw), BF16),
            pltpu.VMEM((slots, 2 * cw), BF16),
            pltpu.VMEM((slots, GROUPS * tok), BF16),
            pltpu.VMEM((slots, 256), F32),
            pltpu.VMEM((UP_BUFS, local, 2 * cw, 256), BF16),
            pltpu.VMEM(wr.shape, BF16),
            pltpu.VMEM((tok, 128), F32),
            sem((UP_BUFS, 4)), sem,
        ] + [sem((UP_STEPS,))] * 10,
        compiler_params=pltpu.CompilerParams(collective_id=0, has_side_effects=True, vmem_limit_bytes=VMEM_LIMIT),
        name='up',
    )(x, g, wr, wg, wu, tok_of, choice)


def run_down(tier, rows_c, rows_n, hid, x, gate, slotkey, poskey, npos, nkey, wd):
    tok, d_model = x.shape
    local = wd.shape[0]
    cw = d_model // 2 // DOWN_STEPS
    slots = hid.shape[0]
    keys = (jnp.arange(GROUPS, dtype=jnp.int32)[:, None] * 128 + jnp.arange(rows_c, dtype=jnp.int32)[None, :]).reshape(-1)
    nkey = nkey[:, :rows_c].reshape(1, -1)
    vm = pl.BlockSpec(memory_space=pltpu.VMEM)
    hbm = pl.BlockSpec(memory_space=pl.ANY)
    sem = pltpu.SemaphoreType.DMA
    return pl.pallas_call(
        functools.partial(down_kernel, rows_c, rows_n),
        out_shape=jax.ShapeDtypeStruct(x.shape, BF16),
        in_specs=[vm] * 9 + [hbm],
        out_specs=vm,
        scratch_shapes=[
            pltpu.VMEM((DOWN_STEPS, 2, GROUPS, rows_c, cw), BF16),
            pltpu.VMEM((DOWN_STEPS, 2, GROUPS, rows_c, cw), BF16),
            pltpu.VMEM((DOWN_STEPS, rows_n, cw), BF16),
            pltpu.VMEM((DOWN_STEPS, rows_n, cw), BF16),
            pltpu.VMEM((slots, 2 * cw), BF16),
            pltpu.VMEM((DOWN_BUFS, local, 128, 2 * cw), BF16),
            pltpu.VMEM((GROUPS * rows_c, slots), BF16),
            pltpu.VMEM((rows_n, GROUPS * rows_c), BF16),
            pltpu.VMEM((3, tok, GROUPS * rows_c), BF16),
            pltpu.VMEM((3, tok, rows_n), BF16),
            sem((DOWN_BUFS, 2)), sem((DOWN_STEPS, 3)), sem((DOWN_STEPS, 3)),
            sem((DOWN_STEPS,)), sem((DOWN_STEPS,)), sem((DOWN_STEPS,)), sem((DOWN_STEPS,)),
        ],
        compiler_params=pltpu.CompilerParams(collective_id=1 + tier, has_side_effects=True, vmem_limit_bytes=VMEM_LIMIT),
        name='down%d' % rows_c,
    )(hid, x, gate, slotkey, keys[:, None], keys[None, :], nkey, poskey, npos, wd)


def solution(mesh):
    row_spec = P(('dp', 'ep'), None)

    def device_step(resid_in, norm_scale, w_router, w_gate, w_up, w_down, choice):
        tok_of, slotkey, poskey, npos, nkey, max_c, max_n = routing(choice)
        hid, gate = run_up(resid_in, norm_scale[None, :], w_router, w_gate, w_up, tok_of, choice)
        args = (hid, resid_in, gate, slotkey, poskey, npos, nkey, w_down)
        small = (max_c <= 64) & (max_n <= 176)
        return lax.cond(small, functools.partial(run_down, 0, 64, 176), functools.partial(run_down, 1, 128, 256), *args)

    return jax.shard_map(device_step, mesh=mesh, in_specs=(row_spec, P(None), P(None, None), P('ep', None, 'tp'), P('ep', None, 'tp'), P('ep', 'tp', None), row_spec), out_specs=row_spec, check_vma=False)
```

```python
import functools

import jax
import jax.numpy as jnp
from jax import lax
from jax.experimental import pallas as pl
from jax.experimental.pallas import tpu as pltpu
from jax.sharding import PartitionSpec as P

NORM_EPS = 1e-5
MESH = pl.DeviceIdType.MESH
F32 = jnp.float32
BF16 = jnp.bfloat16
CAP = 4
GROUPS = 4
UP_STEPS = 14
UP_BUFS = 4
UP_LAG = 3
DOWN_STEPS = 14
DOWN_BUFS = 6
DOWN_LAG = 2
TIERS = ((64, 176), (128, 256))
VMEM_LIMIT = 62 * 1024 * 1024


def remote(src, dst, send_sem, recv_sem, device):
    return pltpu.make_async_remote_copy(src_ref=src, dst_ref=dst, send_sem=send_sem, recv_sem=recv_sem, device_id=device, device_id_type=MESH)


def place():
    dp, tp, ep = lax.axis_index('dp'), lax.axis_index('tp'), lax.axis_index('ep')
    return dp, tp, ep, ep // 2, ep % 2


def column(row):
    n = row.shape[1]
    eye = lax.broadcasted_iota(jnp.int32, (n, n), 0) == lax.broadcasted_iota(jnp.int32, (n, n), 1)
    return jnp.sum(jnp.where(eye, row.astype(F32), 0.0), axis=1, keepdims=True).astype(jnp.int32)


def up_kernel(x_ref, g_ref, wr_hbm, wg_hbm, wu_hbm, choice_ref, hid_ref, gate_ref, tab_ref, flag_ref,
              u_ref, xs_ref, pick_ref, acc_ref, wbuf, wr_ref, logit_ref, ch_ref,
              w_sem, wr_sem, c_s, c_r, own_s, own_r, x_s, x_r, y_s, y_r, dx_s, dx_r, dy_s, dy_r):
    dp, tp, ep, cx, core = place()
    local = wg_hbm.shape[0]
    tok, d_model = x_ref.shape
    half = d_model // 2
    steps = UP_STEPS
    cw = half // steps
    twin = (dp, tp, cx * 2 + (1 - core))
    across = (dp, tp, (1 - cx) * 2 + core)
    far_twin = (dp, tp, (1 - cx) * 2 + (1 - core))
    other_tp = (dp, 1 - tp, ep)
    far = (1 - cx) * 2 + core

    barrier = pltpu.get_barrier_semaphore()
    for peer in (twin, across, far_twin, other_tp):
        pl.semaphore_signal(barrier, inc=1, device_id=peer, device_id_type=MESH)

    def weight_copies(step, slot):
        out = []
        for h in range(2):
            rows = pl.ds(pl.multiple_of(h * half + step * cw, cw), cw)
            for m, w in enumerate((wg_hbm, wu_hbm)):
                out.append(pltpu.make_async_copy(w.at[:, rows, :], wbuf.at[slot, :, h * cw:(h + 1) * cw, m * 128:(m + 1) * 128], w_sem.at[slot, h * 2 + m]))
        return out

    wr_copy = pltpu.make_async_copy(wr_hbm, wr_ref, wr_sem)
    for c in weight_copies(0, 0):
        c.start()
    wr_copy.start()
    for b in range(1, UP_BUFS):
        for c in weight_copies(b, b):
            c.start()

    scale = g_ref[...].astype(F32).reshape(1, d_model)

    def norm_rows(r, carry):
        rows = pl.ds(pl.multiple_of(r * 16, 16), 16)
        xb = x_ref[rows, :].astype(F32)
        cen = xb - jnp.mean(xb, axis=-1, keepdims=True)
        var = jnp.mean(cen * cen, axis=-1, keepdims=True)
        u = (cen * lax.rsqrt(var + NORM_EPS) * scale).astype(BF16)
        for j in range(steps):
            for h in range(2):
                u_ref[j, h, ep, rows, :] = u[:, h * half + j * cw:h * half + (j + 1) * cw]
        return carry

    lax.fori_loop(0, tok // 16, norm_rows, 0)
    pl.semaphore_wait(barrier, 4)

    def choice_copy(n):
        peer = (across, far_twin, twin)[n]
        return remote(choice_ref, ch_ref.at[ep], c_s.at[n], c_r.at[n], peer)

    for n in range(3):
        choice_copy(n).start()

    def own_copy(j):
        return remote(u_ref.at[j, :, ep], u_ref.at[j, :, ep], own_s.at[j], own_r.at[j], twin)

    def x_copy(j):
        return remote(u_ref.at[j, tp, ep], u_ref.at[j, tp, ep], x_s.at[j], x_r.at[j], across)

    def y_copy(j):
        return remote(u_ref.at[j, tp, far], u_ref.at[j, tp, far], y_s.at[j], y_r.at[j], other_tp)

    def dx_copy(j):
        return remote(u_ref.at[j, tp, far], u_ref.at[j, tp, far], dx_s.at[j], dx_r.at[j], twin)

    def dy_copy(j):
        return remote(u_ref.at[j, 1 - tp, far], u_ref.at[j, 1 - tp, far], dy_s.at[j], dy_r.at[j], twin)

    def first_sends(j, carry):
        x_copy(j).start()
        own_copy(j).start()
        return carry

    lax.fori_loop(0, steps, first_sends, 0)
    ch_ref[ep] = choice_ref[...]
    acc_ref[...] = jnp.zeros_like(acc_ref)
    logit_ref[...] = jnp.zeros_like(logit_ref)
    wr_copy.wait()
    for n in range(3):
        choice_copy(n).wait_recv()

    slots = pick_ref.shape[0]
    upper = jnp.where(lax.broadcasted_iota(jnp.int32, (tok, tok), 0) < lax.broadcasted_iota(jnp.int32, (tok, tok), 1), 1.0, 0.0).astype(BF16)
    ids = lax.broadcasted_iota(jnp.int32, (tok, tok), 0)
    lane16 = lax.broadcasted_iota(jnp.int32, (16, tok), 0)
    slot_iota = lax.broadcasted_iota(jnp.int32, (slots, tok), 0)
    most = jnp.zeros((16, 1), F32)
    for g in range(GROUPS):
        c = [ch_ref[g, j:j + 1, :] for j in range(2)]
        hot = [jnp.where(ids == c[j], 1.0, 0.0) for j in range(2)]
        earlier = jnp.dot((hot[0] + hot[1]).astype(BF16), upper, preferred_element_type=F32)
        pos = [jnp.sum(earlier * hot[j], axis=0, keepdims=True).astype(jnp.int32) for j in range(2)]
        kept = [pos[j] < CAP for j in range(2)]
        keptf = [jnp.where(kept[j], 1.0, 0.0) for j in range(2)]
        owner = [c[j] // 32 for j in range(2)]
        mine = [jnp.where(lane16 == owner[j], keptf[j], 0.0) for j in range(2)]
        every = [jnp.where(lane16 == GROUPS, keptf[j], 0.0) for j in range(2)]
        tally = mine[0] + mine[1] + every[0] + every[1]
        before = jnp.dot(tally.astype(BF16), upper, preferred_element_type=F32)
        most = jnp.maximum(most, jnp.sum(tally, axis=1, keepdims=True))
        rank = [jnp.sum(before * mine[j], axis=0, keepdims=True) for j in range(2)]
        rank[1] = rank[1] + jnp.where(owner[0] == owner[1], keptf[0], 0.0)
        nrank = [before[GROUPS:GROUPS + 1, :], before[GROUPS:GROUPS + 1, :] + keptf[0]]
        for j in range(2):
            slot = jnp.where(kept[j] & (owner[j] == ep), (c[j] - ep * 32) * 16 + g * CAP + pos[j], -1)
            tab_ref[g, j:j + 1, :] = slot
            tab_ref[g, 2 + j:3 + j, :] = jnp.where(kept[j], owner[j] * 128 + rank[j].astype(jnp.int32), -1)
            tab_ref[g, 4 + j:5 + j, :] = jnp.where(kept[j], nrank[j].astype(jnp.int32), -1)
        tab_ref[g, 6:8, :] = jnp.zeros((2, tok), jnp.int32)
        pick_ref[:, g * tok:(g + 1) * tok] = jnp.where((slot_iota == tab_ref[g, 0:1, :]) | (slot_iota == tab_ref[g, 1:2, :]), 1.0, 0.0).astype(BF16)
    sub16 = lax.broadcasted_iota(jnp.int32, (16, 1), 0)
    fits = [jnp.where(sub16 < GROUPS, rows_c, jnp.where(sub16 == GROUPS, rows_n, 0)).astype(F32) for rows_c, rows_n in TIERS[:-1]]
    level = jnp.zeros((1, 1), F32)
    for f in fits:
        level = level + jnp.max(jnp.where(most > f, 1.0, 0.0), axis=0, keepdims=True)
    flag_ref[...] = jnp.broadcast_to(level, flag_ref.shape).astype(jnp.int32)

    def main(i, carry):
        @pl.when(i < steps)
        def _():
            x_copy(i).wait_recv()
            y_copy(i).start()
            dx_copy(i).start()

        @pl.when((i >= UP_LAG) & (i < steps + UP_LAG))
        def _():
            j = i - UP_LAG
            y_copy(j).wait_recv()
            dy_copy(j).start()

        @pl.when(i >= UP_LAG + 1)
        def _():
            j = i - UP_LAG - 1
            slot = lax.rem(j, UP_BUFS)
            for h in range(2):
                kr = pl.ds(pl.multiple_of(h * half + j * cw, cw), cw)
                logit_ref[...] += jnp.dot(u_ref[j, h, ep], wr_ref[kr, :], preferred_element_type=F32)
            own_copy(j).wait_recv()
            dx_copy(j).wait_recv()
            dy_copy(j).wait_recv()
            for h in range(2):
                block = u_ref[j, h].reshape(GROUPS * tok, cw)
                xs_ref[:, h * cw:(h + 1) * cw] = jnp.dot(pick_ref[...], block, preferred_element_type=F32).astype(BF16)
            for c in weight_copies(j, slot):
                c.wait()

            def experts(t, carry2):
                for z in range(4):
                    e = t * 4 + z
                    rows = pl.ds(pl.multiple_of(e * 16, 16), 16)
                    acc_ref[rows, :] += jnp.dot(xs_ref[rows, :], wbuf[slot, e], preferred_element_type=F32)
                return carry2

            lax.fori_loop(0, local // 4, experts, 0)

            @pl.when(j + UP_BUFS < steps)
            def _():
                for c in weight_copies(j + UP_BUFS, slot):
                    c.start()
        return carry

    lax.fori_loop(0, steps + UP_LAG + 1, main, 0)

    gate_act = acc_ref[:, :128]
    hid_ref[...] = (gate_act * jax.nn.sigmoid(gate_act) * acc_ref[:, 128:]).astype(BF16)
    logits = logit_ref[...]
    ex = jnp.exp(logits - jnp.max(logits, axis=-1, keepdims=True))
    probs = ex / jnp.sum(ex, axis=-1, keepdims=True)
    lanes = lax.broadcasted_iota(jnp.int32, probs.shape, 1)
    picked = [jnp.sum(jnp.where(column(ch_ref[ep, j:j + 1, :]) == lanes, probs, 0.0), axis=-1, keepdims=True) for j in range(2)]
    for j in range(2):
        gate_ref[:, j:j + 1] = picked[j] / (picked[0] + picked[1])

    def last_waits(j, carry):
        x_copy(j).wait_send()
        own_copy(j).wait_send()
        y_copy(j).wait_send()
        dx_copy(j).wait_send()
        dy_copy(j).wait_send()
        return carry

    lax.fori_loop(0, steps, last_waits, 0)
    for n in range(3):
        choice_copy(n).wait_send()


def down_kernel(rows_c, rows_n, hid_ref, x_ref, gate_ref, tab_ref, wd_hbm, out_ref,
                send_ref, land_ref, fwd_ref, yland_ref, qs_ref, w2buf, p_ref, s_ref, a_ref, b_ref,
                w_sem, q_s, q_r, f_s, f_r, o_s, o_r):
    dp, tp, ep, cx, core = place()
    local = wd_hbm.shape[0]
    tok, d_model = x_ref.shape
    half = d_model // 2
    steps = DOWN_STEPS
    cw = half // steps
    peers = [(1 - cx) * 2 + core, (1 - cx) * 2 + (1 - core), cx * 2 + (1 - core)]
    other_tp = (dp, 1 - tp, ep)

    barrier = pltpu.get_barrier_semaphore()
    for g in peers:
        pl.semaphore_signal(barrier, inc=1, device_id=(dp, tp, g), device_id_type=MESH)
    pl.semaphore_signal(barrier, inc=1, device_id=other_tp, device_id_type=MESH)

    def weight_copies(step, slot):
        out = []
        for h in range(2):
            cols = pl.ds(pl.multiple_of(h * half + step * cw, 128), cw)
            out.append(pltpu.make_async_copy(wd_hbm.at[:, :, cols], w2buf.at[slot, :, :, h * cw:(h + 1) * cw], w_sem.at[slot, h]))
        return out

    for b in range(DOWN_BUFS):
        for c in weight_copies(b, b):
            c.start()

    all_rows = GROUPS * rows_c
    slots = qs_ref.shape[0]
    gap = 128 - rows_c
    slot_iota = lax.broadcasted_iota(jnp.int32, (slots, tok), 0)
    c_iota = lax.broadcasted_iota(jnp.int32, (rows_c, tok), 0)

    def key_of(r):
        for n in range(1, GROUPS):
            r = r + jnp.where(r >= n * rows_c + (n - 1) * gap, gap, 0)
        return r

    def onehot(rows, values):
        return jnp.where(rows == values, 1.0, 0.0).astype(BF16)

    def times_t(a, b):
        return lax.dot_general(a, b, (((1,), (1,)), ((), ())), preferred_element_type=F32)

    for g in range(GROUPS):
        total = jnp.zeros((rows_c, slots), F32)
        for j in range(2):
            total += times_t(onehot(c_iota + ep * 128, tab_ref[g, 2 + j:3 + j, :]), onehot(slot_iota, tab_ref[g, j:j + 1, :]))
        p_ref[g * rows_c:(g + 1) * rows_c, :] = total.astype(BF16)
    key_iota = key_of(lax.broadcasted_iota(jnp.int32, (all_rows, tok), 0))
    n_iota = lax.broadcasted_iota(jnp.int32, (rows_n, tok), 0)
    my_key = [tab_ref[ep, 2 + j:3 + j, :] for j in range(2)]
    my_n = [tab_ref[ep, 4 + j:5 + j, :] for j in range(2)]
    total = jnp.zeros((rows_n, all_rows), F32)
    for j in range(2):
        total += times_t(onehot(n_iota, my_n[j]), onehot(key_iota, my_key[j]))
    s_ref[...] = total.astype(BF16)

    def split_gates(keys, pos, dst):
        mat = jnp.where(pos[0] == keys, gate_ref[:, 0:1], 0.0) + jnp.where(pos[1] == keys, gate_ref[:, 1:2], 0.0)
        for z in range(3):
            part = mat.astype(BF16)
            dst[z] = part
            mat = mat - part.astype(F32)

    split_gates(key_of(lax.broadcasted_iota(jnp.int32, (tok, all_rows), 1)), [column(v) for v in my_key], a_ref)
    split_gates(lax.broadcasted_iota(jnp.int32, (tok, rows_n), 1), [column(v) for v in my_n], b_ref)
    pl.semaphore_wait(barrier, 4)

    def q_copy(k, n):
        return remote(send_ref.at[k, :, peers[n]], land_ref.at[k, :, ep], q_s.at[k, n], q_r.at[k, n], (dp, tp, peers[n]))

    def f_copy(k):
        return remote(fwd_ref.at[k], yland_ref.at[k], f_s.at[k], f_r.at[k], other_tp)

    def o_copy(k):
        cols = pl.ds(pl.multiple_of(tp * half + k * cw, 128), cw)
        return remote(out_ref.at[:, cols], out_ref.at[:, cols], o_s.at[k], o_r.at[k], other_tp)

    def main(i, carry):
        @pl.when(i < steps)
        def _():
            slot = lax.rem(i, DOWN_BUFS)
            for c in weight_copies(i, slot):
                c.wait()

            def experts(t, carry2):
                for z in range(4):
                    e = t * 4 + z
                    rows = pl.ds(pl.multiple_of(e * 16, 16), 16)
                    qs_ref[rows, :] = jnp.dot(hid_ref[rows, :], w2buf[slot, e], preferred_element_type=F32).astype(BF16)
                return carry2

            lax.fori_loop(0, local // 4, experts, 0)
            for h in range(2):
                send_ref[i, h] = jnp.dot(p_ref[...], qs_ref[:, h * cw:(h + 1) * cw], preferred_element_type=F32).astype(BF16).reshape(GROUPS, rows_c, cw)
            land_ref[i, :, ep] = send_ref[i, :, ep]

            @pl.when(i + DOWN_BUFS < steps)
            def _():
                for c in weight_copies(i + DOWN_BUFS, slot):
                    c.start()
            for n in range(3):
                q_copy(i, n).start()

        @pl.when((i >= DOWN_LAG) & (i < steps + DOWN_LAG))
        def _():
            k = i - DOWN_LAG
            for n in range(3):
                q_copy(k, n).wait_recv()
            block = land_ref[k, 1 - tp].reshape(GROUPS * rows_c, cw)
            fwd_ref[k] = jnp.dot(s_ref[...], block, preferred_element_type=F32).astype(BF16)
            f_copy(k).start()

        @pl.when(i >= 2 * DOWN_LAG)
        def _():
            k = i - 2 * DOWN_LAG
            mine = land_ref[k, tp].reshape(GROUPS * rows_c, cw)
            mix = jnp.dot(a_ref[2], mine, preferred_element_type=F32)
            mix += jnp.dot(a_ref[1], mine, preferred_element_type=F32)
            mix += jnp.dot(a_ref[0], mine, preferred_element_type=F32)
            f_copy(k).wait_recv()
            theirs = yland_ref[k]
            for z in (2, 1, 0):
                mix += jnp.dot(b_ref[z], theirs, preferred_element_type=F32)
            cols = pl.ds(pl.multiple_of(tp * half + k * cw, 128), cw)
            out_ref[:, cols] = (x_ref[:, cols].astype(F32) + mix).astype(BF16)
            o_copy(k).start()
        return carry

    lax.fori_loop(0, steps + 2 * DOWN_LAG, main, 0)

    def last_waits(k, carry):
        for n in range(3):
            q_copy(k, n).wait_send()
        f_copy(k).wait_send()
        o_copy(k).wait_send()
        cols = pl.ds(pl.multiple_of((1 - tp) * half + k * cw, 128), cw)
        remote(out_ref.at[:, cols], out_ref.at[:, cols], o_s.at[k], o_r.at[k], other_tp).wait_recv()
        return carry

    lax.fori_loop(0, steps, last_waits, 0)


def run_up(x, g, wr, wg, wu, choice_t):
    tok, d_model = x.shape
    local = wg.shape[0]
    cw = d_model // 2 // UP_STEPS
    slots = local * GROUPS * CAP
    vm = pl.BlockSpec(memory_space=pltpu.VMEM)
    hbm = pl.BlockSpec(memory_space=pl.ANY)
    sem = pltpu.SemaphoreType.DMA
    return pl.pallas_call(
        up_kernel,
        out_shape=(
            jax.ShapeDtypeStruct((slots, 128), BF16),
            jax.ShapeDtypeStruct((tok, 2), F32),
            jax.ShapeDtypeStruct((GROUPS, 8, tok), jnp.int32),
            jax.ShapeDtypeStruct((8, 128), jnp.int32),
        ),
        in_specs=[vm, vm, hbm, hbm, hbm, vm],
        out_specs=(vm, vm, vm, vm),
        scratch_shapes=[
            pltpu.VMEM((UP_STEPS, 2, GROUPS, tok, cw), BF16),
            pltpu.VMEM((slots, 2 * cw), BF16),
            pltpu.VMEM((slots, GROUPS * tok), BF16),
            pltpu.VMEM((slots, 256), F32),
            pltpu.VMEM((UP_BUFS, local, 2 * cw, 256), BF16),
            pltpu.VMEM(wr.shape, BF16),
            pltpu.VMEM((tok, 128), F32),
            pltpu.VMEM((GROUPS, 2, tok), jnp.int32),
            sem((UP_BUFS, 4)), sem, sem((3,)), sem((3,)),
        ] + [sem((UP_STEPS,))] * 10,
        compiler_params=pltpu.CompilerParams(collective_id=0, has_side_effects=True, vmem_limit_bytes=VMEM_LIMIT),
        name='up',
    )(x, g, wr, wg, wu, choice_t)


def run_down(tier, hid, x, gate, tab, wd):
    rows_c, rows_n = TIERS[tier]
    tok, d_model = x.shape
    local = wd.shape[0]
    cw = d_model // 2 // DOWN_STEPS
    slots = hid.shape[0]
    vm = pl.BlockSpec(memory_space=pltpu.VMEM)
    hbm = pl.BlockSpec(memory_space=pl.ANY)
    sem = pltpu.SemaphoreType.DMA
    return pl.pallas_call(
        functools.partial(down_kernel, rows_c, rows_n),
        out_shape=jax.ShapeDtypeStruct(x.shape, BF16),
        in_specs=[vm] * 4 + [hbm],
        out_specs=vm,
        scratch_shapes=[
            pltpu.VMEM((DOWN_STEPS, 2, GROUPS, rows_c, cw), BF16),
            pltpu.VMEM((DOWN_STEPS, 2, GROUPS, rows_c, cw), BF16),
            pltpu.VMEM((DOWN_STEPS, rows_n, cw), BF16),
            pltpu.VMEM((DOWN_STEPS, rows_n, cw), BF16),
            pltpu.VMEM((slots, 2 * cw), BF16),
            pltpu.VMEM((DOWN_BUFS, local, 128, 2 * cw), BF16),
            pltpu.VMEM((GROUPS * rows_c, slots), BF16),
            pltpu.VMEM((rows_n, GROUPS * rows_c), BF16),
            pltpu.VMEM((3, tok, GROUPS * rows_c), BF16),
            pltpu.VMEM((3, tok, rows_n), BF16),
            sem((DOWN_BUFS, 2)), sem((DOWN_STEPS, 3)), sem((DOWN_STEPS, 3)),
            sem((DOWN_STEPS,)), sem((DOWN_STEPS,)), sem((DOWN_STEPS,)), sem((DOWN_STEPS,)),
        ],
        compiler_params=pltpu.CompilerParams(collective_id=1 + tier, has_side_effects=True, vmem_limit_bytes=VMEM_LIMIT),
        name='down%d' % rows_c,
    )(hid, x, gate, tab, wd)


def solution(mesh):
    row_spec = P(('dp', 'ep'), None)

    def device_step(resid_in, norm_scale, w_router, w_gate, w_up, w_down, choice):
        hid, gate, tab, flag = run_up(resid_in, norm_scale, w_router, w_gate, w_up, choice.T)
        return lax.switch(flag[0, 0], [functools.partial(run_down, t) for t in range(len(TIERS))], hid, resid_in, gate, tab, w_down)

    return jax.shard_map(device_step, mesh=mesh, in_specs=(row_spec, P(None), P(None, None), P('ep', None, 'tp'), P('ep', None, 'tp'), P('ep', 'tp', None), row_spec), out_specs=row_spec, check_vma=False)
```

```python
import functools

import jax
import jax.numpy as jnp
from jax import lax
from jax.experimental import pallas as pl
from jax.experimental.pallas import tpu as pltpu
from jax.sharding import PartitionSpec as P

NORM_EPS = 1e-5
MESH = pl.DeviceIdType.MESH
F32 = jnp.float32
BF16 = jnp.bfloat16
CAP = 4
GROUPS = 4
UP_STEPS = 14
UP_BUFS = 4
UP_LAG = 3
DOWN_STEPS = 14
DOWN_BUFS = 6
DOWN_LAG = 2
TIERS = ((64, 176), (128, 256))
DOWN_VMEM = (46 * 1024 * 1024, 56 * 1024 * 1024)
VMEM_LIMIT = 58 * 1024 * 1024


def remote(src, dst, send_sem, recv_sem, device):
    return pltpu.make_async_remote_copy(src_ref=src, dst_ref=dst, send_sem=send_sem, recv_sem=recv_sem, device_id=device, device_id_type=MESH)


def place():
    dp, tp, ep = lax.axis_index('dp'), lax.axis_index('tp'), lax.axis_index('ep')
    return dp, tp, ep, ep // 2, ep % 2


def column(row):
    n = row.shape[1]
    eye = lax.broadcasted_iota(jnp.int32, (n, n), 0) == lax.broadcasted_iota(jnp.int32, (n, n), 1)
    return jnp.sum(jnp.where(eye, row.astype(F32), 0.0), axis=1, keepdims=True).astype(jnp.int32)


def up_kernel(x_ref, g_ref, wr_hbm, wg_hbm, wu_hbm, choice_ref, hid_ref, gate_ref, tab_ref, flag_ref,
              u_ref, xs_ref, pick_ref, acc_ref, wbuf, wr_ref, logit_ref, ch_ref,
              w_sem, wr_sem, c_s, c_r, own_s, own_r, x_s, x_r, y_s, y_r, dx_s, dx_r, dy_s, dy_r):
    dp, tp, ep, cx, core = place()
    local = wg_hbm.shape[0]
    tok, d_model = x_ref.shape
    half = d_model // 2
    steps = UP_STEPS
    cw = half // steps
    twin = (dp, tp, cx * 2 + (1 - core))
    across = (dp, tp, (1 - cx) * 2 + core)
    far_twin = (dp, tp, (1 - cx) * 2 + (1 - core))
    other_tp = (dp, 1 - tp, ep)
    far = (1 - cx) * 2 + core

    barrier = pltpu.get_barrier_semaphore()
    for peer in (twin, across, far_twin, other_tp):
        pl.semaphore_signal(barrier, inc=1, device_id=peer, device_id_type=MESH)

    def weight_copies(step, slot):
        out = []
        for h in range(2):
            rows = pl.ds(pl.multiple_of(h * half + step * cw, cw), cw)
            for m, w in enumerate((wg_hbm, wu_hbm)):
                out.append(pltpu.make_async_copy(w.at[:, rows, :], wbuf.at[slot, m, :, h * cw:(h + 1) * cw, :], w_sem.at[slot, h * 2 + m]))
        return out

    wr_copy = pltpu.make_async_copy(wr_hbm, wr_ref, wr_sem)
    for c in weight_copies(0, 0):
        c.start()
    wr_copy.start()
    for b in range(1, UP_BUFS):
        for c in weight_copies(b, b):
            c.start()

    scale = g_ref[...].astype(F32).reshape(1, d_model)

    def norm_rows(r, carry):
        rows = pl.ds(pl.multiple_of(r * 16, 16), 16)
        xb = x_ref[rows, :].astype(F32)
        cen = xb - jnp.mean(xb, axis=-1, keepdims=True)
        var = jnp.mean(cen * cen, axis=-1, keepdims=True)
        u = (cen * lax.rsqrt(var + NORM_EPS) * scale).astype(BF16)
        for j in range(steps):
            for h in range(2):
                u_ref[j, h, ep, rows, :] = u[:, h * half + j * cw:h * half + (j + 1) * cw]
        return carry

    lax.fori_loop(0, tok // 16, norm_rows, 0)
    pl.semaphore_wait(barrier, 4)

    def choice_copy(n):
        peer = (across, far_twin, twin)[n]
        return remote(choice_ref, ch_ref.at[ep], c_s.at[n], c_r.at[n], peer)

    for n in range(3):
        choice_copy(n).start()

    def own_copy(j):
        return remote(u_ref.at[j, :, ep], u_ref.at[j, :, ep], own_s.at[j], own_r.at[j], twin)

    def x_copy(j):
        return remote(u_ref.at[j, tp, ep], u_ref.at[j, tp, ep], x_s.at[j], x_r.at[j], across)

    def y_copy(j):
        return remote(u_ref.at[j, tp, far], u_ref.at[j, tp, far], y_s.at[j], y_r.at[j], other_tp)

    def dx_copy(j):
        return remote(u_ref.at[j, tp, far], u_ref.at[j, tp, far], dx_s.at[j], dx_r.at[j], twin)

    def dy_copy(j):
        return remote(u_ref.at[j, 1 - tp, far], u_ref.at[j, 1 - tp, far], dy_s.at[j], dy_r.at[j], twin)

    def first_sends(j, carry):
        x_copy(j).start()
        own_copy(j).start()
        return carry

    lax.fori_loop(0, steps, first_sends, 0)
    ch_ref[ep] = choice_ref[...]
    acc_ref[...] = jnp.zeros_like(acc_ref)
    logit_ref[...] = jnp.zeros_like(logit_ref)
    wr_copy.wait()
    for n in range(3):
        choice_copy(n).wait_recv()

    slots = pick_ref.shape[0]
    upper = jnp.where(lax.broadcasted_iota(jnp.int32, (tok, tok), 0) < lax.broadcasted_iota(jnp.int32, (tok, tok), 1), 1.0, 0.0).astype(BF16)
    ids = lax.broadcasted_iota(jnp.int32, (tok, tok), 0)
    lane16 = lax.broadcasted_iota(jnp.int32, (16, tok), 0)
    slot_iota = lax.broadcasted_iota(jnp.int32, (slots, tok), 0)
    most = jnp.zeros((16, 1), F32)
    for g in range(GROUPS):
        c = [ch_ref[g, j:j + 1, :] for j in range(2)]
        hot = [jnp.where(ids == c[j], 1.0, 0.0) for j in range(2)]
        earlier = jnp.dot((hot[0] + hot[1]).astype(BF16), upper, preferred_element_type=F32)
        pos = [jnp.sum(earlier * hot[j], axis=0, keepdims=True).astype(jnp.int32) for j in range(2)]
        kept = [pos[j] < CAP for j in range(2)]
        keptf = [jnp.where(kept[j], 1.0, 0.0) for j in range(2)]
        owner = [c[j] // 32 for j in range(2)]
        mine = [jnp.where(lane16 == owner[j], keptf[j], 0.0) for j in range(2)]
        every = [jnp.where(lane16 == GROUPS, keptf[j], 0.0) for j in range(2)]
        tally = mine[0] + mine[1] + every[0] + every[1]
        before = jnp.dot(tally.astype(BF16), upper, preferred_element_type=F32)
        most = jnp.maximum(most, jnp.sum(tally, axis=1, keepdims=True))
        rank = [jnp.sum(before * mine[j], axis=0, keepdims=True) for j in range(2)]
        rank[1] = rank[1] + jnp.where(owner[0] == owner[1], keptf[0], 0.0)
        nrank = [before[GROUPS:GROUPS + 1, :], before[GROUPS:GROUPS + 1, :] + keptf[0]]
        for j in range(2):
            slot = jnp.where(kept[j] & (owner[j] == ep), (c[j] - ep * 32) * 16 + g * CAP + pos[j], -1)
            tab_ref[g, j:j + 1, :] = slot
            tab_ref[g, 2 + j:3 + j, :] = jnp.where(kept[j], owner[j] * 128 + rank[j].astype(jnp.int32), -1)
            tab_ref[g, 4 + j:5 + j, :] = jnp.where(kept[j], nrank[j].astype(jnp.int32), -1)
        tab_ref[g, 6:8, :] = jnp.zeros((2, tok), jnp.int32)
        pick_ref[:, g * tok:(g + 1) * tok] = jnp.where((slot_iota == tab_ref[g, 0:1, :]) | (slot_iota == tab_ref[g, 1:2, :]), 1.0, 0.0).astype(BF16)
    sub16 = lax.broadcasted_iota(jnp.int32, (16, 1), 0)
    fits = [jnp.where(sub16 < GROUPS, rows_c, jnp.where(sub16 == GROUPS, rows_n, 0)).astype(F32) for rows_c, rows_n in TIERS[:-1]]
    level = jnp.zeros((1, 1), F32)
    for f in fits:
        level = level + jnp.max(jnp.where(most > f, 1.0, 0.0), axis=0, keepdims=True)
    flag_ref[0] = jnp.max(level).astype(jnp.int32)

    def main(i, carry):
        @pl.when(i < steps)
        def _():
            x_copy(i).wait_recv()
            y_copy(i).start()
            dx_copy(i).start()

        @pl.when((i >= UP_LAG) & (i < steps + UP_LAG))
        def _():
            j = i - UP_LAG
            y_copy(j).wait_recv()
            dy_copy(j).start()

        @pl.when(i >= UP_LAG + 1)
        def _():
            j = i - UP_LAG - 1
            slot = lax.rem(j, UP_BUFS)
            for h in range(2):
                kr = pl.ds(pl.multiple_of(h * half + j * cw, cw), cw)
                logit_ref[...] += jnp.dot(u_ref[j, h, ep], wr_ref[kr, :], preferred_element_type=F32)
            own_copy(j).wait_recv()
            dx_copy(j).wait_recv()
            dy_copy(j).wait_recv()
            for h in range(2):
                block = u_ref[j, h].reshape(GROUPS * tok, cw)
                xs_ref[:, h * cw:(h + 1) * cw] = jnp.dot(pick_ref[...], block, preferred_element_type=F32).astype(BF16)
            for c in weight_copies(j, slot):
                c.wait()

            def experts(t, carry2):
                for z in range(4):
                    e = t * 4 + z
                    rows = pl.ds(pl.multiple_of(e * 16, 16), 16)
                    acc_ref[rows, :] += jnp.dot(xs_ref[rows, :], jnp.concatenate([wbuf[slot, 0, e], wbuf[slot, 1, e]], axis=1), preferred_element_type=F32)
                return carry2

            lax.fori_loop(0, local // 4, experts, 0)

            @pl.when(j + UP_BUFS < steps)
            def _():
                for c in weight_copies(j + UP_BUFS, slot):
                    c.start()
        return carry

    lax.fori_loop(0, steps + UP_LAG + 1, main, 0)

    gate_act = acc_ref[:, :128]
    hid_ref[...] = (gate_act * jax.nn.sigmoid(gate_act) * acc_ref[:, 128:]).astype(BF16)
    logits = logit_ref[...]
    ex = jnp.exp(logits - jnp.max(logits, axis=-1, keepdims=True))
    probs = ex / jnp.sum(ex, axis=-1, keepdims=True)
    lanes = lax.broadcasted_iota(jnp.int32, probs.shape, 1)
    picked = [jnp.sum(jnp.where(column(ch_ref[ep, j:j + 1, :]) == lanes, probs, 0.0), axis=-1, keepdims=True) for j in range(2)]
    for j in range(2):
        gate_ref[:, j:j + 1] = picked[j] / (picked[0] + picked[1])

    def last_waits(j, carry):
        x_copy(j).wait_send()
        own_copy(j).wait_send()
        y_copy(j).wait_send()
        dx_copy(j).wait_send()
        dy_copy(j).wait_send()
        return carry

    lax.fori_loop(0, steps, last_waits, 0)
    for n in range(3):
        choice_copy(n).wait_send()


def down_kernel(rows_c, rows_n, hid_ref, x_ref, gate_ref, tab_ref, wd_hbm, out_ref,
                send_ref, land_ref, fwd_ref, yland_ref, qs_ref, w2buf, p_ref, s_ref, a_ref, b_ref,
                w_sem, q_s, q_r, f_s, f_r, o_s, o_r):
    dp, tp, ep, cx, core = place()
    local = wd_hbm.shape[0]
    tok, d_model = x_ref.shape
    half = d_model // 2
    steps = DOWN_STEPS
    cw = half // steps
    peers = [(1 - cx) * 2 + core, (1 - cx) * 2 + (1 - core), cx * 2 + (1 - core)]
    other_tp = (dp, 1 - tp, ep)

    barrier = pltpu.get_barrier_semaphore()
    for g in peers:
        pl.semaphore_signal(barrier, inc=1, device_id=(dp, tp, g), device_id_type=MESH)
    pl.semaphore_signal(barrier, inc=1, device_id=other_tp, device_id_type=MESH)

    def weight_copies(step, slot):
        out = []
        for h in range(2):
            cols = pl.ds(pl.multiple_of(h * half + step * cw, 128), cw)
            out.append(pltpu.make_async_copy(wd_hbm.at[:, :, cols], w2buf.at[slot, :, :, h * cw:(h + 1) * cw], w_sem.at[slot, h]))
        return out

    for b in range(DOWN_BUFS):
        for c in weight_copies(b, b):
            c.start()

    all_rows = GROUPS * rows_c
    slots = qs_ref.shape[0]
    gap = 128 - rows_c
    slot_iota = lax.broadcasted_iota(jnp.int32, (slots, tok), 0)
    c_iota = lax.broadcasted_iota(jnp.int32, (rows_c, tok), 0)

    def key_of(r):
        for n in range(1, GROUPS):
            r = r + jnp.where(r >= n * rows_c + (n - 1) * gap, gap, 0)
        return r

    def onehot(rows, values):
        return jnp.where(rows == values, 1.0, 0.0).astype(BF16)

    def times_t(a, b):
        return lax.dot_general(a, b, (((1,), (1,)), ((), ())), preferred_element_type=F32)

    for g in range(GROUPS):
        total = jnp.zeros((rows_c, slots), F32)
        for j in range(2):
            total += times_t(onehot(c_iota + ep * 128, tab_ref[g, 2 + j:3 + j, :]), onehot(slot_iota, tab_ref[g, j:j + 1, :]))
        p_ref[g * rows_c:(g + 1) * rows_c, :] = total.astype(BF16)
    key_iota = key_of(lax.broadcasted_iota(jnp.int32, (all_rows, tok), 0))
    n_iota = lax.broadcasted_iota(jnp.int32, (rows_n, tok), 0)
    my_key = [tab_ref[ep, 2 + j:3 + j, :] for j in range(2)]
    my_n = [tab_ref[ep, 4 + j:5 + j, :] for j in range(2)]
    total = jnp.zeros((rows_n, all_rows), F32)
    for j in range(2):
        total += times_t(onehot(n_iota, my_n[j]), onehot(key_iota, my_key[j]))
    s_ref[...] = total.astype(BF16)

    def split_gates(keys, pos, dst):
        mat = jnp.where(pos[0] == keys, gate_ref[:, 0:1], 0.0) + jnp.where(pos[1] == keys, gate_ref[:, 1:2], 0.0)
        for z in range(3):
            part = mat.astype(BF16)
            dst[z] = part
            mat = mat - part.astype(F32)

    split_gates(key_of(lax.broadcasted_iota(jnp.int32, (tok, all_rows), 1)), [column(v) for v in my_key], a_ref)
    split_gates(lax.broadcasted_iota(jnp.int32, (tok, rows_n), 1), [column(v) for v in my_n], b_ref)
    pl.semaphore_wait(barrier, 4)

    def q_copy(k, n):
        return remote(send_ref.at[k, :, peers[n]], land_ref.at[k, :, ep], q_s.at[k, n], q_r.at[k, n], (dp, tp, peers[n]))

    def f_copy(k):
        return remote(fwd_ref.at[k], yland_ref.at[k], f_s.at[k], f_r.at[k], other_tp)

    def o_copy(k):
        cols = pl.ds(pl.multiple_of(tp * half + k * cw, 128), cw)
        return remote(out_ref.at[:, cols], out_ref.at[:, cols], o_s.at[k], o_r.at[k], other_tp)

    def main(i, carry):
        @pl.when(i < steps)
        def _():
            slot = lax.rem(i, DOWN_BUFS)
            for c in weight_copies(i, slot):
                c.wait()

            def experts(t, carry2):
                for z in range(4):
                    e = t * 4 + z
                    rows = pl.ds(pl.multiple_of(e * 16, 16), 16)
                    qs_ref[rows, :] = jnp.dot(hid_ref[rows, :], w2buf[slot, e], preferred_element_type=F32).astype(BF16)
                return carry2

            lax.fori_loop(0, local // 4, experts, 0)
            for h in range(2):
                send_ref[i, h] = jnp.dot(p_ref[...], qs_ref[:, h * cw:(h + 1) * cw], preferred_element_type=F32).astype(BF16).reshape(GROUPS, rows_c, cw)
            land_ref[i, :, ep] = send_ref[i, :, ep]

            @pl.when(i + DOWN_BUFS < steps)
            def _():
                for c in weight_copies(i + DOWN_BUFS, slot):
                    c.start()
            for n in range(3):
                q_copy(i, n).start()

        @pl.when((i >= DOWN_LAG) & (i < steps + DOWN_LAG))
        def _():
            k = i - DOWN_LAG
            for n in range(3):
                q_copy(k, n).wait_recv()
            block = land_ref[k, 1 - tp].reshape(GROUPS * rows_c, cw)
            fwd_ref[k] = jnp.dot(s_ref[...], block, preferred_element_type=F32).astype(BF16)
            f_copy(k).start()

        @pl.when(i >= 2 * DOWN_LAG)
        def _():
            k = i - 2 * DOWN_LAG
            mine = land_ref[k, tp].reshape(GROUPS * rows_c, cw)
            mix = jnp.dot(a_ref[2], mine, preferred_element_type=F32)
            mix += jnp.dot(a_ref[1], mine, preferred_element_type=F32)
            mix += jnp.dot(a_ref[0], mine, preferred_element_type=F32)
            f_copy(k).wait_recv()
            theirs = yland_ref[k]
            for z in (2, 1, 0):
                mix += jnp.dot(b_ref[z], theirs, preferred_element_type=F32)
            cols = pl.ds(pl.multiple_of(tp * half + k * cw, 128), cw)
            out_ref[:, cols] = (x_ref[:, cols].astype(F32) + mix).astype(BF16)
            o_copy(k).start()
        return carry

    lax.fori_loop(0, steps + 2 * DOWN_LAG, main, 0)

    def last_waits(k, carry):
        for n in range(3):
            q_copy(k, n).wait_send()
        f_copy(k).wait_send()
        o_copy(k).wait_send()
        cols = pl.ds(pl.multiple_of((1 - tp) * half + k * cw, 128), cw)
        remote(out_ref.at[:, cols], out_ref.at[:, cols], o_s.at[k], o_r.at[k], other_tp).wait_recv()
        return carry

    lax.fori_loop(0, steps, last_waits, 0)


def run_up(x, g, wr, wg, wu, choice_t):
    tok, d_model = x.shape
    local = wg.shape[0]
    cw = d_model // 2 // UP_STEPS
    slots = local * GROUPS * CAP
    vm = pl.BlockSpec(memory_space=pltpu.VMEM)
    hbm = pl.BlockSpec(memory_space=pl.ANY)
    sem = pltpu.SemaphoreType.DMA
    return pl.pallas_call(
        up_kernel,
        out_shape=(
            jax.ShapeDtypeStruct((slots, 128), BF16),
            jax.ShapeDtypeStruct((tok, 2), F32),
            jax.ShapeDtypeStruct((GROUPS, 8, tok), jnp.int32),
            jax.ShapeDtypeStruct((1,), jnp.int32),
        ),
        in_specs=[vm, vm, hbm, hbm, hbm, vm],
        out_specs=(vm, vm, vm, pl.BlockSpec(memory_space=pltpu.SMEM)),
        scratch_shapes=[
            pltpu.VMEM((UP_STEPS, 2, GROUPS, tok, cw), BF16),
            pltpu.VMEM((slots, 2 * cw), BF16),
            pltpu.VMEM((slots, GROUPS * tok), BF16),
            pltpu.VMEM((slots, 256), F32),
            pltpu.VMEM((UP_BUFS, 2, local, 2 * cw, 128), BF16),
            pltpu.VMEM(wr.shape, BF16),
            pltpu.VMEM((tok, 128), F32),
            pltpu.VMEM((GROUPS, 2, tok), jnp.int32),
            sem((UP_BUFS, 4)), sem, sem((3,)), sem((3,)),
        ] + [sem((UP_STEPS,))] * 10,
        compiler_params=pltpu.CompilerParams(collective_id=0, has_side_effects=True, vmem_limit_bytes=VMEM_LIMIT),
        name='up',
    )(x, g, wr, wg, wu, choice_t)


def run_down(tier, hid, x, gate, tab, wd):
    rows_c, rows_n = TIERS[tier]
    tok, d_model = x.shape
    local = wd.shape[0]
    cw = d_model // 2 // DOWN_STEPS
    slots = hid.shape[0]
    vm = pl.BlockSpec(memory_space=pltpu.VMEM)
    hbm = pl.BlockSpec(memory_space=pl.ANY)
    sem = pltpu.SemaphoreType.DMA
    return pl.pallas_call(
        functools.partial(down_kernel, rows_c, rows_n),
        out_shape=jax.ShapeDtypeStruct(x.shape, BF16),
        in_specs=[vm] * 4 + [hbm],
        out_specs=vm,
        scratch_shapes=[
            pltpu.VMEM((DOWN_STEPS, 2, GROUPS, rows_c, cw), BF16),
            pltpu.VMEM((DOWN_STEPS, 2, GROUPS, rows_c, cw), BF16),
            pltpu.VMEM((DOWN_STEPS, rows_n, cw), BF16),
            pltpu.VMEM((DOWN_STEPS, rows_n, cw), BF16),
            pltpu.VMEM((slots, 2 * cw), BF16),
            pltpu.VMEM((DOWN_BUFS, local, 128, 2 * cw), BF16),
            pltpu.VMEM((GROUPS * rows_c, slots), BF16),
            pltpu.VMEM((rows_n, GROUPS * rows_c), BF16),
            pltpu.VMEM((3, tok, GROUPS * rows_c), BF16),
            pltpu.VMEM((3, tok, rows_n), BF16),
            sem((DOWN_BUFS, 2)), sem((DOWN_STEPS, 3)), sem((DOWN_STEPS, 3)),
            sem((DOWN_STEPS,)), sem((DOWN_STEPS,)), sem((DOWN_STEPS,)), sem((DOWN_STEPS,)),
        ],
        compiler_params=pltpu.CompilerParams(collective_id=1 + tier, has_side_effects=True, vmem_limit_bytes=DOWN_VMEM[tier]),
        name='down%d' % rows_c,
    )(hid, x, gate, tab, wd)


def solution(mesh):
    row_spec = P(('dp', 'ep'), None)

    def device_step(resid_in, norm_scale, w_router, w_gate, w_up, w_down, choice):
        hid, gate, tab, flag = run_up(resid_in, norm_scale, w_router, w_gate, w_up, choice.T)
        return lax.switch(flag[0], [functools.partial(run_down, t) for t in range(len(TIERS))], hid, resid_in, gate, tab, w_down)

    return jax.shard_map(device_step, mesh=mesh, in_specs=(row_spec, P(None), P(None, None), P('ep', None, 'tp'), P('ep', None, 'tp'), P('ep', 'tp', None), row_spec), out_specs=row_spec, check_vma=False)
```

```python
import functools

import jax
import jax.numpy as jnp
from jax import lax
from jax.experimental import pallas as pl
from jax.experimental.pallas import tpu as pltpu
from jax.sharding import PartitionSpec as P

NORM_EPS = 1e-5
MESH = pl.DeviceIdType.MESH
F32 = jnp.float32
BF16 = jnp.bfloat16
CAP = 4
GROUPS = 4
UP_STEPS = 14
UP_BUFS = 6
EARLY = 18
LATE_BUFS = 6
UP_LAG = 3
DOWN_STEPS = 14
DOWN_BUFS = 6
DOWN_LAG = 2
TIERS = ((64, 176), (128, 256))
DOWN_VMEM = (46 * 1024 * 1024, 56 * 1024 * 1024)
VMEM_LIMIT = 48 * 1024 * 1024


def remote(src, dst, send_sem, recv_sem, device):
    return pltpu.make_async_remote_copy(src_ref=src, dst_ref=dst, send_sem=send_sem, recv_sem=recv_sem, device_id=device, device_id_type=MESH)


def place():
    dp, tp, ep = lax.axis_index('dp'), lax.axis_index('tp'), lax.axis_index('ep')
    return dp, tp, ep, ep // 2, ep % 2


def column(row):
    n = row.shape[1]
    eye = lax.broadcasted_iota(jnp.int32, (n, n), 0) == lax.broadcasted_iota(jnp.int32, (n, n), 1)
    return jnp.sum(jnp.where(eye, row.astype(F32), 0.0), axis=1, keepdims=True).astype(jnp.int32)


def up_kernel(x_ref, g_ref, wr_ref, wg_hbm, wu_hbm, choice_ref, hid_ref, late_ref, gate_ref, tab_ref, act_ref, flag_ref,
              u_ref, xs_ref, pick_ref, acc_ref, wbuf, logit_ref, ch_ref,
              w_sem, c_s, c_r, own_s, own_r, x_s, x_r, y_s, y_r, dx_s, dx_r, dy_s, dy_r):
    dp, tp, ep, cx, core = place()
    tok, d_model = x_ref.shape
    half = d_model // 2
    steps = UP_STEPS
    cw = half // steps
    twin = (dp, tp, cx * 2 + (1 - core))
    across = (dp, tp, (1 - cx) * 2 + core)
    far_twin = (dp, tp, (1 - cx) * 2 + (1 - core))
    other_tp = (dp, 1 - tp, ep)
    far = (1 - cx) * 2 + core

    barrier = pltpu.get_barrier_semaphore()
    for peer in (twin, across, far_twin, other_tp):
        pl.semaphore_signal(barrier, inc=1, device_id=peer, device_id_type=MESH)

    def weight_copies(step, slot):
        out = []
        for h in range(2):
            rows = pl.ds(pl.multiple_of(h * half + step * cw, cw), cw)
            for m, w in enumerate((wg_hbm, wu_hbm)):
                out.append(pltpu.make_async_copy(w.at[0:EARLY, rows, :], wbuf.at[slot, :, h * cw:(h + 1) * cw, m * 128:(m + 1) * 128], w_sem.at[slot, h * 2 + m]))
        return out

    for b in range(UP_BUFS):
        for c in weight_copies(b, b):
            c.start()

    scale = g_ref[...].astype(F32).reshape(1, d_model)

    def norm_rows(r, carry):
        rows = pl.ds(pl.multiple_of(r * 16, 16), 16)
        xb = x_ref[rows, :].astype(F32)
        cen = xb - jnp.mean(xb, axis=-1, keepdims=True)
        var = jnp.mean(cen * cen, axis=-1, keepdims=True)
        u = (cen * lax.rsqrt(var + NORM_EPS) * scale).astype(BF16)
        for j in range(steps):
            for h in range(2):
                u_ref[j, h, ep, rows, :] = u[:, h * half + j * cw:h * half + (j + 1) * cw]
        return carry

    lax.fori_loop(0, tok // 16, norm_rows, 0)
    pl.semaphore_wait(barrier, 4)

    def choice_copy(n):
        peer = (across, far_twin, twin)[n]
        return remote(choice_ref, ch_ref.at[ep], c_s.at[n], c_r.at[n], peer)

    for n in range(3):
        choice_copy(n).start()

    def own_copy(j):
        return remote(u_ref.at[j, :, ep], u_ref.at[j, :, ep], own_s.at[j], own_r.at[j], twin)

    def x_copy(j):
        return remote(u_ref.at[j, tp, ep], u_ref.at[j, tp, ep], x_s.at[j], x_r.at[j], across)

    def y_copy(j):
        return remote(u_ref.at[j, tp, far], u_ref.at[j, tp, far], y_s.at[j], y_r.at[j], other_tp)

    def dx_copy(j):
        return remote(u_ref.at[j, tp, far], u_ref.at[j, tp, far], dx_s.at[j], dx_r.at[j], twin)

    def dy_copy(j):
        return remote(u_ref.at[j, 1 - tp, far], u_ref.at[j, 1 - tp, far], dy_s.at[j], dy_r.at[j], twin)

    def first_sends(j, carry):
        x_copy(j).start()
        own_copy(j).start()
        return carry

    lax.fori_loop(0, steps, first_sends, 0)
    ch_ref[ep] = choice_ref[...]
    acc_ref[...] = jnp.zeros_like(acc_ref)
    logit_ref[...] = jnp.zeros_like(logit_ref)
    for n in range(3):
        choice_copy(n).wait_recv()

    slots = pick_ref.shape[0]
    upper = jnp.where(lax.broadcasted_iota(jnp.int32, (tok, tok), 0) < lax.broadcasted_iota(jnp.int32, (tok, tok), 1), 1.0, 0.0).astype(BF16)
    ids = lax.broadcasted_iota(jnp.int32, (tok, tok), 0)
    lane16 = lax.broadcasted_iota(jnp.int32, (16, tok), 0)
    slot_iota = lax.broadcasted_iota(jnp.int32, (slots, tok), 0)
    most = jnp.zeros((16, 1), F32)
    load = jnp.zeros((tok, 1), F32)
    for g in range(GROUPS):
        c = [ch_ref[g, j:j + 1, :] for j in range(2)]
        hot = [jnp.where(ids == c[j], 1.0, 0.0) for j in range(2)]
        earlier = jnp.dot((hot[0] + hot[1]).astype(BF16), upper, preferred_element_type=F32)
        pos = [jnp.sum(earlier * hot[j], axis=0, keepdims=True).astype(jnp.int32) for j in range(2)]
        kept = [pos[j] < CAP for j in range(2)]
        keptf = [jnp.where(kept[j], 1.0, 0.0) for j in range(2)]
        owner = [c[j] // 32 for j in range(2)]
        mine = [jnp.where(lane16 == owner[j], keptf[j], 0.0) for j in range(2)]
        every = [jnp.where(lane16 == GROUPS, keptf[j], 0.0) for j in range(2)]
        tally = mine[0] + mine[1] + every[0] + every[1]
        before = jnp.dot(tally.astype(BF16), upper, preferred_element_type=F32)
        load = load + jnp.sum(hot[0] + hot[1], axis=1, keepdims=True)
        most = jnp.maximum(most, jnp.sum(tally, axis=1, keepdims=True))
        rank = [jnp.sum(before * mine[j], axis=0, keepdims=True) for j in range(2)]
        rank[1] = rank[1] + jnp.where(owner[0] == owner[1], keptf[0], 0.0)
        nrank = [before[GROUPS:GROUPS + 1, :], before[GROUPS:GROUPS + 1, :] + keptf[0]]
        for j in range(2):
            slot = jnp.where(kept[j] & (owner[j] == ep), (c[j] - ep * 32) * 16 + g * CAP + pos[j], -1)
            tab_ref[g, j:j + 1, :] = slot
            tab_ref[g, 2 + j:3 + j, :] = jnp.where(kept[j], owner[j] * 128 + rank[j].astype(jnp.int32), -1)
            tab_ref[g, 4 + j:5 + j, :] = jnp.where(kept[j], nrank[j].astype(jnp.int32), -1)
        tab_ref[g, 6:8, :] = jnp.zeros((2, tok), jnp.int32)
        pick_ref[:, g * tok:(g + 1) * tok] = jnp.where((slot_iota == tab_ref[g, 0:1, :]) | (slot_iota == tab_ref[g, 1:2, :]), 1.0, 0.0).astype(BF16)
    sub16 = lax.broadcasted_iota(jnp.int32, (16, 1), 0)
    fits = [jnp.where(sub16 < GROUPS, rows_c, jnp.where(sub16 == GROUPS, rows_n, 0)).astype(F32) for rows_c, rows_n in TIERS[:-1]]
    level = jnp.zeros((1, 1), F32)
    for f in fits:
        level = level + jnp.max(jnp.where(most > f, 1.0, 0.0), axis=0, keepdims=True)
    diag = ids == lax.broadcasted_iota(jnp.int32, (tok, tok), 1)
    act_ref[...] = jnp.sum(jnp.where(diag, load, 0.0), axis=0, keepdims=True).astype(jnp.int32)
    flag_ref[0] = jnp.max(level).astype(jnp.int32)

    def main(i, carry):
        @pl.when(i < steps)
        def _():
            x_copy(i).wait_recv()
            y_copy(i).start()
            dx_copy(i).start()

        @pl.when((i >= UP_LAG) & (i < steps + UP_LAG))
        def _():
            j = i - UP_LAG
            y_copy(j).wait_recv()
            dy_copy(j).start()

        @pl.when(i >= UP_LAG + 1)
        def _():
            j = i - UP_LAG - 1
            slot = lax.rem(j, UP_BUFS)
            for h in range(2):
                kr = pl.ds(pl.multiple_of(h * half + j * cw, cw), cw)
                logit_ref[...] += jnp.dot(u_ref[j, h, ep], wr_ref[kr, :], preferred_element_type=F32)
            own_copy(j).wait_recv()
            dx_copy(j).wait_recv()
            dy_copy(j).wait_recv()
            for h in range(2):
                block = u_ref[j, h].reshape(GROUPS * tok, cw)
                rows_u = jnp.dot(pick_ref[...], block, preferred_element_type=F32).astype(BF16)
                xs_ref[:, h * cw:(h + 1) * cw] = rows_u[0:EARLY * 16]
                late_ref[:, pl.ds(pl.multiple_of(h * half + j * cw, cw), cw)] = rows_u[EARLY * 16:]
            for c in weight_copies(j, slot):
                c.wait()

            def experts(t, carry2):
                for z in range(3):
                    e = t * 3 + z
                    rows = pl.ds(pl.multiple_of(e * 16, 16), 16)
                    acc_ref[rows, :] += jnp.dot(xs_ref[rows, :], wbuf[slot, e], preferred_element_type=F32)
                return carry2

            lax.fori_loop(0, EARLY // 3, experts, 0)

            @pl.when(j + UP_BUFS < steps)
            def _():
                for c in weight_copies(j + UP_BUFS, slot):
                    c.start()
        return carry

    lax.fori_loop(0, steps + UP_LAG + 1, main, 0)

    gate_act = acc_ref[:, :128]
    hid_ref[...] = (gate_act * jax.nn.sigmoid(gate_act) * acc_ref[:, 128:]).astype(BF16)
    logits = logit_ref[...]
    ex = jnp.exp(logits - jnp.max(logits, axis=-1, keepdims=True))
    probs = ex / jnp.sum(ex, axis=-1, keepdims=True)
    lanes = lax.broadcasted_iota(jnp.int32, probs.shape, 1)
    picked = [jnp.sum(jnp.where(column(ch_ref[ep, j:j + 1, :]) == lanes, probs, 0.0), axis=-1, keepdims=True) for j in range(2)]
    for j in range(2):
        gate_ref[:, j:j + 1] = picked[j] / (picked[0] + picked[1])

    def last_waits(j, carry):
        x_copy(j).wait_send()
        own_copy(j).wait_send()
        y_copy(j).wait_send()
        dx_copy(j).wait_send()
        dy_copy(j).wait_send()
        return carry

    lax.fori_loop(0, steps, last_waits, 0)
    for n in range(3):
        choice_copy(n).wait_send()


def late_kernel(act_ref, late_ref, wg_hbm, wu_hbm, hid_ref, list_ref, wbuf, w_sem):
    ep = lax.axis_index('ep')
    local = wg_hbm.shape[0]
    hid_ref[...] = jnp.zeros_like(hid_ref)

    def scan(e, n):
        busy = act_ref[0, ep * local + e] > 0

        @pl.when(busy)
        def _():
            list_ref[n] = e
        return n + busy.astype(jnp.int32)

    count = lax.fori_loop(EARLY, local, scan, 0)

    def weight_copies(n):
        slot = lax.rem(n, LATE_BUFS)
        e = list_ref[n]
        return [pltpu.make_async_copy(w.at[e], wbuf.at[slot, :, m * 128:(m + 1) * 128], w_sem.at[slot, m]) for m, w in enumerate((wg_hbm, wu_hbm))]

    def start(n):
        @pl.when(n < count)
        def _():
            for c in weight_copies(n):
                c.start()

    for n in range(LATE_BUFS):
        start(n)

    def step(n, carry):
        for c in weight_copies(n):
            c.wait()
        rows = pl.ds(pl.multiple_of((list_ref[n] - EARLY) * 16, 16), 16)
        both = jnp.dot(late_ref[rows, :], wbuf[lax.rem(n, LATE_BUFS)], preferred_element_type=F32)
        gate_act = both[:, :128]
        hid_ref[rows, :] = (gate_act * jax.nn.sigmoid(gate_act) * both[:, 128:]).astype(BF16)
        start(n + LATE_BUFS)
        return carry

    lax.fori_loop(0, count, step, 0)


def down_kernel(rows_c, rows_n, early_ref, late_ref, x_ref, gate_ref, tab_ref, wd_hbm, out_ref,
                hid_ref, send_ref, land_ref, fwd_ref, yland_ref, qs_ref, w2buf, p_ref, s_ref, a_ref, b_ref,
                w_sem, q_s, q_r, f_s, f_r, o_s, o_r):
    dp, tp, ep, cx, core = place()
    local = wd_hbm.shape[0]
    tok, d_model = x_ref.shape
    half = d_model // 2
    steps = DOWN_STEPS
    cw = half // steps
    peers = [(1 - cx) * 2 + core, (1 - cx) * 2 + (1 - core), cx * 2 + (1 - core)]
    other_tp = (dp, 1 - tp, ep)

    barrier = pltpu.get_barrier_semaphore()
    for g in peers:
        pl.semaphore_signal(barrier, inc=1, device_id=(dp, tp, g), device_id_type=MESH)
    pl.semaphore_signal(barrier, inc=1, device_id=other_tp, device_id_type=MESH)

    def weight_copies(step, slot):
        out = []
        for h in range(2):
            cols = pl.ds(pl.multiple_of(h * half + step * cw, 128), cw)
            out.append(pltpu.make_async_copy(wd_hbm.at[:, :, cols], w2buf.at[slot, :, :, h * cw:(h + 1) * cw], w_sem.at[slot, h]))
        return out

    for b in range(DOWN_BUFS):
        for c in weight_copies(b, b):
            c.start()

    hid_ref[0:EARLY * 16, :] = early_ref[...]
    hid_ref[EARLY * 16:, :] = late_ref[...]
    all_rows = GROUPS * rows_c
    slots = qs_ref.shape[0]
    gap = 128 - rows_c
    slot_iota = lax.broadcasted_iota(jnp.int32, (slots, tok), 0)
    c_iota = lax.broadcasted_iota(jnp.int32, (rows_c, tok), 0)

    def key_of(r):
        for n in range(1, GROUPS):
            r = r + jnp.where(r >= n * rows_c + (n - 1) * gap, gap, 0)
        return r

    def onehot(rows, values):
        return jnp.where(rows == values, 1.0, 0.0).astype(BF16)

    def times_t(a, b):
        return lax.dot_general(a, b, (((1,), (1,)), ((), ())), preferred_element_type=F32)

    for g in range(GROUPS):
        total = jnp.zeros((rows_c, slots), F32)
        for j in range(2):
            total += times_t(onehot(c_iota + ep * 128, tab_ref[g, 2 + j:3 + j, :]), onehot(slot_iota, tab_ref[g, j:j + 1, :]))
        p_ref[g * rows_c:(g + 1) * rows_c, :] = total.astype(BF16)
    key_iota = key_of(lax.broadcasted_iota(jnp.int32, (all_rows, tok), 0))
    n_iota = lax.broadcasted_iota(jnp.int32, (rows_n, tok), 0)
    my_key = [tab_ref[ep, 2 + j:3 + j, :] for j in range(2)]
    my_n = [tab_ref[ep, 4 + j:5 + j, :] for j in range(2)]
    total = jnp.zeros((rows_n, all_rows), F32)
    for j in range(2):
        total += times_t(onehot(n_iota, my_n[j]), onehot(key_iota, my_key[j]))
    s_ref[...] = total.astype(BF16)

    def split_gates(keys, pos, dst):
        mat = jnp.where(pos[0] == keys, gate_ref[:, 0:1], 0.0) + jnp.where(pos[1] == keys, gate_ref[:, 1:2], 0.0)
        for z in range(3):
            part = mat.astype(BF16)
            dst[z] = part
            mat = mat - part.astype(F32)

    split_gates(key_of(lax.broadcasted_iota(jnp.int32, (tok, all_rows), 1)), [column(v) for v in my_key], a_ref)
    split_gates(lax.broadcasted_iota(jnp.int32, (tok, rows_n), 1), [column(v) for v in my_n], b_ref)
    pl.semaphore_wait(barrier, 4)

    def q_copy(k, n):
        return remote(send_ref.at[k, :, peers[n]], land_ref.at[k, :, ep], q_s.at[k, n], q_r.at[k, n], (dp, tp, peers[n]))

    def f_copy(k):
        return remote(fwd_ref.at[k], yland_ref.at[k], f_s.at[k], f_r.at[k], other_tp)

    def o_copy(k):
        cols = pl.ds(pl.multiple_of(tp * half + k * cw, 128), cw)
        return remote(out_ref.at[:, cols], out_ref.at[:, cols], o_s.at[k], o_r.at[k], other_tp)

    def main(i, carry):
        @pl.when(i < steps)
        def _():
            slot = lax.rem(i, DOWN_BUFS)
            for c in weight_copies(i, slot):
                c.wait()

            def experts(t, carry2):
                for z in range(4):
                    e = t * 4 + z
                    rows = pl.ds(pl.multiple_of(e * 16, 16), 16)
                    qs_ref[rows, :] = jnp.dot(hid_ref[rows, :], w2buf[slot, e], preferred_element_type=F32).astype(BF16)
                return carry2

            lax.fori_loop(0, local // 4, experts, 0)
            for h in range(2):
                send_ref[i, h] = jnp.dot(p_ref[...], qs_ref[:, h * cw:(h + 1) * cw], preferred_element_type=F32).astype(BF16).reshape(GROUPS, rows_c, cw)
            land_ref[i, :, ep] = send_ref[i, :, ep]

            @pl.when(i + DOWN_BUFS < steps)
            def _():
                for c in weight_copies(i + DOWN_BUFS, slot):
                    c.start()
            for n in range(3):
                q_copy(i, n).start()

        @pl.when((i >= DOWN_LAG) & (i < steps + DOWN_LAG))
        def _():
            k = i - DOWN_LAG
            for n in range(3):
                q_copy(k, n).wait_recv()
            block = land_ref[k, 1 - tp].reshape(GROUPS * rows_c, cw)
            fwd_ref[k] = jnp.dot(s_ref[...], block, preferred_element_type=F32).astype(BF16)
            f_copy(k).start()

        @pl.when(i >= 2 * DOWN_LAG)
        def _():
            k = i - 2 * DOWN_LAG
            mine = land_ref[k, tp].reshape(GROUPS * rows_c, cw)
            mix = jnp.dot(a_ref[2], mine, preferred_element_type=F32)
            mix += jnp.dot(a_ref[1], mine, preferred_element_type=F32)
            mix += jnp.dot(a_ref[0], mine, preferred_element_type=F32)
            f_copy(k).wait_recv()
            theirs = yland_ref[k]
            for z in (2, 1, 0):
                mix += jnp.dot(b_ref[z], theirs, preferred_element_type=F32)
            cols = pl.ds(pl.multiple_of(tp * half + k * cw, 128), cw)
            out_ref[:, cols] = (x_ref[:, cols].astype(F32) + mix).astype(BF16)
            o_copy(k).start()
        return carry

    lax.fori_loop(0, steps + 2 * DOWN_LAG, main, 0)

    def last_waits(k, carry):
        for n in range(3):
            q_copy(k, n).wait_send()
        f_copy(k).wait_send()
        o_copy(k).wait_send()
        cols = pl.ds(pl.multiple_of((1 - tp) * half + k * cw, 128), cw)
        remote(out_ref.at[:, cols], out_ref.at[:, cols], o_s.at[k], o_r.at[k], other_tp).wait_recv()
        return carry

    lax.fori_loop(0, steps, last_waits, 0)


def run_up(x, g, wr, wg, wu, choice_t):
    tok, d_model = x.shape
    local = wg.shape[0]
    cw = d_model // 2 // UP_STEPS
    slots = local * GROUPS * CAP
    vm = pl.BlockSpec(memory_space=pltpu.VMEM)
    hbm = pl.BlockSpec(memory_space=pltpu.HBM)
    sem = pltpu.SemaphoreType.DMA
    return pl.pallas_call(
        up_kernel,
        out_shape=(
            jax.ShapeDtypeStruct((EARLY * 16, 128), BF16),
            jax.ShapeDtypeStruct((slots - EARLY * 16, d_model), BF16),
            jax.ShapeDtypeStruct((tok, 2), F32),
            jax.ShapeDtypeStruct((GROUPS, 8, tok), jnp.int32),
            jax.ShapeDtypeStruct((1, 128), jnp.int32),
            jax.ShapeDtypeStruct((1,), jnp.int32),
        ),
        in_specs=[vm, vm, vm, hbm, hbm, vm],
        out_specs=(vm, vm, vm, vm, vm, pl.BlockSpec(memory_space=pltpu.SMEM)),
        scratch_shapes=[
            pltpu.VMEM((UP_STEPS, 2, GROUPS, tok, cw), BF16),
            pltpu.VMEM((EARLY * 16, 2 * cw), BF16),
            pltpu.VMEM((slots, GROUPS * tok), BF16),
            pltpu.VMEM((EARLY * 16, 256), F32),
            pltpu.VMEM((UP_BUFS, EARLY, 2 * cw, 256), BF16),
            pltpu.VMEM((tok, 128), F32),
            pltpu.VMEM((GROUPS, 2, tok), jnp.int32),
            sem((UP_BUFS, 4)), sem((3,)), sem((3,)),
        ] + [sem((UP_STEPS,))] * 10,
        compiler_params=pltpu.CompilerParams(collective_id=0, has_side_effects=True, vmem_limit_bytes=VMEM_LIMIT),
        name='up',
    )(x, g, wr, wg, wu, choice_t)


def run_late(act, late, wg, wu):
    d_model = late.shape[1]
    vm = pl.BlockSpec(memory_space=pltpu.VMEM)
    hbm = pl.BlockSpec(memory_space=pltpu.HBM)
    return pl.pallas_call(
        late_kernel,
        out_shape=jax.ShapeDtypeStruct((late.shape[0], 128), BF16),
        in_specs=[pl.BlockSpec(memory_space=pltpu.SMEM), vm, hbm, hbm],
        out_specs=vm,
        scratch_shapes=[
            pltpu.SMEM((64,), jnp.int32),
            pltpu.VMEM((LATE_BUFS, d_model, 256), BF16),
            pltpu.SemaphoreType.DMA((LATE_BUFS, 2)),
        ],
        compiler_params=pltpu.CompilerParams(vmem_limit_bytes=40 * 1024 * 1024),
        name='late',
    )(act, late, wg, wu)


def run_down(tier, early, late, x, gate, tab, wd):
    rows_c, rows_n = TIERS[tier]
    tok, d_model = x.shape
    local = wd.shape[0]
    cw = d_model // 2 // DOWN_STEPS
    slots = local * GROUPS * CAP
    vm = pl.BlockSpec(memory_space=pltpu.VMEM)
    hbm = pl.BlockSpec(memory_space=pltpu.HBM)
    sem = pltpu.SemaphoreType.DMA
    return pl.pallas_call(
        functools.partial(down_kernel, rows_c, rows_n),
        out_shape=jax.ShapeDtypeStruct(x.shape, BF16),
        in_specs=[vm] * 5 + [hbm],
        out_specs=vm,
        scratch_shapes=[
            pltpu.VMEM((slots, 128), BF16),
            pltpu.VMEM((DOWN_STEPS, 2, GROUPS, rows_c, cw), BF16),
            pltpu.VMEM((DOWN_STEPS, 2, GROUPS, rows_c, cw), BF16),
            pltpu.VMEM((DOWN_STEPS, rows_n, cw), BF16),
            pltpu.VMEM((DOWN_STEPS, rows_n, cw), BF16),
            pltpu.VMEM((slots, 2 * cw), BF16),
            pltpu.VMEM((DOWN_BUFS, local, 128, 2 * cw), BF16),
            pltpu.VMEM((GROUPS * rows_c, slots), BF16),
            pltpu.VMEM((rows_n, GROUPS * rows_c), BF16),
            pltpu.VMEM((3, tok, GROUPS * rows_c), BF16),
            pltpu.VMEM((3, tok, rows_n), BF16),
            sem((DOWN_BUFS, 2)), sem((DOWN_STEPS, 3)), sem((DOWN_STEPS, 3)),
            sem((DOWN_STEPS,)), sem((DOWN_STEPS,)), sem((DOWN_STEPS,)), sem((DOWN_STEPS,)),
        ],
        compiler_params=pltpu.CompilerParams(collective_id=1 + tier, has_side_effects=True, vmem_limit_bytes=DOWN_VMEM[tier]),
        name='down%d' % rows_c,
    )(early, late, x, gate, tab, wd)


def solution(mesh):
    row_spec = P(('dp', 'ep'), None)

    def device_step(resid_in, norm_scale, w_router, w_gate, w_up, w_down, choice):
        early, rows_late, gate, tab, act, flag = run_up(resid_in, norm_scale, w_router, w_gate, w_up, choice.T)
        late = run_late(act, rows_late, w_gate, w_up)
        return lax.switch(flag[0], [functools.partial(run_down, t) for t in range(len(TIERS))], early, late, resid_in, gate, tab, w_down)

    return jax.shard_map(device_step, mesh=mesh, in_specs=(row_spec, P(None), P(None, None), P('ep', None, 'tp'), P('ep', None, 'tp'), P('ep', 'tp', None), row_spec), out_specs=row_spec, check_vma=False)
```

```python
import functools

import jax
import jax.numpy as jnp
from jax import lax
from jax.experimental import pallas as pl
from jax.experimental.pallas import tpu as pltpu
from jax.sharding import PartitionSpec as P

NORM_EPS = 1e-5
MESH = pl.DeviceIdType.MESH
F32 = jnp.float32
BF16 = jnp.bfloat16
CAP = 4
GROUPS = 4
UP_STEPS = 14
UP_BUFS = 6
EARLY = 18
AHEAD = 3
LATE_BUFS = 6
UP_LAG = 3
DOWN_STEPS = 14
DOWN_BUFS = 4
DOWN_LAG = 2
TIERS = ((64, 176), (128, 256))
DOWN_VMEM = (46 * 1024 * 1024, 56 * 1024 * 1024)
VMEM_LIMIT = 48 * 1024 * 1024


def remote(src, dst, send_sem, recv_sem, device):
    return pltpu.make_async_remote_copy(src_ref=src, dst_ref=dst, send_sem=send_sem, recv_sem=recv_sem, device_id=device, device_id_type=MESH)


def place():
    dp, tp, ep = lax.axis_index('dp'), lax.axis_index('tp'), lax.axis_index('ep')
    return dp, tp, ep, ep // 2, ep % 2


def column(row):
    n = row.shape[1]
    eye = lax.broadcasted_iota(jnp.int32, (n, n), 0) == lax.broadcasted_iota(jnp.int32, (n, n), 1)
    return jnp.sum(jnp.where(eye, row.astype(F32), 0.0), axis=1, keepdims=True).astype(jnp.int32)


def up_kernel(x_ref, g_ref, wr_ref, wg_hbm, wu_hbm, choice_ref, hid_ref, late_ref, gate_ref, tab_ref, act_ref, flag_ref,
              u_ref, xs_ref, pick_ref, acc_ref, wbuf, logit_ref, ch_ref,
              w_sem, c_s, c_r, own_s, own_r, x_s, x_r, y_s, y_r, dx_s, dx_r, dy_s, dy_r):
    dp, tp, ep, cx, core = place()
    tok, d_model = x_ref.shape
    half = d_model // 2
    steps = UP_STEPS
    cw = half // steps
    twin = (dp, tp, cx * 2 + (1 - core))
    across = (dp, tp, (1 - cx) * 2 + core)
    far_twin = (dp, tp, (1 - cx) * 2 + (1 - core))
    other_tp = (dp, 1 - tp, ep)
    far = (1 - cx) * 2 + core

    barrier = pltpu.get_barrier_semaphore()
    for peer in (twin, across, far_twin, other_tp):
        pl.semaphore_signal(barrier, inc=1, device_id=peer, device_id_type=MESH)

    def weight_copies(step, slot):
        out = []
        for h in range(2):
            rows = pl.ds(pl.multiple_of(h * half + step * cw, cw), cw)
            for m, w in enumerate((wg_hbm, wu_hbm)):
                out.append(pltpu.make_async_copy(w.at[0:EARLY, rows, :], wbuf.at[slot, :, h * cw:(h + 1) * cw, m * 128:(m + 1) * 128], w_sem.at[slot, h * 2 + m]))
        return out

    for b in range(2):
        for c in weight_copies(b, b):
            c.start()

    scale = g_ref[...].astype(F32).reshape(1, d_model)

    def norm_rows(r, carry):
        rows = pl.ds(pl.multiple_of(r * 16, 16), 16)
        xb = x_ref[rows, :].astype(F32)
        cen = xb - jnp.mean(xb, axis=-1, keepdims=True)
        var = jnp.mean(cen * cen, axis=-1, keepdims=True)
        u = (cen * lax.rsqrt(var + NORM_EPS) * scale).astype(BF16)
        for j in range(steps):
            for h in range(2):
                u_ref[j, h, ep, rows, :] = u[:, h * half + j * cw:h * half + (j + 1) * cw]
        return carry

    lax.fori_loop(0, tok // 16, norm_rows, 0)
    pl.semaphore_wait(barrier, 4)

    def choice_copy(n):
        peer = (across, far_twin, twin)[n]
        return remote(choice_ref, ch_ref.at[ep], c_s.at[n], c_r.at[n], peer)

    for n in range(3):
        choice_copy(n).start()

    def own_copy(j):
        return remote(u_ref.at[j, :, ep], u_ref.at[j, :, ep], own_s.at[j], own_r.at[j], twin)

    def x_copy(j):
        return remote(u_ref.at[j, tp, ep], u_ref.at[j, tp, ep], x_s.at[j], x_r.at[j], across)

    def y_copy(j):
        return remote(u_ref.at[j, tp, far], u_ref.at[j, tp, far], y_s.at[j], y_r.at[j], other_tp)

    def dx_copy(j):
        return remote(u_ref.at[j, tp, far], u_ref.at[j, tp, far], dx_s.at[j], dx_r.at[j], twin)

    def dy_copy(j):
        return remote(u_ref.at[j, 1 - tp, far], u_ref.at[j, 1 - tp, far], dy_s.at[j], dy_r.at[j], twin)

    def first_sends(j, carry):
        x_copy(j).start()
        own_copy(j).start()
        return carry

    lax.fori_loop(0, AHEAD, first_sends, 0)
    for b in range(2, UP_BUFS):
        for c in weight_copies(b, b):
            c.start()
    ch_ref[ep] = choice_ref[...]
    acc_ref[...] = jnp.zeros_like(acc_ref)
    logit_ref[...] = jnp.zeros_like(logit_ref)
    for n in range(3):
        choice_copy(n).wait_recv()

    slots = pick_ref.shape[0]
    upper = jnp.where(lax.broadcasted_iota(jnp.int32, (tok, tok), 0) < lax.broadcasted_iota(jnp.int32, (tok, tok), 1), 1.0, 0.0).astype(BF16)
    ids = lax.broadcasted_iota(jnp.int32, (tok, tok), 0)
    lane16 = lax.broadcasted_iota(jnp.int32, (16, tok), 0)
    slot_iota = lax.broadcasted_iota(jnp.int32, (slots, tok), 0)
    most = jnp.zeros((16, 1), F32)
    load = jnp.zeros((tok, 1), F32)
    for g in range(GROUPS):
        c = [ch_ref[g, j:j + 1, :] for j in range(2)]
        hot = [jnp.where(ids == c[j], 1.0, 0.0) for j in range(2)]
        earlier = jnp.dot((hot[0] + hot[1]).astype(BF16), upper, preferred_element_type=F32)
        pos = [jnp.sum(earlier * hot[j], axis=0, keepdims=True).astype(jnp.int32) for j in range(2)]
        kept = [pos[j] < CAP for j in range(2)]
        keptf = [jnp.where(kept[j], 1.0, 0.0) for j in range(2)]
        owner = [c[j] // 32 for j in range(2)]
        mine = [jnp.where(lane16 == owner[j], keptf[j], 0.0) for j in range(2)]
        every = [jnp.where(lane16 == GROUPS, keptf[j], 0.0) for j in range(2)]
        tally = mine[0] + mine[1] + every[0] + every[1]
        before = jnp.dot(tally.astype(BF16), upper, preferred_element_type=F32)
        load = load + jnp.sum(hot[0] + hot[1], axis=1, keepdims=True)
        most = jnp.maximum(most, jnp.sum(tally, axis=1, keepdims=True))
        rank = [jnp.sum(before * mine[j], axis=0, keepdims=True) for j in range(2)]
        rank[1] = rank[1] + jnp.where(owner[0] == owner[1], keptf[0], 0.0)
        nrank = [before[GROUPS:GROUPS + 1, :], before[GROUPS:GROUPS + 1, :] + keptf[0]]
        for j in range(2):
            slot = jnp.where(kept[j] & (owner[j] == ep), (c[j] - ep * 32) * 16 + g * CAP + pos[j], -1)
            tab_ref[g, j:j + 1, :] = slot
            tab_ref[g, 2 + j:3 + j, :] = jnp.where(kept[j], owner[j] * 128 + rank[j].astype(jnp.int32), -1)
            tab_ref[g, 4 + j:5 + j, :] = jnp.where(kept[j], nrank[j].astype(jnp.int32), -1)
        tab_ref[g, 6:8, :] = jnp.zeros((2, tok), jnp.int32)
        pick_ref[:, g * tok:(g + 1) * tok] = jnp.where((slot_iota == tab_ref[g, 0:1, :]) | (slot_iota == tab_ref[g, 1:2, :]), 1.0, 0.0).astype(BF16)
    sub16 = lax.broadcasted_iota(jnp.int32, (16, 1), 0)
    fits = [jnp.where(sub16 < GROUPS, rows_c, jnp.where(sub16 == GROUPS, rows_n, 0)).astype(F32) for rows_c, rows_n in TIERS[:-1]]
    level = jnp.zeros((1, 1), F32)
    for f in fits:
        level = level + jnp.max(jnp.where(most > f, 1.0, 0.0), axis=0, keepdims=True)
    diag = ids == lax.broadcasted_iota(jnp.int32, (tok, tok), 1)
    act_ref[...] = jnp.sum(jnp.where(diag, load, 0.0), axis=0, keepdims=True).astype(jnp.int32)
    flag_ref[0] = jnp.max(level).astype(jnp.int32)

    def main(i, carry):
        @pl.when(i < steps)
        def _():
            x_copy(i).wait_recv()
            y_copy(i).start()
            dx_copy(i).start()

        @pl.when(i + AHEAD < steps)
        def _():
            first_sends(i + AHEAD, 0)

        @pl.when((i >= UP_LAG) & (i < steps + UP_LAG))
        def _():
            j = i - UP_LAG
            y_copy(j).wait_recv()
            dy_copy(j).start()

        @pl.when(i >= UP_LAG + 1)
        def _():
            j = i - UP_LAG - 1
            slot = lax.rem(j, UP_BUFS)
            for h in range(2):
                kr = pl.ds(pl.multiple_of(h * half + j * cw, cw), cw)
                logit_ref[...] += jnp.dot(u_ref[j, h, ep], wr_ref[kr, :], preferred_element_type=F32)
            own_copy(j).wait_recv()
            dx_copy(j).wait_recv()
            dy_copy(j).wait_recv()
            for h in range(2):
                block = u_ref[j, h].reshape(GROUPS * tok, cw)
                rows_u = jnp.dot(pick_ref[...], block, preferred_element_type=F32).astype(BF16)
                xs_ref[:, h * cw:(h + 1) * cw] = rows_u[0:EARLY * 16]
                late_ref[:, pl.ds(pl.multiple_of(h * half + j * cw, cw), cw)] = rows_u[EARLY * 16:]
            for c in weight_copies(j, slot):
                c.wait()

            def experts(t, carry2):
                for z in range(3):
                    e = t * 3 + z
                    rows = pl.ds(pl.multiple_of(e * 16, 16), 16)
                    acc_ref[rows, :] += jnp.dot(xs_ref[rows, :], wbuf[slot, e], preferred_element_type=F32)
                return carry2

            lax.fori_loop(0, EARLY // 3, experts, 0)

            @pl.when(j + UP_BUFS < steps)
            def _():
                for c in weight_copies(j + UP_BUFS, slot):
                    c.start()
        return carry

    lax.fori_loop(0, steps + UP_LAG + 1, main, 0)

    gate_act = acc_ref[:, :128]
    hid_ref[...] = (gate_act * jax.nn.sigmoid(gate_act) * acc_ref[:, 128:]).astype(BF16)
    logits = logit_ref[...]
    ex = jnp.exp(logits - jnp.max(logits, axis=-1, keepdims=True))
    probs = ex / jnp.sum(ex, axis=-1, keepdims=True)
    lanes = lax.broadcasted_iota(jnp.int32, probs.shape, 1)
    picked = [jnp.sum(jnp.where(column(ch_ref[ep, j:j + 1, :]) == lanes, probs, 0.0), axis=-1, keepdims=True) for j in range(2)]
    for j in range(2):
        gate_ref[:, j:j + 1] = picked[j] / (picked[0] + picked[1])

    def last_waits(j, carry):
        x_copy(j).wait_send()
        own_copy(j).wait_send()
        y_copy(j).wait_send()
        dx_copy(j).wait_send()
        dy_copy(j).wait_send()
        return carry

    lax.fori_loop(0, steps, last_waits, 0)
    for n in range(3):
        choice_copy(n).wait_send()


def late_kernel(act_ref, late_ref, wg_hbm, wu_hbm, hid_ref, list_ref, wbuf, w_sem):
    ep = lax.axis_index('ep')
    local = wg_hbm.shape[0]
    hid_ref[...] = jnp.zeros_like(hid_ref)

    def scan(e, n):
        busy = act_ref[0, ep * local + e] > 0

        @pl.when(busy)
        def _():
            list_ref[n] = e
        return n + busy.astype(jnp.int32)

    count = lax.fori_loop(EARLY, local, scan, 0)

    def weight_copies(n):
        slot = lax.rem(n, LATE_BUFS)
        e = list_ref[n]
        return [pltpu.make_async_copy(w.at[e], wbuf.at[slot, :, m * 128:(m + 1) * 128], w_sem.at[slot, m]) for m, w in enumerate((wg_hbm, wu_hbm))]

    def start(n):
        @pl.when(n < count)
        def _():
            for c in weight_copies(n):
                c.start()

    for n in range(LATE_BUFS):
        start(n)

    def step(n, carry):
        for c in weight_copies(n):
            c.wait()
        rows = pl.ds(pl.multiple_of((list_ref[n] - EARLY) * 16, 16), 16)
        both = jnp.dot(late_ref[rows, :], wbuf[lax.rem(n, LATE_BUFS)], preferred_element_type=F32)
        gate_act = both[:, :128]
        hid_ref[rows, :] = (gate_act * jax.nn.sigmoid(gate_act) * both[:, 128:]).astype(BF16)
        start(n + LATE_BUFS)
        return carry

    lax.fori_loop(0, count, step, 0)


def down_kernel(rows_c, rows_n, early_ref, late_ref, x_ref, gate_ref, tab_ref, wd_hbm, out_ref,
                hid_ref, send_ref, land_ref, fwd_ref, yland_ref, qs_ref, w2buf, p_ref, s_ref, a_ref, b_ref,
                w_sem, q_s, q_r, f_s, f_r, o_s, o_r):
    dp, tp, ep, cx, core = place()
    local = wd_hbm.shape[0]
    tok, d_model = x_ref.shape
    half = d_model // 2
    steps = DOWN_STEPS
    cw = half // steps
    peers = [(1 - cx) * 2 + core, (1 - cx) * 2 + (1 - core), cx * 2 + (1 - core)]
    other_tp = (dp, 1 - tp, ep)

    barrier = pltpu.get_barrier_semaphore()
    for g in peers:
        pl.semaphore_signal(barrier, inc=1, device_id=(dp, tp, g), device_id_type=MESH)
    pl.semaphore_signal(barrier, inc=1, device_id=other_tp, device_id_type=MESH)

    def weight_copies(step, slot):
        out = []
        for h in range(2):
            cols = pl.ds(pl.multiple_of(h * half + step * cw, 128), cw)
            out.append(pltpu.make_async_copy(wd_hbm.at[:, :, cols], w2buf.at[slot, :, :, h * cw:(h + 1) * cw], w_sem.at[slot, h]))
        return out

    for b in range(DOWN_BUFS - 2):
        for c in weight_copies(b, b):
            c.start()

    hid_ref[0:EARLY * 16, :] = early_ref[...]
    hid_ref[EARLY * 16:, :] = late_ref[...]
    all_rows = GROUPS * rows_c
    slots = qs_ref.shape[0]
    gap = 128 - rows_c
    slot_iota = lax.broadcasted_iota(jnp.int32, (slots, tok), 0)
    c_iota = lax.broadcasted_iota(jnp.int32, (rows_c, tok), 0)

    def key_of(r):
        for n in range(1, GROUPS):
            r = r + jnp.where(r >= n * rows_c + (n - 1) * gap, gap, 0)
        return r

    def onehot(rows, values):
        return jnp.where(rows == values, 1.0, 0.0).astype(BF16)

    def times_t(a, b):
        return lax.dot_general(a, b, (((1,), (1,)), ((), ())), preferred_element_type=F32)

    for g in range(GROUPS):
        total = jnp.zeros((rows_c, slots), F32)
        for j in range(2):
            total += times_t(onehot(c_iota + ep * 128, tab_ref[g, 2 + j:3 + j, :]), onehot(slot_iota, tab_ref[g, j:j + 1, :]))
        p_ref[g * rows_c:(g + 1) * rows_c, :] = total.astype(BF16)
    key_iota = key_of(lax.broadcasted_iota(jnp.int32, (all_rows, tok), 0))
    n_iota = lax.broadcasted_iota(jnp.int32, (rows_n, tok), 0)
    my_key = [tab_ref[ep, 2 + j:3 + j, :] for j in range(2)]
    my_n = [tab_ref[ep, 4 + j:5 + j, :] for j in range(2)]
    total = jnp.zeros((rows_n, all_rows), F32)
    for j in range(2):
        total += times_t(onehot(n_iota, my_n[j]), onehot(key_iota, my_key[j]))
    s_ref[...] = total.astype(BF16)

    def split_gates(keys, pos, dst):
        mat = jnp.where(pos[0] == keys, gate_ref[:, 0:1], 0.0) + jnp.where(pos[1] == keys, gate_ref[:, 1:2], 0.0)
        for z in range(3):
            part = mat.astype(BF16)
            dst[z] = part
            mat = mat - part.astype(F32)

    split_gates(key_of(lax.broadcasted_iota(jnp.int32, (tok, all_rows), 1)), [column(v) for v in my_key], a_ref)
    split_gates(lax.broadcasted_iota(jnp.int32, (tok, rows_n), 1), [column(v) for v in my_n], b_ref)
    pl.semaphore_wait(barrier, 4)

    def q_copy(k, n):
        return remote(send_ref.at[k, :, peers[n]], land_ref.at[k, :, ep], q_s.at[k, n], q_r.at[k, n], (dp, tp, peers[n]))

    def f_copy(k):
        return remote(fwd_ref.at[k], yland_ref.at[k], f_s.at[k], f_r.at[k], other_tp)

    def o_copy(k):
        cols = pl.ds(pl.multiple_of(tp * half + k * cw, 128), cw)
        return remote(out_ref.at[:, cols], out_ref.at[:, cols], o_s.at[k], o_r.at[k], other_tp)

    def main(i, carry):
        @pl.when(i < steps)
        def _():
            slot = lax.rem(i, DOWN_BUFS)
            for c in weight_copies(i, slot):
                c.wait()

            def experts(t, carry2):
                for z in range(4):
                    e = t * 4 + z
                    rows = pl.ds(pl.multiple_of(e * 16, 16), 16)
                    qs_ref[rows, :] = jnp.dot(hid_ref[rows, :], w2buf[slot, e], preferred_element_type=F32).astype(BF16)
                return carry2

            lax.fori_loop(0, local // 4, experts, 0)
            for h in range(2):
                send_ref[i, h] = jnp.dot(p_ref[...], qs_ref[:, h * cw:(h + 1) * cw], preferred_element_type=F32).astype(BF16).reshape(GROUPS, rows_c, cw)
            land_ref[i, :, ep] = send_ref[i, :, ep]

            for n in range(3):
                q_copy(i, n).start()

            @pl.when(i + DOWN_BUFS - 2 < steps)
            def _():
                for c in weight_copies(i + DOWN_BUFS - 2, lax.rem(i + DOWN_BUFS - 2, DOWN_BUFS)):
                    c.start()

        @pl.when((i >= DOWN_LAG) & (i < steps + DOWN_LAG))
        def _():
            k = i - DOWN_LAG
            for n in range(3):
                q_copy(k, n).wait_recv()
            block = land_ref[k, 1 - tp].reshape(GROUPS * rows_c, cw)
            fwd_ref[k] = jnp.dot(s_ref[...], block, preferred_element_type=F32).astype(BF16)
            f_copy(k).start()

        @pl.when(i >= 2 * DOWN_LAG)
        def _():
            k = i - 2 * DOWN_LAG
            mine = land_ref[k, tp].reshape(GROUPS * rows_c, cw)
            mix = jnp.dot(a_ref[2], mine, preferred_element_type=F32)
            mix += jnp.dot(a_ref[1], mine, preferred_element_type=F32)
            mix += jnp.dot(a_ref[0], mine, preferred_element_type=F32)
            f_copy(k).wait_recv()
            theirs = yland_ref[k]
            for z in (2, 1, 0):
                mix += jnp.dot(b_ref[z], theirs, preferred_element_type=F32)
            cols = pl.ds(pl.multiple_of(tp * half + k * cw, 128), cw)
            out_ref[:, cols] = (x_ref[:, cols].astype(F32) + mix).astype(BF16)
            o_copy(k).start()
        return carry

    lax.fori_loop(0, steps + 2 * DOWN_LAG, main, 0)

    def last_waits(k, carry):
        for n in range(3):
            q_copy(k, n).wait_send()
        f_copy(k).wait_send()
        o_copy(k).wait_send()
        cols = pl.ds(pl.multiple_of((1 - tp) * half + k * cw, 128), cw)
        remote(out_ref.at[:, cols], out_ref.at[:, cols], o_s.at[k], o_r.at[k], other_tp).wait_recv()
        return carry

    lax.fori_loop(0, steps, last_waits, 0)


def run_up(x, g, wr, wg, wu, choice_t):
    tok, d_model = x.shape
    local = wg.shape[0]
    cw = d_model // 2 // UP_STEPS
    slots = local * GROUPS * CAP
    vm = pl.BlockSpec(memory_space=pltpu.VMEM)
    hbm = pl.BlockSpec(memory_space=pltpu.HBM)
    sem = pltpu.SemaphoreType.DMA
    return pl.pallas_call(
        up_kernel,
        out_shape=(
            jax.ShapeDtypeStruct((EARLY * 16, 128), BF16),
            jax.ShapeDtypeStruct((slots - EARLY * 16, d_model), BF16),
            jax.ShapeDtypeStruct((tok, 2), F32),
            jax.ShapeDtypeStruct((GROUPS, 8, tok), jnp.int32),
            jax.ShapeDtypeStruct((1, 128), jnp.int32),
            jax.ShapeDtypeStruct((1,), jnp.int32),
        ),
        in_specs=[vm, vm, vm, hbm, hbm, vm],
        out_specs=(vm, vm, vm, vm, vm, pl.BlockSpec(memory_space=pltpu.SMEM)),
        scratch_shapes=[
            pltpu.VMEM((UP_STEPS, 2, GROUPS, tok, cw), BF16),
            pltpu.VMEM((EARLY * 16, 2 * cw), BF16),
            pltpu.VMEM((slots, GROUPS * tok), BF16),
            pltpu.VMEM((EARLY * 16, 256), F32),
            pltpu.VMEM((UP_BUFS, EARLY, 2 * cw, 256), BF16),
            pltpu.VMEM((tok, 128), F32),
            pltpu.VMEM((GROUPS, 2, tok), jnp.int32),
            sem((UP_BUFS, 4)), sem((3,)), sem((3,)),
        ] + [sem((UP_STEPS,))] * 10,
        compiler_params=pltpu.CompilerParams(collective_id=0, has_side_effects=True, vmem_limit_bytes=VMEM_LIMIT),
        name='up',
    )(x, g, wr, wg, wu, choice_t)


def run_late(act, late, wg, wu):
    d_model = late.shape[1]
    vm = pl.BlockSpec(memory_space=pltpu.VMEM)
    hbm = pl.BlockSpec(memory_space=pltpu.HBM)
    return pl.pallas_call(
        late_kernel,
        out_shape=jax.ShapeDtypeStruct((late.shape[0], 128), BF16),
        in_specs=[pl.BlockSpec(memory_space=pltpu.SMEM), vm, hbm, hbm],
        out_specs=vm,
        scratch_shapes=[
            pltpu.SMEM((64,), jnp.int32),
            pltpu.VMEM((LATE_BUFS, d_model, 256), BF16),
            pltpu.SemaphoreType.DMA((LATE_BUFS, 2)),
        ],
        compiler_params=pltpu.CompilerParams(vmem_limit_bytes=40 * 1024 * 1024),
        name='late',
    )(act, late, wg, wu)


def run_down(tier, early, late, x, gate, tab, wd):
    rows_c, rows_n = TIERS[tier]
    tok, d_model = x.shape
    local = wd.shape[0]
    cw = d_model // 2 // DOWN_STEPS
    slots = local * GROUPS * CAP
    vm = pl.BlockSpec(memory_space=pltpu.VMEM)
    hbm = pl.BlockSpec(memory_space=pltpu.HBM)
    sem = pltpu.SemaphoreType.DMA
    return pl.pallas_call(
        functools.partial(down_kernel, rows_c, rows_n),
        out_shape=jax.ShapeDtypeStruct(x.shape, BF16),
        in_specs=[vm] * 5 + [hbm],
        out_specs=vm,
        scratch_shapes=[
            pltpu.VMEM((slots, 128), BF16),
            pltpu.VMEM((DOWN_STEPS, 2, GROUPS, rows_c, cw), BF16),
            pltpu.VMEM((DOWN_STEPS, 2, GROUPS, rows_c, cw), BF16),
            pltpu.VMEM((DOWN_STEPS, rows_n, cw), BF16),
            pltpu.VMEM((DOWN_STEPS, rows_n, cw), BF16),
            pltpu.VMEM((slots, 2 * cw), BF16),
            pltpu.VMEM((DOWN_BUFS, local, 128, 2 * cw), BF16),
            pltpu.VMEM((GROUPS * rows_c, slots), BF16),
            pltpu.VMEM((rows_n, GROUPS * rows_c), BF16),
            pltpu.VMEM((3, tok, GROUPS * rows_c), BF16),
            pltpu.VMEM((3, tok, rows_n), BF16),
            sem((DOWN_BUFS, 2)), sem((DOWN_STEPS, 3)), sem((DOWN_STEPS, 3)),
            sem((DOWN_STEPS,)), sem((DOWN_STEPS,)), sem((DOWN_STEPS,)), sem((DOWN_STEPS,)),
        ],
        compiler_params=pltpu.CompilerParams(collective_id=1 + tier, has_side_effects=True, vmem_limit_bytes=DOWN_VMEM[tier]),
        name='down%d' % rows_c,
    )(early, late, x, gate, tab, wd)


def solution(mesh):
    row_spec = P(('dp', 'ep'), None)

    def device_step(resid_in, norm_scale, w_router, w_gate, w_up, w_down, choice):
        early, rows_late, gate, tab, act, flag = run_up(resid_in, norm_scale, w_router, w_gate, w_up, choice.T)
        late = run_late(act, rows_late, w_gate, w_up)
        return lax.switch(flag[0], [functools.partial(run_down, t) for t in range(len(TIERS))], early, late, resid_in, gate, tab, w_down)

    return jax.shard_map(device_step, mesh=mesh, in_specs=(row_spec, P(None), P(None, None), P('ep', None, 'tp'), P('ep', None, 'tp'), P('ep', 'tp', None), row_spec), out_specs=row_spec, check_vma=False)
```

```python
import functools

import jax
import jax.numpy as jnp
from jax import lax
from jax.experimental import pallas as pl
from jax.experimental.pallas import tpu as pltpu
from jax.sharding import PartitionSpec as P

NORM_EPS = 1e-5
MESH = pl.DeviceIdType.MESH
F32 = jnp.float32
BF16 = jnp.bfloat16
CAP = 4
GROUPS = 4
UP_STEPS = 7
UP_BUFS = 3
EARLY = 18
AHEAD = 3
LATE_BUFS = 6
UP_LAG = 2
DOWN_STEPS = 14
DOWN_BUFS = 4
DOWN_LAG = 2
TIERS = ((64, 176), (80, 192), (96, 224), (128, 256))
DOWN_VMEM = (46 * 1024 * 1024, 48 * 1024 * 1024, 52 * 1024 * 1024, 56 * 1024 * 1024)
VMEM_LIMIT = 48 * 1024 * 1024


def remote(src, dst, send_sem, recv_sem, device):
    return pltpu.make_async_remote_copy(src_ref=src, dst_ref=dst, send_sem=send_sem, recv_sem=recv_sem, device_id=device, device_id_type=MESH)


def place():
    dp, tp, ep = lax.axis_index('dp'), lax.axis_index('tp'), lax.axis_index('ep')
    return dp, tp, ep, ep // 2, ep % 2


def column(row):
    n = row.shape[1]
    eye = lax.broadcasted_iota(jnp.int32, (n, n), 0) == lax.broadcasted_iota(jnp.int32, (n, n), 1)
    return jnp.sum(jnp.where(eye, row.astype(F32), 0.0), axis=1, keepdims=True).astype(jnp.int32)


def up_kernel(x_ref, g_ref, wr_ref, wg_hbm, wu_hbm, choice_ref, hid_ref, late_ref, gate_ref, tab_ref, act_ref, flag_ref,
              u_ref, xs_ref, pick_ref, acc_ref, wbuf, logit_ref, ch_ref,
              w_sem, c_s, c_r, own_s, own_r, x_s, x_r, y_s, y_r, dx_s, dx_r, dy_s, dy_r):
    dp, tp, ep, cx, core = place()
    tok, d_model = x_ref.shape
    half = d_model // 2
    steps = UP_STEPS
    cw = half // steps
    twin = (dp, tp, cx * 2 + (1 - core))
    across = (dp, tp, (1 - cx) * 2 + core)
    far_twin = (dp, tp, (1 - cx) * 2 + (1 - core))
    other_tp = (dp, 1 - tp, ep)
    far = (1 - cx) * 2 + core

    barrier = pltpu.get_barrier_semaphore()
    for peer in (twin, across, far_twin, other_tp):
        pl.semaphore_signal(barrier, inc=1, device_id=peer, device_id_type=MESH)

    def weight_copies(step, slot):
        out = []
        for h in range(2):
            rows = pl.ds(pl.multiple_of(h * half + step * cw, cw), cw)
            for m, w in enumerate((wg_hbm, wu_hbm)):
                out.append(pltpu.make_async_copy(w.at[0:EARLY, rows, :], wbuf.at[slot, :, h * cw:(h + 1) * cw, m * 128:(m + 1) * 128], w_sem.at[slot, h * 2 + m]))
        return out

    for b in range(2):
        for c in weight_copies(b, b):
            c.start()

    scale = g_ref[...].astype(F32).reshape(1, d_model)

    def norm_rows(r, carry):
        rows = pl.ds(pl.multiple_of(r * 16, 16), 16)
        xb = x_ref[rows, :].astype(F32)
        cen = xb - jnp.mean(xb, axis=-1, keepdims=True)
        var = jnp.mean(cen * cen, axis=-1, keepdims=True)
        u = (cen * lax.rsqrt(var + NORM_EPS) * scale).astype(BF16)
        for j in range(steps):
            for h in range(2):
                u_ref[j, h, ep, rows, :] = u[:, h * half + j * cw:h * half + (j + 1) * cw]
        return carry

    lax.fori_loop(0, tok // 16, norm_rows, 0)
    pl.semaphore_wait(barrier, 4)

    def choice_copy(n):
        peer = (across, far_twin, twin)[n]
        return remote(choice_ref, ch_ref.at[ep], c_s.at[n], c_r.at[n], peer)

    for n in range(3):
        choice_copy(n).start()

    own_copy = remote(u_ref.at[:, :, ep], u_ref.at[:, :, ep], own_s, own_r, twin)

    def x_copy(j):
        return remote(u_ref.at[j, tp, ep], u_ref.at[j, tp, ep], x_s.at[j], x_r.at[j], across)

    def y_copy(j):
        return remote(u_ref.at[j, tp, far], u_ref.at[j, tp, far], y_s.at[j], y_r.at[j], other_tp)

    def dx_copy(j):
        return remote(u_ref.at[j, tp, far], u_ref.at[j, tp, far], dx_s.at[j], dx_r.at[j], twin)

    def dy_copy(j):
        return remote(u_ref.at[j, 1 - tp, far], u_ref.at[j, 1 - tp, far], dy_s.at[j], dy_r.at[j], twin)

    def first_sends(j, carry):
        x_copy(j).start()
        return carry

    lax.fori_loop(0, AHEAD, first_sends, 0)
    own_copy.start()
    for b in range(2, UP_BUFS):
        for c in weight_copies(b, b):
            c.start()
    ch_ref[ep] = choice_ref[...]
    acc_ref[...] = jnp.zeros_like(acc_ref)
    logit_ref[...] = jnp.zeros_like(logit_ref)
    for n in range(3):
        choice_copy(n).wait_recv()

    slots = pick_ref.shape[0]
    upper = jnp.where(lax.broadcasted_iota(jnp.int32, (tok, tok), 0) < lax.broadcasted_iota(jnp.int32, (tok, tok), 1), 1.0, 0.0).astype(BF16)
    ids = lax.broadcasted_iota(jnp.int32, (tok, tok), 0)
    lane16 = lax.broadcasted_iota(jnp.int32, (16, tok), 0)
    slot_iota = lax.broadcasted_iota(jnp.int32, (slots, tok), 0)
    most = jnp.zeros((16, 1), F32)
    load = jnp.zeros((tok, 1), F32)
    for g in range(GROUPS):
        c = [ch_ref[g, j:j + 1, :] for j in range(2)]
        hot = [jnp.where(ids == c[j], 1.0, 0.0) for j in range(2)]
        earlier = jnp.dot((hot[0] + hot[1]).astype(BF16), upper, preferred_element_type=F32)
        pos = [jnp.sum(earlier * hot[j], axis=0, keepdims=True).astype(jnp.int32) for j in range(2)]
        kept = [pos[j] < CAP for j in range(2)]
        keptf = [jnp.where(kept[j], 1.0, 0.0) for j in range(2)]
        owner = [c[j] // 32 for j in range(2)]
        mine = [jnp.where(lane16 == owner[j], keptf[j], 0.0) for j in range(2)]
        every = [jnp.where(lane16 == GROUPS, keptf[j], 0.0) for j in range(2)]
        tally = mine[0] + mine[1] + every[0] + every[1]
        before = jnp.dot(tally.astype(BF16), upper, preferred_element_type=F32)
        load = load + jnp.sum(hot[0] + hot[1], axis=1, keepdims=True)
        most = jnp.maximum(most, jnp.sum(tally, axis=1, keepdims=True))
        rank = [jnp.sum(before * mine[j], axis=0, keepdims=True) for j in range(2)]
        rank[1] = rank[1] + jnp.where(owner[0] == owner[1], keptf[0], 0.0)
        nrank = [before[GROUPS:GROUPS + 1, :], before[GROUPS:GROUPS + 1, :] + keptf[0]]
        for j in range(2):
            slot = jnp.where(kept[j] & (owner[j] == ep), (c[j] - ep * 32) * 16 + g * CAP + pos[j], -1)
            tab_ref[g, j:j + 1, :] = slot
            tab_ref[g, 2 + j:3 + j, :] = jnp.where(kept[j], owner[j] * 128 + rank[j].astype(jnp.int32), -1)
            tab_ref[g, 4 + j:5 + j, :] = jnp.where(kept[j], nrank[j].astype(jnp.int32), -1)
        tab_ref[g, 6:8, :] = jnp.zeros((2, tok), jnp.int32)
        pick_ref[:, g * tok:(g + 1) * tok] = jnp.where((slot_iota == tab_ref[g, 0:1, :]) | (slot_iota == tab_ref[g, 1:2, :]), 1.0, 0.0).astype(BF16)
    sub16 = lax.broadcasted_iota(jnp.int32, (16, 1), 0)
    fits = [jnp.where(sub16 < GROUPS, rows_c, jnp.where(sub16 == GROUPS, rows_n, 0)).astype(F32) for rows_c, rows_n in TIERS[:-1]]
    level = jnp.zeros((1, 1), F32)
    for f in fits:
        level = level + jnp.max(jnp.where(most > f, 1.0, 0.0), axis=0, keepdims=True)
    diag = ids == lax.broadcasted_iota(jnp.int32, (tok, tok), 1)
    act_ref[...] = jnp.sum(jnp.where(diag, load, 0.0), axis=0, keepdims=True).astype(jnp.int32)
    flag_ref[0] = jnp.max(level).astype(jnp.int32)

    def main(i, carry):
        @pl.when(i < steps)
        def _():
            x_copy(i).wait_recv()
            y_copy(i).start()
            dx_copy(i).start()

        @pl.when(i + AHEAD < steps)
        def _():
            first_sends(i + AHEAD, 0)

        @pl.when((i >= UP_LAG) & (i < steps + UP_LAG))
        def _():
            j = i - UP_LAG
            y_copy(j).wait_recv()
            dy_copy(j).start()

        @pl.when(i >= UP_LAG + 1)
        def _():
            j = i - UP_LAG - 1
            slot = lax.rem(j, UP_BUFS)
            for h in range(2):
                kr = pl.ds(pl.multiple_of(h * half + j * cw, cw), cw)
                logit_ref[...] += jnp.dot(u_ref[j, h, ep], wr_ref[kr, :], preferred_element_type=F32)
            @pl.when(j == 0)
            def _():
                own_copy.wait_recv()
            dx_copy(j).wait_recv()
            dy_copy(j).wait_recv()
            for h in range(2):
                block = u_ref[j, h].reshape(GROUPS * tok, cw)
                rows_u = jnp.dot(pick_ref[...], block, preferred_element_type=F32).astype(BF16)
                xs_ref[:, h * cw:(h + 1) * cw] = rows_u[0:EARLY * 16]
                late_ref[:, pl.ds(pl.multiple_of(h * half + j * cw, cw), cw)] = rows_u[EARLY * 16:]
            for c in weight_copies(j, slot):
                c.wait()

            def experts(t, carry2):
                for z in range(3):
                    e = t * 3 + z
                    rows = pl.ds(pl.multiple_of(e * 16, 16), 16)
                    acc_ref[rows, :] += jnp.dot(xs_ref[rows, :], wbuf[slot, e], preferred_element_type=F32)
                return carry2

            lax.fori_loop(0, EARLY // 3, experts, 0)

            @pl.when(j + UP_BUFS < steps)
            def _():
                for c in weight_copies(j + UP_BUFS, slot):
                    c.start()
        return carry

    lax.fori_loop(0, steps + UP_LAG + 1, main, 0)

    gate_act = acc_ref[:, :128]
    hid_ref[...] = (gate_act * jax.nn.sigmoid(gate_act) * acc_ref[:, 128:]).astype(BF16)
    logits = logit_ref[...]
    ex = jnp.exp(logits - jnp.max(logits, axis=-1, keepdims=True))
    probs = ex / jnp.sum(ex, axis=-1, keepdims=True)
    lanes = lax.broadcasted_iota(jnp.int32, probs.shape, 1)
    picked = [jnp.sum(jnp.where(column(ch_ref[ep, j:j + 1, :]) == lanes, probs, 0.0), axis=-1, keepdims=True) for j in range(2)]
    for j in range(2):
        gate_ref[:, j:j + 1] = picked[j] / (picked[0] + picked[1])

    def last_waits(j, carry):
        x_copy(j).wait_send()
        y_copy(j).wait_send()
        dx_copy(j).wait_send()
        dy_copy(j).wait_send()
        return carry

    lax.fori_loop(0, steps, last_waits, 0)
    own_copy.wait_send()
    for n in range(3):
        choice_copy(n).wait_send()


def late_kernel(act_ref, late_ref, wg_hbm, wu_hbm, hid_ref, list_ref, wbuf, w_sem):
    ep = lax.axis_index('ep')
    local = wg_hbm.shape[0]
    hid_ref[...] = jnp.zeros_like(hid_ref)

    def scan(e, n):
        busy = act_ref[0, ep * local + e] > 0

        @pl.when(busy)
        def _():
            list_ref[n] = e
        return n + busy.astype(jnp.int32)

    count = lax.fori_loop(EARLY, local, scan, 0)

    def weight_copies(n):
        slot = lax.rem(n, LATE_BUFS)
        e = list_ref[n]
        return [pltpu.make_async_copy(w.at[e], wbuf.at[slot, :, m * 128:(m + 1) * 128], w_sem.at[slot, m]) for m, w in enumerate((wg_hbm, wu_hbm))]

    def start(n):
        @pl.when(n < count)
        def _():
            for c in weight_copies(n):
                c.start()

    for n in range(LATE_BUFS):
        start(n)

    def step(n, carry):
        for c in weight_copies(n):
            c.wait()
        rows = pl.ds(pl.multiple_of((list_ref[n] - EARLY) * 16, 16), 16)
        both = jnp.dot(late_ref[rows, :], wbuf[lax.rem(n, LATE_BUFS)], preferred_element_type=F32)
        gate_act = both[:, :128]
        hid_ref[rows, :] = (gate_act * jax.nn.sigmoid(gate_act) * both[:, 128:]).astype(BF16)
        start(n + LATE_BUFS)
        return carry

    lax.fori_loop(0, count, step, 0)


def down_kernel(rows_c, rows_n, early_ref, late_ref, x_ref, gate_ref, tab_ref, wd_hbm, out_ref,
                hid_ref, send_ref, land_ref, fwd_ref, yland_ref, qs_ref, w2buf, p_ref, s_ref, a_ref, b_ref,
                w_sem, q_s, q_r, f_s, f_r, o_s, o_r):
    dp, tp, ep, cx, core = place()
    local = wd_hbm.shape[0]
    tok, d_model = x_ref.shape
    half = d_model // 2
    steps = DOWN_STEPS
    cw = half // steps
    peers = [(1 - cx) * 2 + core, (1 - cx) * 2 + (1 - core), cx * 2 + (1 - core)]
    other_tp = (dp, 1 - tp, ep)

    barrier = pltpu.get_barrier_semaphore()
    for g in peers:
        pl.semaphore_signal(barrier, inc=1, device_id=(dp, tp, g), device_id_type=MESH)
    pl.semaphore_signal(barrier, inc=1, device_id=other_tp, device_id_type=MESH)

    def weight_copies(step, slot):
        out = []
        for h in range(2):
            cols = pl.ds(pl.multiple_of(h * half + step * cw, 128), cw)
            out.append(pltpu.make_async_copy(wd_hbm.at[:, :, cols], w2buf.at[slot, :, :, h * cw:(h + 1) * cw], w_sem.at[slot, h]))
        return out

    for b in range(DOWN_BUFS - 2):
        for c in weight_copies(b, b):
            c.start()

    hid_ref[0:EARLY * 16, :] = early_ref[...]
    hid_ref[EARLY * 16:, :] = late_ref[...]
    all_rows = GROUPS * rows_c
    slots = qs_ref.shape[0]
    gap = 128 - rows_c
    slot_iota = lax.broadcasted_iota(jnp.int32, (slots, tok), 0)
    c_iota = lax.broadcasted_iota(jnp.int32, (rows_c, tok), 0)

    def key_of(r):
        for n in range(1, GROUPS):
            r = r + jnp.where(r >= n * rows_c + (n - 1) * gap, gap, 0)
        return r

    def onehot(rows, values):
        return jnp.where(rows == values, 1.0, 0.0).astype(BF16)

    def times_t(a, b):
        return lax.dot_general(a, b, (((1,), (1,)), ((), ())), preferred_element_type=F32)

    for g in range(GROUPS):
        total = jnp.zeros((rows_c, slots), F32)
        for j in range(2):
            total += times_t(onehot(c_iota + ep * 128, tab_ref[g, 2 + j:3 + j, :]), onehot(slot_iota, tab_ref[g, j:j + 1, :]))
        p_ref[g * rows_c:(g + 1) * rows_c, :] = total.astype(BF16)
    key_iota = key_of(lax.broadcasted_iota(jnp.int32, (all_rows, tok), 0))
    n_iota = lax.broadcasted_iota(jnp.int32, (rows_n, tok), 0)
    my_key = [tab_ref[ep, 2 + j:3 + j, :] for j in range(2)]
    my_n = [tab_ref[ep, 4 + j:5 + j, :] for j in range(2)]
    total = jnp.zeros((rows_n, all_rows), F32)
    for j in range(2):
        total += times_t(onehot(n_iota, my_n[j]), onehot(key_iota, my_key[j]))
    s_ref[...] = total.astype(BF16)

    def split_gates(keys, pos, dst):
        mat = jnp.where(pos[0] == keys, gate_ref[:, 0:1], 0.0) + jnp.where(pos[1] == keys, gate_ref[:, 1:2], 0.0)
        for z in range(3):
            part = mat.astype(BF16)
            dst[z] = part
            mat = mat - part.astype(F32)

    split_gates(key_of(lax.broadcasted_iota(jnp.int32, (tok, all_rows), 1)), [column(v) for v in my_key], a_ref)
    split_gates(lax.broadcasted_iota(jnp.int32, (tok, rows_n), 1), [column(v) for v in my_n], b_ref)
    pl.semaphore_wait(barrier, 4)

    def q_copy(k, n):
        return remote(send_ref.at[k, :, peers[n]], land_ref.at[k, :, ep], q_s.at[k, n], q_r.at[k, n], (dp, tp, peers[n]))

    def f_copy(k):
        return remote(fwd_ref.at[k], yland_ref.at[k], f_s.at[k], f_r.at[k], other_tp)

    def o_copy(k):
        cols = pl.ds(pl.multiple_of(tp * half + k * cw, 128), cw)
        return remote(out_ref.at[:, cols], out_ref.at[:, cols], o_s.at[k], o_r.at[k], other_tp)

    def main(i, carry):
        @pl.when(i < steps)
        def _():
            slot = lax.rem(i, DOWN_BUFS)
            for c in weight_copies(i, slot):
                c.wait()

            def experts(t, carry2):
                for z in range(4):
                    e = t * 4 + z
                    rows = pl.ds(pl.multiple_of(e * 16, 16), 16)
                    qs_ref[rows, :] = jnp.dot(hid_ref[rows, :], w2buf[slot, e], preferred_element_type=F32).astype(BF16)
                return carry2

            lax.fori_loop(0, local // 4, experts, 0)
            for h in range(2):
                send_ref[i, h] = jnp.dot(p_ref[...], qs_ref[:, h * cw:(h + 1) * cw], preferred_element_type=F32).astype(BF16).reshape(GROUPS, rows_c, cw)
            land_ref[i, :, ep] = send_ref[i, :, ep]

            for n in range(3):
                q_copy(i, n).start()

            @pl.when(i + DOWN_BUFS - 2 < steps)
            def _():
                for c in weight_copies(i + DOWN_BUFS - 2, lax.rem(i + DOWN_BUFS - 2, DOWN_BUFS)):
                    c.start()

        @pl.when((i >= DOWN_LAG) & (i < steps + DOWN_LAG))
        def _():
            k = i - DOWN_LAG
            for n in range(3):
                q_copy(k, n).wait_recv()
            block = land_ref[k, 1 - tp].reshape(GROUPS * rows_c, cw)
            fwd_ref[k] = jnp.dot(s_ref[...], block, preferred_element_type=F32).astype(BF16)
            f_copy(k).start()

        @pl.when(i >= 2 * DOWN_LAG)
        def _():
            k = i - 2 * DOWN_LAG
            mine = land_ref[k, tp].reshape(GROUPS * rows_c, cw)
            mix = jnp.dot(a_ref[2], mine, preferred_element_type=F32)
            mix += jnp.dot(a_ref[1], mine, preferred_element_type=F32)
            mix += jnp.dot(a_ref[0], mine, preferred_element_type=F32)
            f_copy(k).wait_recv()
            theirs = yland_ref[k]
            for z in (2, 1, 0):
                mix += jnp.dot(b_ref[z], theirs, preferred_element_type=F32)
            cols = pl.ds(pl.multiple_of(tp * half + k * cw, 128), cw)
            out_ref[:, cols] = (x_ref[:, cols].astype(F32) + mix).astype(BF16)
            o_copy(k).start()
        return carry

    lax.fori_loop(0, steps + 2 * DOWN_LAG, main, 0)

    def last_waits(k, carry):
        for n in range(3):
            q_copy(k, n).wait_send()
        f_copy(k).wait_send()
        o_copy(k).wait_send()
        cols = pl.ds(pl.multiple_of((1 - tp) * half + k * cw, 128), cw)
        remote(out_ref.at[:, cols], out_ref.at[:, cols], o_s.at[k], o_r.at[k], other_tp).wait_recv()
        return carry

    lax.fori_loop(0, steps, last_waits, 0)


def run_up(x, g, wr, wg, wu, choice_t):
    tok, d_model = x.shape
    local = wg.shape[0]
    cw = d_model // 2 // UP_STEPS
    slots = local * GROUPS * CAP
    vm = pl.BlockSpec(memory_space=pltpu.VMEM)
    hbm = pl.BlockSpec(memory_space=pltpu.HBM)
    sem = pltpu.SemaphoreType.DMA
    return pl.pallas_call(
        up_kernel,
        out_shape=(
            jax.ShapeDtypeStruct((EARLY * 16, 128), BF16),
            jax.ShapeDtypeStruct((slots - EARLY * 16, d_model), BF16),
            jax.ShapeDtypeStruct((tok, 2), F32),
            jax.ShapeDtypeStruct((GROUPS, 8, tok), jnp.int32),
            jax.ShapeDtypeStruct((1, 128), jnp.int32),
            jax.ShapeDtypeStruct((1,), jnp.int32),
        ),
        in_specs=[vm, vm, vm, hbm, hbm, vm],
        out_specs=(vm, vm, vm, vm, vm, pl.BlockSpec(memory_space=pltpu.SMEM)),
        scratch_shapes=[
            pltpu.VMEM((UP_STEPS, 2, GROUPS, tok, cw), BF16),
            pltpu.VMEM((EARLY * 16, 2 * cw), BF16),
            pltpu.VMEM((slots, GROUPS * tok), BF16),
            pltpu.VMEM((EARLY * 16, 256), F32),
            pltpu.VMEM((UP_BUFS, EARLY, 2 * cw, 256), BF16),
            pltpu.VMEM((tok, 128), F32),
            pltpu.VMEM((GROUPS, 2, tok), jnp.int32),
            sem((UP_BUFS, 4)), sem((3,)), sem((3,)), sem, sem,
        ] + [sem((UP_STEPS,))] * 8,
        compiler_params=pltpu.CompilerParams(collective_id=0, has_side_effects=True, vmem_limit_bytes=VMEM_LIMIT),
        name='up',
    )(x, g, wr, wg, wu, choice_t)


def run_late(act, late, wg, wu):
    d_model = late.shape[1]
    vm = pl.BlockSpec(memory_space=pltpu.VMEM)
    hbm = pl.BlockSpec(memory_space=pltpu.HBM)
    return pl.pallas_call(
        late_kernel,
        out_shape=jax.ShapeDtypeStruct((late.shape[0], 128), BF16),
        in_specs=[pl.BlockSpec(memory_space=pltpu.SMEM), vm, hbm, hbm],
        out_specs=vm,
        scratch_shapes=[
            pltpu.SMEM((64,), jnp.int32),
            pltpu.VMEM((LATE_BUFS, d_model, 256), BF16),
            pltpu.SemaphoreType.DMA((LATE_BUFS, 2)),
        ],
        compiler_params=pltpu.CompilerParams(vmem_limit_bytes=40 * 1024 * 1024),
        name='late',
    )(act, late, wg, wu)


def run_down(tier, early, late, x, gate, tab, wd):
    rows_c, rows_n = TIERS[tier]
    tok, d_model = x.shape
    local = wd.shape[0]
    cw = d_model // 2 // DOWN_STEPS
    slots = local * GROUPS * CAP
    vm = pl.BlockSpec(memory_space=pltpu.VMEM)
    hbm = pl.BlockSpec(memory_space=pltpu.HBM)
    sem = pltpu.SemaphoreType.DMA
    return pl.pallas_call(
        functools.partial(down_kernel, rows_c, rows_n),
        out_shape=jax.ShapeDtypeStruct(x.shape, BF16),
        in_specs=[vm] * 5 + [hbm],
        out_specs=vm,
        scratch_shapes=[
            pltpu.VMEM((slots, 128), BF16),
            pltpu.VMEM((DOWN_STEPS, 2, GROUPS, rows_c, cw), BF16),
            pltpu.VMEM((DOWN_STEPS, 2, GROUPS, rows_c, cw), BF16),
            pltpu.VMEM((DOWN_STEPS, rows_n, cw), BF16),
            pltpu.VMEM((DOWN_STEPS, rows_n, cw), BF16),
            pltpu.VMEM((slots, 2 * cw), BF16),
            pltpu.VMEM((DOWN_BUFS, local, 128, 2 * cw), BF16),
            pltpu.VMEM((GROUPS * rows_c, slots), BF16),
            pltpu.VMEM((rows_n, GROUPS * rows_c), BF16),
            pltpu.VMEM((3, tok, GROUPS * rows_c), BF16),
            pltpu.VMEM((3, tok, rows_n), BF16),
            sem((DOWN_BUFS, 2)), sem((DOWN_STEPS, 3)), sem((DOWN_STEPS, 3)),
            sem((DOWN_STEPS,)), sem((DOWN_STEPS,)), sem((DOWN_STEPS,)), sem((DOWN_STEPS,)),
        ],
        compiler_params=pltpu.CompilerParams(collective_id=1 + tier, has_side_effects=True, vmem_limit_bytes=DOWN_VMEM[tier]),
        name='down%d' % rows_c,
    )(early, late, x, gate, tab, wd)


def solution(mesh):
    row_spec = P(('dp', 'ep'), None)

    def device_step(resid_in, norm_scale, w_router, w_gate, w_up, w_down, choice):
        early, rows_late, gate, tab, act, flag = run_up(resid_in, norm_scale, w_router, w_gate, w_up, choice.T)
        late = run_late(act, rows_late, w_gate, w_up)
        return lax.switch(flag[0], [functools.partial(run_down, t) for t in range(len(TIERS))], early, late, resid_in, gate, tab, w_down)

    return jax.shard_map(device_step, mesh=mesh, in_specs=(row_spec, P(None), P(None, None), P('ep', None, 'tp'), P('ep', None, 'tp'), P('ep', 'tp', None), row_spec), out_specs=row_spec, check_vma=False)
```

```python
import functools

import jax
import jax.numpy as jnp
from jax import lax
from jax.experimental import pallas as pl
from jax.experimental.pallas import tpu as pltpu
from jax.sharding import PartitionSpec as P

NORM_EPS = 1e-5
MESH = pl.DeviceIdType.MESH
F32 = jnp.float32
BF16 = jnp.bfloat16
CAP = 4
GROUPS = 4
UP_STEPS = 7
UP_BUFS = 3
EARLY = 24
AHEAD = 3
LATE_BUFS = 6
UP_LAG = 2
DOWN_STEPS = 14
DOWN_BUFS = 4
DOWN_LAG = 2
TIERS = ((64, 160, 112), (64, 176, 112), (80, 192, 128), (96, 224, 128), (128, 256, 128))
DOWN_VMEM = (46 * 1024 * 1024, 46 * 1024 * 1024, 48 * 1024 * 1024, 52 * 1024 * 1024, 56 * 1024 * 1024)
VMEM_LIMIT = 50 * 1024 * 1024


def remote(src, dst, send_sem, recv_sem, device):
    return pltpu.make_async_remote_copy(src_ref=src, dst_ref=dst, send_sem=send_sem, recv_sem=recv_sem, device_id=device, device_id_type=MESH)


def place():
    dp, tp, ep = lax.axis_index('dp'), lax.axis_index('tp'), lax.axis_index('ep')
    return dp, tp, ep, ep // 2, ep % 2


def column(row):
    n = row.shape[1]
    eye = lax.broadcasted_iota(jnp.int32, (n, n), 0) == lax.broadcasted_iota(jnp.int32, (n, n), 1)
    return jnp.sum(jnp.where(eye, row.astype(F32), 0.0), axis=1, keepdims=True).astype(jnp.int32)


def up_kernel(x_ref, g_ref, wr_ref, wg_hbm, wu_hbm, choice_ref, hid_ref, late_ref, gate_ref, tab_ref, act_ref, flag_ref,
              u_ref, xs_ref, pick_ref, acc_ref, wbuf, logit_ref, ch_ref,
              w_sem, c_s, c_r, own_s, own_r, x_s, x_r, y_s, y_r, dx_s, dx_r, dy_s, dy_r):
    dp, tp, ep, cx, core = place()
    tok, d_model = x_ref.shape
    half = d_model // 2
    steps = UP_STEPS
    cw = half // steps
    twin = (dp, tp, cx * 2 + (1 - core))
    across = (dp, tp, (1 - cx) * 2 + core)
    far_twin = (dp, tp, (1 - cx) * 2 + (1 - core))
    other_tp = (dp, 1 - tp, ep)
    far = (1 - cx) * 2 + core

    barrier = pltpu.get_barrier_semaphore()
    for peer in (twin, across, far_twin, other_tp):
        pl.semaphore_signal(barrier, inc=1, device_id=peer, device_id_type=MESH)

    def weight_copies(step, slot):
        out = []
        for h in range(2):
            rows = pl.ds(pl.multiple_of(h * half + step * cw, cw), cw)
            for m, w in enumerate((wg_hbm, wu_hbm)):
                out.append(pltpu.make_async_copy(w.at[0:EARLY, rows, :], wbuf.at[slot, :, h * cw:(h + 1) * cw, m * 128:(m + 1) * 128], w_sem.at[slot, h * 2 + m]))
        return out

    for b in range(2):
        for c in weight_copies(b, b):
            c.start()

    scale = g_ref[...].astype(F32).reshape(1, d_model)

    def norm_rows(r, carry):
        rows = pl.ds(pl.multiple_of(r * 16, 16), 16)
        xb = x_ref[rows, :].astype(F32)
        cen = xb - jnp.mean(xb, axis=-1, keepdims=True)
        var = jnp.mean(cen * cen, axis=-1, keepdims=True)
        u = (cen * lax.rsqrt(var + NORM_EPS) * scale).astype(BF16)
        for j in range(steps):
            for h in range(2):
                u_ref[j, h, ep, rows, :] = u[:, h * half + j * cw:h * half + (j + 1) * cw]
        return carry

    lax.fori_loop(0, tok // 16, norm_rows, 0)
    pl.semaphore_wait(barrier, 4)

    def choice_copy(n):
        peer = (across, far_twin, twin)[n]
        return remote(choice_ref, ch_ref.at[ep], c_s.at[n], c_r.at[n], peer)

    for n in range(3):
        choice_copy(n).start()

    own_copy = remote(u_ref.at[:, :, ep], u_ref.at[:, :, ep], own_s, own_r, twin)

    def x_copy(j):
        return remote(u_ref.at[j, tp, ep], u_ref.at[j, tp, ep], x_s.at[j], x_r.at[j], across)

    def y_copy(j):
        return remote(u_ref.at[j, tp, far], u_ref.at[j, tp, far], y_s.at[j], y_r.at[j], other_tp)

    def dx_copy(j):
        return remote(u_ref.at[j, tp, far], u_ref.at[j, tp, far], dx_s.at[j], dx_r.at[j], twin)

    def dy_copy(j):
        return remote(u_ref.at[j, 1 - tp, far], u_ref.at[j, 1 - tp, far], dy_s.at[j], dy_r.at[j], twin)

    def first_sends(j, carry):
        x_copy(j).start()
        return carry

    lax.fori_loop(0, AHEAD, first_sends, 0)
    own_copy.start()
    for b in range(2, UP_BUFS):
        for c in weight_copies(b, b):
            c.start()
    ch_ref[ep] = choice_ref[...]
    acc_ref[...] = jnp.zeros_like(acc_ref)
    logit_ref[...] = jnp.zeros_like(logit_ref)
    for n in range(3):
        choice_copy(n).wait_recv()

    slots = pick_ref.shape[0]
    upper = jnp.where(lax.broadcasted_iota(jnp.int32, (tok, tok), 0) < lax.broadcasted_iota(jnp.int32, (tok, tok), 1), 1.0, 0.0).astype(BF16)
    ids = lax.broadcasted_iota(jnp.int32, (tok, tok), 0)
    lane16 = lax.broadcasted_iota(jnp.int32, (16, tok), 0)
    slot_iota = lax.broadcasted_iota(jnp.int32, (slots, tok), 0)
    most = jnp.zeros((16, 1), F32)
    load = jnp.zeros((tok, 1), F32)
    for g in range(GROUPS):
        c = [ch_ref[g, j:j + 1, :] for j in range(2)]
        hot = [jnp.where(ids == c[j], 1.0, 0.0) for j in range(2)]
        earlier = jnp.dot((hot[0] + hot[1]).astype(BF16), upper, preferred_element_type=F32)
        pos = [jnp.sum(earlier * hot[j], axis=0, keepdims=True).astype(jnp.int32) for j in range(2)]
        kept = [pos[j] < CAP for j in range(2)]
        keptf = [jnp.where(kept[j], 1.0, 0.0) for j in range(2)]
        owner = [c[j] // 32 for j in range(2)]
        mine = [jnp.where(lane16 == owner[j], keptf[j], 0.0) for j in range(2)]
        every = [jnp.where(lane16 == GROUPS, keptf[j], 0.0) for j in range(2)]
        some = jnp.maximum(keptf[0], keptf[1])
        tally = mine[0] + mine[1] + every[0] + every[1] + jnp.where(lane16 == GROUPS + 1, some, 0.0)
        before = jnp.dot(tally.astype(BF16), upper, preferred_element_type=F32)
        load = load + jnp.sum(hot[0] + hot[1], axis=1, keepdims=True)
        most = jnp.maximum(most, jnp.sum(tally, axis=1, keepdims=True))
        rank = [jnp.sum(before * mine[j], axis=0, keepdims=True) for j in range(2)]
        rank[1] = rank[1] + jnp.where(owner[0] == owner[1], keptf[0], 0.0)
        nrank = [before[GROUPS:GROUPS + 1, :], before[GROUPS:GROUPS + 1, :] + keptf[0]]
        for j in range(2):
            slot = jnp.where(kept[j] & (owner[j] == ep), (c[j] - ep * 32) * 16 + g * CAP + pos[j], -1)
            tab_ref[g, j:j + 1, :] = slot
            tab_ref[g, 2 + j:3 + j, :] = jnp.where(kept[j], owner[j] * 128 + rank[j].astype(jnp.int32), -1)
            tab_ref[g, 4 + j:5 + j, :] = jnp.where(kept[j], nrank[j].astype(jnp.int32), -1)
        tab_ref[g, 6:7, :] = jnp.where(some > 0.0, before[GROUPS + 1:GROUPS + 2, :].astype(jnp.int32), -1)
        tab_ref[g, 7:8, :] = jnp.zeros((1, tok), jnp.int32)
        pick_ref[:, g * tok:(g + 1) * tok] = jnp.where((slot_iota == tab_ref[g, 0:1, :]) | (slot_iota == tab_ref[g, 1:2, :]), 1.0, 0.0).astype(BF16)
    sub16 = lax.broadcasted_iota(jnp.int32, (16, 1), 0)
    fits = [jnp.where(sub16 < GROUPS, rows_c, jnp.where(sub16 == GROUPS, rows_n, jnp.where(sub16 == GROUPS + 1, rows_t, 0))).astype(F32) for rows_c, rows_n, rows_t in TIERS[:-1]]
    level = jnp.zeros((1, 1), F32)
    for f in fits:
        level = level + jnp.max(jnp.where(most > f, 1.0, 0.0), axis=0, keepdims=True)
    diag = ids == lax.broadcasted_iota(jnp.int32, (tok, tok), 1)
    act_ref[...] = jnp.sum(jnp.where(diag, load, 0.0), axis=0, keepdims=True).astype(jnp.int32)
    flag_ref[0] = jnp.max(level).astype(jnp.int32)

    def main(i, carry):
        @pl.when(i < steps)
        def _():
            x_copy(i).wait_recv()
            y_copy(i).start()
            dx_copy(i).start()

        @pl.when(i + AHEAD < steps)
        def _():
            first_sends(i + AHEAD, 0)

        @pl.when((i >= UP_LAG) & (i < steps + UP_LAG))
        def _():
            j = i - UP_LAG
            y_copy(j).wait_recv()
            dy_copy(j).start()

        @pl.when(i >= UP_LAG + 1)
        def _():
            j = i - UP_LAG - 1
            slot = lax.rem(j, UP_BUFS)
            for h in range(2):
                kr = pl.ds(pl.multiple_of(h * half + j * cw, cw), cw)
                logit_ref[...] += jnp.dot(u_ref[j, h, ep], wr_ref[kr, :], preferred_element_type=F32)
            @pl.when(j == 0)
            def _():
                own_copy.wait_recv()
            dx_copy(j).wait_recv()
            dy_copy(j).wait_recv()
            for h in range(2):
                block = u_ref[j, h].reshape(GROUPS * tok, cw)
                rows_u = jnp.dot(pick_ref[...], block, preferred_element_type=F32).astype(BF16)
                xs_ref[:, h * cw:(h + 1) * cw] = rows_u[0:EARLY * 16]
                late_ref[:, pl.ds(pl.multiple_of(h * half + j * cw, cw), cw)] = rows_u[EARLY * 16:]
            for c in weight_copies(j, slot):
                c.wait()

            def experts(t, carry2):
                for z in range(3):
                    e = t * 3 + z
                    rows = pl.ds(pl.multiple_of(e * 16, 16), 16)
                    acc_ref[rows, :] += jnp.dot(xs_ref[rows, :], wbuf[slot, e], preferred_element_type=F32)
                return carry2

            lax.fori_loop(0, EARLY // 3, experts, 0)

            @pl.when(j + UP_BUFS < steps)
            def _():
                for c in weight_copies(j + UP_BUFS, slot):
                    c.start()
        return carry

    lax.fori_loop(0, steps + UP_LAG + 1, main, 0)

    gate_act = acc_ref[:, :128]
    hid_ref[...] = (gate_act * jax.nn.sigmoid(gate_act) * acc_ref[:, 128:]).astype(BF16)
    logits = logit_ref[...]
    ex = jnp.exp(logits - jnp.max(logits, axis=-1, keepdims=True))
    probs = ex / jnp.sum(ex, axis=-1, keepdims=True)
    lanes = lax.broadcasted_iota(jnp.int32, probs.shape, 1)
    picked = [jnp.sum(jnp.where(column(ch_ref[ep, j:j + 1, :]) == lanes, probs, 0.0), axis=-1, keepdims=True) for j in range(2)]
    for j in range(2):
        gate_ref[:, j:j + 1] = picked[j] / (picked[0] + picked[1])

    def last_waits(j, carry):
        x_copy(j).wait_send()
        y_copy(j).wait_send()
        dx_copy(j).wait_send()
        dy_copy(j).wait_send()
        return carry

    lax.fori_loop(0, steps, last_waits, 0)
    own_copy.wait_send()
    for n in range(3):
        choice_copy(n).wait_send()


def late_kernel(act_ref, late_ref, wg_hbm, wu_hbm, hid_ref, list_ref, wbuf, w_sem):
    ep = lax.axis_index('ep')
    local = wg_hbm.shape[0]
    hid_ref[...] = jnp.zeros_like(hid_ref)

    def scan(e, n):
        busy = act_ref[0, ep * local + e] > 0

        @pl.when(busy)
        def _():
            list_ref[n] = e
        return n + busy.astype(jnp.int32)

    count = lax.fori_loop(EARLY, local, scan, 0)

    def weight_copies(n):
        slot = lax.rem(n, LATE_BUFS)
        e = list_ref[n]
        return [pltpu.make_async_copy(w.at[e], wbuf.at[slot, :, m * 128:(m + 1) * 128], w_sem.at[slot, m]) for m, w in enumerate((wg_hbm, wu_hbm))]

    def start(n):
        @pl.when(n < count)
        def _():
            for c in weight_copies(n):
                c.start()

    for n in range(LATE_BUFS):
        start(n)

    def step(n, carry):
        for c in weight_copies(n):
            c.wait()
        rows = pl.ds(pl.multiple_of((list_ref[n] - EARLY) * 16, 16), 16)
        both = jnp.dot(late_ref[rows, :], wbuf[lax.rem(n, LATE_BUFS)], preferred_element_type=F32)
        gate_act = both[:, :128]
        hid_ref[rows, :] = (gate_act * jax.nn.sigmoid(gate_act) * both[:, 128:]).astype(BF16)
        start(n + LATE_BUFS)
        return carry

    lax.fori_loop(0, count, step, 0)


def down_kernel(rows_c, rows_n, rows_t, early_ref, late_ref, x_ref, gate_ref, tab_ref, wd_hbm, out_ref,
                hid_ref, send_ref, land_ref, fwd_ref, yland_ref, done_ref, theirs_ref, qs_ref, w2buf, p_ref, s_ref, a_ref, b_ref, t_ref, e_ref,
                w_sem, q_s, q_r, f_s, f_r, o_s, o_r):
    dp, tp, ep, cx, core = place()
    local = wd_hbm.shape[0]
    tok, d_model = x_ref.shape
    half = d_model // 2
    steps = DOWN_STEPS
    cw = half // steps
    peers = [(1 - cx) * 2 + core, (1 - cx) * 2 + (1 - core), cx * 2 + (1 - core)]
    other_tp = (dp, 1 - tp, ep)

    barrier = pltpu.get_barrier_semaphore()
    for g in peers:
        pl.semaphore_signal(barrier, inc=1, device_id=(dp, tp, g), device_id_type=MESH)
    pl.semaphore_signal(barrier, inc=1, device_id=other_tp, device_id_type=MESH)

    def weight_copies(step, slot):
        out = []
        for h in range(2):
            cols = pl.ds(pl.multiple_of(h * half + step * cw, 128), cw)
            out.append(pltpu.make_async_copy(wd_hbm.at[:, :, cols], w2buf.at[slot, :, :, h * cw:(h + 1) * cw], w_sem.at[slot, h]))
        return out

    for b in range(DOWN_BUFS - 2):
        for c in weight_copies(b, b):
            c.start()

    hid_ref[0:EARLY * 16, :] = early_ref[...]
    hid_ref[EARLY * 16:, :] = late_ref[...]
    all_rows = GROUPS * rows_c
    slots = qs_ref.shape[0]
    gap = 128 - rows_c
    slot_iota = lax.broadcasted_iota(jnp.int32, (slots, tok), 0)
    c_iota = lax.broadcasted_iota(jnp.int32, (rows_c, tok), 0)

    def key_of(r):
        for n in range(1, GROUPS):
            r = r + jnp.where(r >= n * rows_c + (n - 1) * gap, gap, 0)
        return r

    def onehot(rows, values):
        return jnp.where(rows == values, 1.0, 0.0).astype(BF16)

    def times_t(a, b):
        return lax.dot_general(a, b, (((1,), (1,)), ((), ())), preferred_element_type=F32)

    for g in range(GROUPS):
        total = jnp.zeros((rows_c, slots), F32)
        for j in range(2):
            total += times_t(onehot(c_iota + ep * 128, tab_ref[g, 2 + j:3 + j, :]), onehot(slot_iota, tab_ref[g, j:j + 1, :]))
        p_ref[g * rows_c:(g + 1) * rows_c, :] = total.astype(BF16)
    key_iota = key_of(lax.broadcasted_iota(jnp.int32, (all_rows, tok), 0))
    n_iota = lax.broadcasted_iota(jnp.int32, (rows_n, tok), 0)
    my_key = [tab_ref[ep, 2 + j:3 + j, :] for j in range(2)]
    my_n = [tab_ref[ep, 4 + j:5 + j, :] for j in range(2)]
    total = jnp.zeros((rows_n, all_rows), F32)
    for j in range(2):
        total += times_t(onehot(n_iota, my_n[j]), onehot(key_iota, my_key[j]))
    s_ref[...] = total.astype(BF16)

    def split_gates(keys, pos, dst):
        mat = jnp.where(pos[0] == keys, gate_ref[:, 0:1], 0.0) + jnp.where(pos[1] == keys, gate_ref[:, 1:2], 0.0)
        for z in range(3):
            part = mat.astype(BF16)
            dst[z] = part
            mat = mat - part.astype(F32)

    split_gates(key_of(lax.broadcasted_iota(jnp.int32, (tok, all_rows), 1)), [column(v) for v in my_key], a_ref)
    split_gates(lax.broadcasted_iota(jnp.int32, (tok, rows_n), 1), [column(v) for v in my_n], b_ref)
    my_t = tab_ref[ep, 6:7, :]
    t_ref[...] = onehot(lax.broadcasted_iota(jnp.int32, (rows_t, tok), 0), my_t)
    e_ref[...] = onehot(lax.broadcasted_iota(jnp.int32, (tok, rows_t), 1), column(my_t))
    some = column(my_t) >= 0
    pl.semaphore_wait(barrier, 4)

    def q_copy(k, n):
        return remote(send_ref.at[k, :, peers[n]], land_ref.at[k, :, ep], q_s.at[k, n], q_r.at[k, n], (dp, tp, peers[n]))

    def f_copy(k):
        return remote(fwd_ref.at[k], yland_ref.at[k], f_s.at[k], f_r.at[k], other_tp)

    def o_copy(k):
        return remote(done_ref.at[k], theirs_ref.at[k], o_s.at[k], o_r.at[k], other_tp)

    def main(i, carry):
        @pl.when(i < steps)
        def _():
            slot = lax.rem(i, DOWN_BUFS)
            for c in weight_copies(i, slot):
                c.wait()

            def experts(t, carry2):
                for z in range(4):
                    e = t * 4 + z
                    rows = pl.ds(pl.multiple_of(e * 16, 16), 16)
                    qs_ref[rows, :] = jnp.dot(hid_ref[rows, :], w2buf[slot, e], preferred_element_type=F32).astype(BF16)
                return carry2

            lax.fori_loop(0, local // 4, experts, 0)
            for h in range(2):
                send_ref[i, h] = jnp.dot(p_ref[...], qs_ref[:, h * cw:(h + 1) * cw], preferred_element_type=F32).astype(BF16).reshape(GROUPS, rows_c, cw)
            land_ref[i, :, ep] = send_ref[i, :, ep]

            for n in range(3):
                q_copy(i, n).start()

            @pl.when(i + DOWN_BUFS - 2 < steps)
            def _():
                for c in weight_copies(i + DOWN_BUFS - 2, lax.rem(i + DOWN_BUFS - 2, DOWN_BUFS)):
                    c.start()

        @pl.when((i >= DOWN_LAG) & (i < steps + DOWN_LAG))
        def _():
            k = i - DOWN_LAG
            for n in range(3):
                q_copy(k, n).wait_recv()
            block = land_ref[k, 1 - tp].reshape(GROUPS * rows_c, cw)
            fwd_ref[k] = jnp.dot(s_ref[...], block, preferred_element_type=F32).astype(BF16)
            f_copy(k).start()

        @pl.when((i >= 2 * DOWN_LAG) & (i < steps + 2 * DOWN_LAG))
        def _():
            k = i - 2 * DOWN_LAG
            mine = land_ref[k, tp].reshape(GROUPS * rows_c, cw)
            mix = jnp.dot(a_ref[2], mine, preferred_element_type=F32)
            mix += jnp.dot(a_ref[1], mine, preferred_element_type=F32)
            mix += jnp.dot(a_ref[0], mine, preferred_element_type=F32)
            f_copy(k).wait_recv()
            theirs = yland_ref[k]
            for z in (2, 1, 0):
                mix += jnp.dot(b_ref[z], theirs, preferred_element_type=F32)
            cols = pl.ds(pl.multiple_of(tp * half + k * cw, 128), cw)
            rows = (x_ref[:, cols].astype(F32) + mix).astype(BF16)
            done_ref[k] = jnp.dot(t_ref[...], rows, preferred_element_type=F32).astype(BF16)
            o_copy(k).start()
            out_ref[:, cols] = rows

        @pl.when(i >= 3 * DOWN_LAG)
        def _():
            k = i - 3 * DOWN_LAG
            cols = pl.ds(pl.multiple_of((1 - tp) * half + k * cw, 128), cw)
            o_copy(k).wait_recv()
            rows = jnp.dot(e_ref[...], theirs_ref[k], preferred_element_type=F32)
            out_ref[:, cols] = jnp.where(some, rows, x_ref[:, cols].astype(F32)).astype(BF16)
        return carry

    lax.fori_loop(0, steps + 3 * DOWN_LAG, main, 0)

    def last_waits(k, carry):
        for n in range(3):
            q_copy(k, n).wait_send()
        f_copy(k).wait_send()
        o_copy(k).wait_send()
        return carry

    lax.fori_loop(0, steps, last_waits, 0)


def run_up(x, g, wr, wg, wu, choice_t):
    tok, d_model = x.shape
    local = wg.shape[0]
    cw = d_model // 2 // UP_STEPS
    slots = local * GROUPS * CAP
    vm = pl.BlockSpec(memory_space=pltpu.VMEM)
    hbm = pl.BlockSpec(memory_space=pltpu.HBM)
    sem = pltpu.SemaphoreType.DMA
    return pl.pallas_call(
        up_kernel,
        out_shape=(
            jax.ShapeDtypeStruct((EARLY * 16, 128), BF16),
            jax.ShapeDtypeStruct((slots - EARLY * 16, d_model), BF16),
            jax.ShapeDtypeStruct((tok, 2), F32),
            jax.ShapeDtypeStruct((GROUPS, 8, tok), jnp.int32),
            jax.ShapeDtypeStruct((1, 128), jnp.int32),
            jax.ShapeDtypeStruct((1,), jnp.int32),
        ),
        in_specs=[vm, vm, vm, hbm, hbm, vm],
        out_specs=(vm, vm, vm, vm, vm, pl.BlockSpec(memory_space=pltpu.SMEM)),
        scratch_shapes=[
            pltpu.VMEM((UP_STEPS, 2, GROUPS, tok, cw), BF16),
            pltpu.VMEM((EARLY * 16, 2 * cw), BF16),
            pltpu.VMEM((slots, GROUPS * tok), BF16),
            pltpu.VMEM((EARLY * 16, 256), F32),
            pltpu.VMEM((UP_BUFS, EARLY, 2 * cw, 256), BF16),
            pltpu.VMEM((tok, 128), F32),
            pltpu.VMEM((GROUPS, 2, tok), jnp.int32),
            sem((UP_BUFS, 4)), sem((3,)), sem((3,)), sem, sem,
        ] + [sem((UP_STEPS,))] * 8,
        compiler_params=pltpu.CompilerParams(collective_id=0, has_side_effects=True, vmem_limit_bytes=VMEM_LIMIT),
        name='up',
    )(x, g, wr, wg, wu, choice_t)


def run_late(act, late, wg, wu):
    d_model = late.shape[1]
    vm = pl.BlockSpec(memory_space=pltpu.VMEM)
    hbm = pl.BlockSpec(memory_space=pltpu.HBM)
    return pl.pallas_call(
        late_kernel,
        out_shape=jax.ShapeDtypeStruct((late.shape[0], 128), BF16),
        in_specs=[pl.BlockSpec(memory_space=pltpu.SMEM), vm, hbm, hbm],
        out_specs=vm,
        scratch_shapes=[
            pltpu.SMEM((64,), jnp.int32),
            pltpu.VMEM((LATE_BUFS, d_model, 256), BF16),
            pltpu.SemaphoreType.DMA((LATE_BUFS, 2)),
        ],
        compiler_params=pltpu.CompilerParams(vmem_limit_bytes=40 * 1024 * 1024),
        name='late',
    )(act, late, wg, wu)


def run_down(tier, early, late, x, gate, tab, wd):
    rows_c, rows_n, rows_t = TIERS[tier]
    tok, d_model = x.shape
    local = wd.shape[0]
    cw = d_model // 2 // DOWN_STEPS
    slots = local * GROUPS * CAP
    vm = pl.BlockSpec(memory_space=pltpu.VMEM)
    hbm = pl.BlockSpec(memory_space=pltpu.HBM)
    sem = pltpu.SemaphoreType.DMA
    return pl.pallas_call(
        functools.partial(down_kernel, rows_c, rows_n, rows_t),
        out_shape=jax.ShapeDtypeStruct(x.shape, BF16),
        in_specs=[vm] * 5 + [hbm],
        out_specs=vm,
        scratch_shapes=[
            pltpu.VMEM((slots, 128), BF16),
            pltpu.VMEM((DOWN_STEPS, 2, GROUPS, rows_c, cw), BF16),
            pltpu.VMEM((DOWN_STEPS, 2, GROUPS, rows_c, cw), BF16),
            pltpu.VMEM((DOWN_STEPS, rows_n, cw), BF16),
            pltpu.VMEM((DOWN_STEPS, rows_n, cw), BF16),
            pltpu.VMEM((DOWN_STEPS, rows_t, cw), BF16),
            pltpu.VMEM((DOWN_STEPS, rows_t, cw), BF16),
            pltpu.VMEM((slots, 2 * cw), BF16),
            pltpu.VMEM((DOWN_BUFS, local, 128, 2 * cw), BF16),
            pltpu.VMEM((GROUPS * rows_c, slots), BF16),
            pltpu.VMEM((rows_n, GROUPS * rows_c), BF16),
            pltpu.VMEM((3, tok, GROUPS * rows_c), BF16),
            pltpu.VMEM((3, tok, rows_n), BF16),
            pltpu.VMEM((rows_t, tok), BF16),
            pltpu.VMEM((tok, rows_t), BF16),
            sem((DOWN_BUFS, 2)), sem((DOWN_STEPS, 3)), sem((DOWN_STEPS, 3)),
            sem((DOWN_STEPS,)), sem((DOWN_STEPS,)), sem((DOWN_STEPS,)), sem((DOWN_STEPS,)),
        ],
        compiler_params=pltpu.CompilerParams(collective_id=1 + tier, has_side_effects=True, vmem_limit_bytes=DOWN_VMEM[tier]),
        name='down%d_%d' % (rows_c, rows_n),
    )(early, late, x, gate, tab, wd)


def solution(mesh):
    row_spec = P(('dp', 'ep'), None)

    def device_step(resid_in, norm_scale, w_router, w_gate, w_up, w_down, choice):
        early, rows_late, gate, tab, act, flag = run_up(resid_in, norm_scale, w_router, w_gate, w_up, choice.T)
        late = run_late(act, rows_late, w_gate, w_up)
        return lax.switch(flag[0], [functools.partial(run_down, t) for t in range(len(TIERS))], early, late, resid_in, gate, tab, w_down)

    return jax.shard_map(device_step, mesh=mesh, in_specs=(row_spec, P(None), P(None, None), P('ep', None, 'tp'), P('ep', None, 'tp'), P('ep', 'tp', None), row_spec), out_specs=row_spec, check_vma=False)
```

```python
import functools

import jax
import jax.numpy as jnp
from jax import lax
from jax.experimental import pallas as pl
from jax.experimental.pallas import tpu as pltpu
from jax.sharding import PartitionSpec as P

NORM_EPS = 1e-5
MESH = pl.DeviceIdType.MESH
F32 = jnp.float32
BF16 = jnp.bfloat16
CAP = 4
GROUPS = 4
UP_STEPS = 7
UP_BUFS = 4
EARLY = 18
AHEAD = 3
LATE_BUFS = 6
UP_LAG = 2
DOWN_STEPS = 14
DOWN_BUFS = 4
DOWN_LAG = 2
TIERS = ((64, 160, 112), (64, 176, 112), (80, 176, 128), (96, 224, 128), (128, 256, 128))
DOWN_VMEM = (46 * 1024 * 1024, 46 * 1024 * 1024, 48 * 1024 * 1024, 52 * 1024 * 1024, 56 * 1024 * 1024)
VMEM_LIMIT = 60 * 1024 * 1024


def remote(src, dst, send_sem, recv_sem, device):
    return pltpu.make_async_remote_copy(src_ref=src, dst_ref=dst, send_sem=send_sem, recv_sem=recv_sem, device_id=device, device_id_type=MESH)


def place():
    dp, tp, ep = lax.axis_index('dp'), lax.axis_index('tp'), lax.axis_index('ep')
    return dp, tp, ep, ep // 2, ep % 2


def column(row):
    n = row.shape[1]
    eye = lax.broadcasted_iota(jnp.int32, (n, n), 0) == lax.broadcasted_iota(jnp.int32, (n, n), 1)
    return jnp.sum(jnp.where(eye, row.astype(F32), 0.0), axis=1, keepdims=True).astype(jnp.int32)


def up_kernel(x_ref, g_ref, wr_hbm, wg_hbm, wu_hbm, choice_ref, hid_ref, late_hbm, gate_ref, tab_ref, act_ref, flag_ref,
              u_ref, xs_ref, pick_ref, acc_ref, wbuf, logit_ref, ch_ref, wr_ref, stage_ref,
              w_sem, wr_sem, l_sem, c_s, c_r, own_s, own_r, x_s, x_r, y_s, y_r, dx_s, dx_r, dy_s, dy_r):
    dp, tp, ep, cx, core = place()
    tok, d_model = x_ref.shape
    half = d_model // 2
    steps = UP_STEPS
    cw = half // steps
    twin = (dp, tp, cx * 2 + (1 - core))
    across = (dp, tp, (1 - cx) * 2 + core)
    far_twin = (dp, tp, (1 - cx) * 2 + (1 - core))
    other_tp = (dp, 1 - tp, ep)
    far = (1 - cx) * 2 + core

    barrier = pltpu.get_barrier_semaphore()
    for peer in (twin, across, far_twin, other_tp):
        pl.semaphore_signal(barrier, inc=1, device_id=peer, device_id_type=MESH)

    def weight_copies(step, slot):
        out = []
        for h in range(2):
            rows = pl.ds(pl.multiple_of(h * half + step * cw, cw), cw)
            for m, w in enumerate((wg_hbm, wu_hbm)):
                out.append(pltpu.make_async_copy(w.at[0:EARLY, rows, :], wbuf.at[slot, :, h * cw:(h + 1) * cw, m * 128:(m + 1) * 128], w_sem.at[slot, h * 2 + m]))
        return out

    for b in range(2):
        for c in weight_copies(b, b):
            c.start()

    scale = g_ref[...].astype(F32).reshape(1, d_model)

    def norm_rows(r, carry):
        rows = pl.ds(pl.multiple_of(r * 16, 16), 16)
        xb = x_ref[rows, :].astype(F32)
        cen = xb - jnp.mean(xb, axis=-1, keepdims=True)
        var = jnp.mean(cen * cen, axis=-1, keepdims=True)
        u = (cen * lax.rsqrt(var + NORM_EPS) * scale).astype(BF16)
        for j in range(steps):
            for h in range(2):
                u_ref[j, h, ep, rows, :] = u[:, h * half + j * cw:h * half + (j + 1) * cw]
        return carry

    lax.fori_loop(0, tok // 16, norm_rows, 0)
    pl.semaphore_wait(barrier, 4)

    def choice_copy(n):
        peer = (across, far_twin, twin)[n]
        return remote(choice_ref, ch_ref.at[ep], c_s.at[n], c_r.at[n], peer)

    for n in range(3):
        choice_copy(n).start()

    own_copy = remote(u_ref.at[:, :, ep], u_ref.at[:, :, ep], own_s, own_r, twin)

    def x_copy(j):
        return remote(u_ref.at[j, tp, ep], u_ref.at[j, tp, ep], x_s.at[j], x_r.at[j], across)

    def y_copy(j):
        return remote(u_ref.at[j, tp, far], u_ref.at[j, tp, far], y_s.at[j], y_r.at[j], other_tp)

    def dx_copy(j):
        return remote(u_ref.at[j, tp, far], u_ref.at[j, tp, far], dx_s.at[j], dx_r.at[j], twin)

    def dy_copy(j):
        return remote(u_ref.at[j, 1 - tp, far], u_ref.at[j, 1 - tp, far], dy_s.at[j], dy_r.at[j], twin)

    def first_sends(j, carry):
        x_copy(j).start()
        return carry

    lax.fori_loop(0, AHEAD, first_sends, 0)
    own_copy.start()
    wr_copy = pltpu.make_async_copy(wr_hbm, wr_ref, wr_sem)
    wr_copy.start()
    for b in range(2, UP_BUFS):
        for c in weight_copies(b, b):
            c.start()
    ch_ref[ep] = choice_ref[...]
    acc_ref[...] = jnp.zeros_like(acc_ref)
    logit_ref[...] = jnp.zeros_like(logit_ref)
    for n in range(3):
        choice_copy(n).wait_recv()

    slots = pick_ref.shape[0]
    upper = jnp.where(lax.broadcasted_iota(jnp.int32, (tok, tok), 0) < lax.broadcasted_iota(jnp.int32, (tok, tok), 1), 1.0, 0.0).astype(BF16)
    ids = lax.broadcasted_iota(jnp.int32, (tok, tok), 0)
    lane16 = lax.broadcasted_iota(jnp.int32, (16, tok), 0)
    slot_iota = lax.broadcasted_iota(jnp.int32, (slots, tok), 0)
    most = jnp.zeros((16, 1), F32)
    load = jnp.zeros((tok, 1), F32)
    for g in range(GROUPS):
        c = [ch_ref[g, j:j + 1, :] for j in range(2)]
        hot = [jnp.where(ids == c[j], 1.0, 0.0) for j in range(2)]
        earlier = jnp.dot((hot[0] + hot[1]).astype(BF16), upper, preferred_element_type=F32)
        pos = [jnp.sum(earlier * hot[j], axis=0, keepdims=True).astype(jnp.int32) for j in range(2)]
        kept = [pos[j] < CAP for j in range(2)]
        keptf = [jnp.where(kept[j], 1.0, 0.0) for j in range(2)]
        owner = [c[j] // 32 for j in range(2)]
        mine = [jnp.where(lane16 == owner[j], keptf[j], 0.0) for j in range(2)]
        every = [jnp.where(lane16 == GROUPS, keptf[j], 0.0) for j in range(2)]
        some = jnp.maximum(keptf[0], keptf[1])
        tally = mine[0] + mine[1] + every[0] + every[1] + jnp.where(lane16 == GROUPS + 1, some, 0.0)
        before = jnp.dot(tally.astype(BF16), upper, preferred_element_type=F32)
        load = load + jnp.sum(hot[0] + hot[1], axis=1, keepdims=True)
        most = jnp.maximum(most, jnp.sum(tally, axis=1, keepdims=True))
        rank = [jnp.sum(before * mine[j], axis=0, keepdims=True) for j in range(2)]
        rank[1] = rank[1] + jnp.where(owner[0] == owner[1], keptf[0], 0.0)
        nrank = [before[GROUPS:GROUPS + 1, :], before[GROUPS:GROUPS + 1, :] + keptf[0]]
        for j in range(2):
            slot = jnp.where(kept[j] & (owner[j] == ep), (c[j] - ep * 32) * 16 + g * CAP + pos[j], -1)
            tab_ref[g, j:j + 1, :] = slot
            tab_ref[g, 2 + j:3 + j, :] = jnp.where(kept[j], owner[j] * 128 + rank[j].astype(jnp.int32), -1)
            tab_ref[g, 4 + j:5 + j, :] = jnp.where(kept[j], nrank[j].astype(jnp.int32), -1)
        tab_ref[g, 6:7, :] = jnp.where(some > 0.0, before[GROUPS + 1:GROUPS + 2, :].astype(jnp.int32), -1)
        tab_ref[g, 7:8, :] = jnp.zeros((1, tok), jnp.int32)
        pick_ref[:, g * tok:(g + 1) * tok] = jnp.where((slot_iota == tab_ref[g, 0:1, :]) | (slot_iota == tab_ref[g, 1:2, :]), 1.0, 0.0).astype(BF16)
    sub16 = lax.broadcasted_iota(jnp.int32, (16, 1), 0)
    fits = [jnp.where(sub16 < GROUPS, rows_c, jnp.where(sub16 == GROUPS, rows_n, jnp.where(sub16 == GROUPS + 1, rows_t, 0))).astype(F32) for rows_c, rows_n, rows_t in TIERS[:-1]]
    level = jnp.zeros((1, 1), F32)
    for f in fits:
        level = level + jnp.max(jnp.where(most > f, 1.0, 0.0), axis=0, keepdims=True)
    diag = ids == lax.broadcasted_iota(jnp.int32, (tok, tok), 1)
    act_ref[...] = jnp.sum(jnp.where(diag, load, 0.0), axis=0, keepdims=True).astype(jnp.int32)
    flag_ref[0] = jnp.max(level).astype(jnp.int32)

    wr_copy.wait()

    def late_copies(j):
        out = []
        for h in range(2):
            cols = pl.ds(pl.multiple_of(h * half + j * cw, cw), cw)
            out.append(pltpu.make_async_copy(stage_ref.at[j, h], late_hbm.at[:, cols], l_sem.at[j, h]))
        return out

    def main(i, carry):
        @pl.when(i < steps)
        def _():
            x_copy(i).wait_recv()
            y_copy(i).start()
            dx_copy(i).start()

        @pl.when(i + AHEAD < steps)
        def _():
            first_sends(i + AHEAD, 0)

        @pl.when((i >= UP_LAG) & (i < steps + UP_LAG))
        def _():
            j = i - UP_LAG
            y_copy(j).wait_recv()
            dy_copy(j).start()

        @pl.when(i >= UP_LAG + 1)
        def _():
            j = i - UP_LAG - 1
            slot = lax.rem(j, UP_BUFS)
            for h in range(2):
                kr = pl.ds(pl.multiple_of(h * half + j * cw, cw), cw)
                logit_ref[...] += jnp.dot(u_ref[j, h, ep], wr_ref[kr, :], preferred_element_type=F32)
            @pl.when(j == 0)
            def _():
                own_copy.wait_recv()
            dx_copy(j).wait_recv()
            dy_copy(j).wait_recv()
            for h in range(2):
                block = u_ref[j, h].reshape(GROUPS * tok, cw)
                rows_u = jnp.dot(pick_ref[...], block, preferred_element_type=F32).astype(BF16)
                xs_ref[:, h * cw:(h + 1) * cw] = rows_u[0:EARLY * 16]
                stage_ref[j, h] = rows_u[EARLY * 16:]
            for c in weight_copies(j, slot):
                c.wait()
            for c in late_copies(j):
                c.start()

            def experts(t, carry2):
                for z in range(3):
                    e = t * 3 + z
                    rows = pl.ds(pl.multiple_of(e * 16, 16), 16)
                    acc_ref[rows, :] += jnp.dot(xs_ref[rows, :], wbuf[slot, e], preferred_element_type=F32)
                return carry2

            lax.fori_loop(0, EARLY // 3, experts, 0)

            @pl.when(j + UP_BUFS < steps)
            def _():
                for c in weight_copies(j + UP_BUFS, slot):
                    c.start()
        return carry

    lax.fori_loop(0, steps + UP_LAG + 1, main, 0)

    gate_act = acc_ref[:, :128]
    hid_ref[...] = (gate_act * jax.nn.sigmoid(gate_act) * acc_ref[:, 128:]).astype(BF16)
    logits = logit_ref[...]
    ex = jnp.exp(logits - jnp.max(logits, axis=-1, keepdims=True))
    probs = ex / jnp.sum(ex, axis=-1, keepdims=True)
    lanes = lax.broadcasted_iota(jnp.int32, probs.shape, 1)
    picked = [jnp.sum(jnp.where(column(ch_ref[ep, j:j + 1, :]) == lanes, probs, 0.0), axis=-1, keepdims=True) for j in range(2)]
    for j in range(2):
        gate_ref[:, j:j + 1] = picked[j] / (picked[0] + picked[1])

    def last_waits(j, carry):
        for c in late_copies(j):
            c.wait()
        x_copy(j).wait_send()
        y_copy(j).wait_send()
        dx_copy(j).wait_send()
        dy_copy(j).wait_send()
        return carry

    lax.fori_loop(0, steps, last_waits, 0)
    own_copy.wait_send()
    for n in range(3):
        choice_copy(n).wait_send()


def late_kernel(act_ref, late_hbm, wg_hbm, wu_hbm, hid_ref, list_ref, late_ref, wbuf, w_sem, l_sem):
    ep = lax.axis_index('ep')
    local = wg_hbm.shape[0]
    hid_ref[...] = jnp.zeros_like(hid_ref)

    def scan(e, n):
        busy = act_ref[0, ep * local + e] > 0

        @pl.when(busy)
        def _():
            list_ref[n] = e
        return n + busy.astype(jnp.int32)

    count = lax.fori_loop(EARLY, local, scan, 0)

    def weight_copies(n):
        slot = lax.rem(n, LATE_BUFS)
        e = list_ref[n]
        return [pltpu.make_async_copy(w.at[e], wbuf.at[slot, :, m * 128:(m + 1) * 128], w_sem.at[slot, m]) for m, w in enumerate((wg_hbm, wu_hbm))]

    def start(n):
        @pl.when(n < count)
        def _():
            for c in weight_copies(n):
                c.start()

    rows_copy = pltpu.make_async_copy(late_hbm, late_ref, l_sem)
    rows_copy.start()
    for n in range(LATE_BUFS):
        start(n)
    rows_copy.wait()

    def step(n, carry):
        for c in weight_copies(n):
            c.wait()
        rows = pl.ds(pl.multiple_of((list_ref[n] - EARLY) * 16, 16), 16)
        both = jnp.dot(late_ref[rows, :], wbuf[lax.rem(n, LATE_BUFS)], preferred_element_type=F32)
        gate_act = both[:, :128]
        hid_ref[rows, :] = (gate_act * jax.nn.sigmoid(gate_act) * both[:, 128:]).astype(BF16)
        start(n + LATE_BUFS)
        return carry

    lax.fori_loop(0, count, step, 0)


def down_kernel(rows_c, rows_n, rows_t, early_ref, late_ref, x_ref, gate_ref, tab_ref, wd_hbm, out_ref,
                hid_ref, send_ref, land_ref, fwd_ref, yland_ref, done_ref, theirs_ref, qs_ref, w2buf, p_ref, s_ref, a_ref, b_ref, t_ref, e_ref,
                w_sem, q_s, q_r, f_s, f_r, o_s, o_r):
    dp, tp, ep, cx, core = place()
    local = wd_hbm.shape[0]
    tok, d_model = x_ref.shape
    half = d_model // 2
    steps = DOWN_STEPS
    cw = half // steps
    peers = [(1 - cx) * 2 + core, (1 - cx) * 2 + (1 - core), cx * 2 + (1 - core)]
    other_tp = (dp, 1 - tp, ep)

    barrier = pltpu.get_barrier_semaphore()
    for g in peers:
        pl.semaphore_signal(barrier, inc=1, device_id=(dp, tp, g), device_id_type=MESH)
    pl.semaphore_signal(barrier, inc=1, device_id=other_tp, device_id_type=MESH)

    def weight_copies(step, slot):
        out = []
        for h in range(2):
            cols = pl.ds(pl.multiple_of(h * half + step * cw, 128), cw)
            out.append(pltpu.make_async_copy(wd_hbm.at[:, :, cols], w2buf.at[slot, :, :, h * cw:(h + 1) * cw], w_sem.at[slot, h]))
        return out

    for c in weight_copies(0, 0):
        c.start()

    hid_ref[0:EARLY * 16, :] = early_ref[...]
    hid_ref[EARLY * 16:, :] = late_ref[...]
    all_rows = GROUPS * rows_c
    slots = qs_ref.shape[0]
    gap = 128 - rows_c
    slot_iota = lax.broadcasted_iota(jnp.int32, (slots, tok), 0)
    c_iota = lax.broadcasted_iota(jnp.int32, (rows_c, tok), 0)

    def key_of(r):
        for n in range(1, GROUPS):
            r = r + jnp.where(r >= n * rows_c + (n - 1) * gap, gap, 0)
        return r

    def onehot(rows, values):
        return jnp.where(rows == values, 1.0, 0.0).astype(BF16)

    def times_t(a, b):
        return lax.dot_general(a, b, (((1,), (1,)), ((), ())), preferred_element_type=F32)

    for g in range(GROUPS):
        total = jnp.zeros((rows_c, slots), F32)
        for j in range(2):
            total += times_t(onehot(c_iota + ep * 128, tab_ref[g, 2 + j:3 + j, :]), onehot(slot_iota, tab_ref[g, j:j + 1, :]))
        p_ref[g * rows_c:(g + 1) * rows_c, :] = total.astype(BF16)
    key_iota = key_of(lax.broadcasted_iota(jnp.int32, (all_rows, tok), 0))
    n_iota = lax.broadcasted_iota(jnp.int32, (rows_n, tok), 0)
    my_key = [tab_ref[ep, 2 + j:3 + j, :] for j in range(2)]
    my_n = [tab_ref[ep, 4 + j:5 + j, :] for j in range(2)]
    total = jnp.zeros((rows_n, all_rows), F32)
    for j in range(2):
        total += times_t(onehot(n_iota, my_n[j]), onehot(key_iota, my_key[j]))
    s_ref[...] = total.astype(BF16)

    def split_gates(keys, pos, dst):
        mat = jnp.where(pos[0] == keys, gate_ref[:, 0:1], 0.0) + jnp.where(pos[1] == keys, gate_ref[:, 1:2], 0.0)
        for z in range(3):
            part = mat.astype(BF16)
            dst[z] = part
            mat = mat - part.astype(F32)

    split_gates(key_of(lax.broadcasted_iota(jnp.int32, (tok, all_rows), 1)), [column(v) for v in my_key], a_ref)
    split_gates(lax.broadcasted_iota(jnp.int32, (tok, rows_n), 1), [column(v) for v in my_n], b_ref)
    my_t = tab_ref[ep, 6:7, :]
    t_ref[...] = onehot(lax.broadcasted_iota(jnp.int32, (rows_t, tok), 0), my_t)
    e_ref[...] = onehot(lax.broadcasted_iota(jnp.int32, (tok, rows_t), 1), column(my_t))
    some = column(my_t) >= 0
    for c in weight_copies(1, 1):
        c.start()
    pl.semaphore_wait(barrier, 4)

    def q_copy(k, n):
        return remote(send_ref.at[k, :, peers[n]], land_ref.at[k, :, ep], q_s.at[k, n], q_r.at[k, n], (dp, tp, peers[n]))

    def f_copy(k):
        return remote(fwd_ref.at[k], yland_ref.at[k], f_s.at[k], f_r.at[k], other_tp)

    def o_copy(k):
        return remote(done_ref.at[k], theirs_ref.at[k], o_s.at[k], o_r.at[k], other_tp)

    def main(i, carry):
        @pl.when(i < steps)
        def _():
            slot = lax.rem(i, DOWN_BUFS)
            for c in weight_copies(i, slot):
                c.wait()

            def experts(t, carry2):
                for z in range(4):
                    e = t * 4 + z
                    rows = pl.ds(pl.multiple_of(e * 16, 16), 16)
                    qs_ref[rows, :] = jnp.dot(hid_ref[rows, :], w2buf[slot, e], preferred_element_type=F32).astype(BF16)
                return carry2

            lax.fori_loop(0, local // 4, experts, 0)
            for h in range(2):
                send_ref[i, h] = jnp.dot(p_ref[...], qs_ref[:, h * cw:(h + 1) * cw], preferred_element_type=F32).astype(BF16).reshape(GROUPS, rows_c, cw)
            land_ref[i, :, ep] = send_ref[i, :, ep]

            for n in range(3):
                q_copy(i, n).start()

            @pl.when(i + DOWN_BUFS - 2 < steps)
            def _():
                for c in weight_copies(i + DOWN_BUFS - 2, lax.rem(i + DOWN_BUFS - 2, DOWN_BUFS)):
                    c.start()

        @pl.when((i >= DOWN_LAG) & (i < steps + DOWN_LAG))
        def _():
            k = i - DOWN_LAG
            for n in range(3):
                q_copy(k, n).wait_recv()
            block = land_ref[k, 1 - tp].reshape(GROUPS * rows_c, cw)
            fwd_ref[k] = jnp.dot(s_ref[...], block, preferred_element_type=F32).astype(BF16)
            f_copy(k).start()

        @pl.when((i >= 2 * DOWN_LAG) & (i < steps + 2 * DOWN_LAG))
        def _():
            k = i - 2 * DOWN_LAG
            mine = land_ref[k, tp].reshape(GROUPS * rows_c, cw)
            mix = jnp.dot(a_ref[2], mine, preferred_element_type=F32)
            mix += jnp.dot(a_ref[1], mine, preferred_element_type=F32)
            mix += jnp.dot(a_ref[0], mine, preferred_element_type=F32)
            f_copy(k).wait_recv()
            theirs = yland_ref[k]
            for z in (2, 1, 0):
                mix += jnp.dot(b_ref[z], theirs, preferred_element_type=F32)
            cols = pl.ds(pl.multiple_of(tp * half + k * cw, 128), cw)
            rows = (x_ref[:, cols].astype(F32) + mix).astype(BF16)
            done_ref[k] = jnp.dot(t_ref[...], rows, preferred_element_type=F32).astype(BF16)
            o_copy(k).start()
            out_ref[:, cols] = rows

        @pl.when(i >= 3 * DOWN_LAG)
        def _():
            k = i - 3 * DOWN_LAG
            cols = pl.ds(pl.multiple_of((1 - tp) * half + k * cw, 128), cw)
            o_copy(k).wait_recv()
            rows = jnp.dot(e_ref[...], theirs_ref[k], preferred_element_type=F32)
            out_ref[:, cols] = jnp.where(some, rows, x_ref[:, cols].astype(F32)).astype(BF16)
        return carry

    lax.fori_loop(0, steps + 3 * DOWN_LAG, main, 0)

    def last_waits(k, carry):
        for n in range(3):
            q_copy(k, n).wait_send()
        f_copy(k).wait_send()
        o_copy(k).wait_send()
        return carry

    lax.fori_loop(0, steps, last_waits, 0)


def run_up(x, g, wr, wg, wu, choice_t):
    tok, d_model = x.shape
    local = wg.shape[0]
    cw = d_model // 2 // UP_STEPS
    slots = local * GROUPS * CAP
    vm = pl.BlockSpec(memory_space=pltpu.VMEM)
    hbm = pl.BlockSpec(memory_space=pltpu.HBM)
    sem = pltpu.SemaphoreType.DMA
    return pl.pallas_call(
        up_kernel,
        out_shape=(
            jax.ShapeDtypeStruct((EARLY * 16, 128), BF16),
            jax.ShapeDtypeStruct((slots - EARLY * 16, d_model), BF16),
            jax.ShapeDtypeStruct((tok, 2), F32),
            jax.ShapeDtypeStruct((GROUPS, 8, tok), jnp.int32),
            jax.ShapeDtypeStruct((1, 128), jnp.int32),
            jax.ShapeDtypeStruct((1,), jnp.int32),
        ),
        in_specs=[vm, vm, hbm, hbm, hbm, vm],
        out_specs=(vm, hbm, vm, vm, vm, pl.BlockSpec(memory_space=pltpu.SMEM)),
        scratch_shapes=[
            pltpu.VMEM((UP_STEPS, 2, GROUPS, tok, cw), BF16),
            pltpu.VMEM((EARLY * 16, 2 * cw), BF16),
            pltpu.VMEM((slots, GROUPS * tok), BF16),
            pltpu.VMEM((EARLY * 16, 256), F32),
            pltpu.VMEM((UP_BUFS, EARLY, 2 * cw, 256), BF16),
            pltpu.VMEM((tok, 128), F32),
            pltpu.VMEM((GROUPS, 2, tok), jnp.int32),
            pltpu.VMEM(wr.shape, BF16),
            pltpu.VMEM((UP_STEPS, 2, slots - EARLY * 16, cw), BF16),
            sem((UP_BUFS, 4)), sem, sem((UP_STEPS, 2)), sem((3,)), sem((3,)), sem, sem,
        ] + [sem((UP_STEPS,))] * 8,
        compiler_params=pltpu.CompilerParams(collective_id=0, has_side_effects=True, vmem_limit_bytes=VMEM_LIMIT),
        name='up',
    )(x, g, wr, wg, wu, choice_t)


def run_late(act, late, wg, wu):
    d_model = late.shape[1]
    vm = pl.BlockSpec(memory_space=pltpu.VMEM)
    hbm = pl.BlockSpec(memory_space=pltpu.HBM)
    return pl.pallas_call(
        late_kernel,
        out_shape=jax.ShapeDtypeStruct((late.shape[0], 128), BF16),
        in_specs=[pl.BlockSpec(memory_space=pltpu.SMEM), hbm, hbm, hbm],
        out_specs=vm,
        scratch_shapes=[
            pltpu.SMEM((64,), jnp.int32),
            pltpu.VMEM(late.shape, BF16),
            pltpu.VMEM((LATE_BUFS, d_model, 256), BF16),
            pltpu.SemaphoreType.DMA((LATE_BUFS, 2)),
            pltpu.SemaphoreType.DMA,
        ],
        compiler_params=pltpu.CompilerParams(vmem_limit_bytes=44 * 1024 * 1024),
        name='late',
    )(act, late, wg, wu)


def run_down(tier, early, late, x, gate, tab, wd):
    rows_c, rows_n, rows_t = TIERS[tier]
    tok, d_model = x.shape
    local = wd.shape[0]
    cw = d_model // 2 // DOWN_STEPS
    slots = local * GROUPS * CAP
    vm = pl.BlockSpec(memory_space=pltpu.VMEM)
    hbm = pl.BlockSpec(memory_space=pltpu.HBM)
    sem = pltpu.SemaphoreType.DMA
    return pl.pallas_call(
        functools.partial(down_kernel, rows_c, rows_n, rows_t),
        out_shape=jax.ShapeDtypeStruct(x.shape, BF16),
        in_specs=[vm] * 5 + [hbm],
        out_specs=vm,
        scratch_shapes=[
            pltpu.VMEM((slots, 128), BF16),
            pltpu.VMEM((DOWN_STEPS, 2, GROUPS, rows_c, cw), BF16),
            pltpu.VMEM((DOWN_STEPS, 2, GROUPS, rows_c, cw), BF16),
            pltpu.VMEM((DOWN_STEPS, rows_n, cw), BF16),
            pltpu.VMEM((DOWN_STEPS, rows_n, cw), BF16),
            pltpu.VMEM((DOWN_STEPS, rows_t, cw), BF16),
            pltpu.VMEM((DOWN_STEPS, rows_t, cw), BF16),
            pltpu.VMEM((slots, 2 * cw), BF16),
            pltpu.VMEM((DOWN_BUFS, local, 128, 2 * cw), BF16),
            pltpu.VMEM((GROUPS * rows_c, slots), BF16),
            pltpu.VMEM((rows_n, GROUPS * rows_c), BF16),
            pltpu.VMEM((3, tok, GROUPS * rows_c), BF16),
            pltpu.VMEM((3, tok, rows_n), BF16),
            pltpu.VMEM((rows_t, tok), BF16),
            pltpu.VMEM((tok, rows_t), BF16),
            sem((DOWN_BUFS, 2)), sem((DOWN_STEPS, 3)), sem((DOWN_STEPS, 3)),
            sem((DOWN_STEPS,)), sem((DOWN_STEPS,)), sem((DOWN_STEPS,)), sem((DOWN_STEPS,)),
        ],
        compiler_params=pltpu.CompilerParams(collective_id=1 + tier, has_side_effects=True, vmem_limit_bytes=DOWN_VMEM[tier]),
        name='down%d_%d' % (rows_c, rows_n),
    )(early, late, x, gate, tab, wd)


def solution(mesh):
    row_spec = P(('dp', 'ep'), None)

    def device_step(resid_in, norm_scale, w_router, w_gate, w_up, w_down, choice):
        early, rows_late, gate, tab, act, flag = run_up(resid_in, norm_scale, w_router, w_gate, w_up, choice.T)
        late = run_late(act, rows_late, w_gate, w_up)
        return lax.switch(flag[0], [functools.partial(run_down, t) for t in range(len(TIERS))], early, late, resid_in, gate, tab, w_down)

    return jax.shard_map(device_step, mesh=mesh, in_specs=(row_spec, P(None), P(None, None), P('ep', None, 'tp'), P('ep', None, 'tp'), P('ep', 'tp', None), row_spec), out_specs=row_spec, check_vma=False)
```

```python
import functools

import jax
import jax.numpy as jnp
from jax import lax
from jax.experimental import pallas as pl
from jax.experimental.pallas import tpu as pltpu
from jax.sharding import PartitionSpec as P

NORM_EPS = 1e-5
MESH = pl.DeviceIdType.MESH
F32 = jnp.float32
BF16 = jnp.bfloat16
CAP = 4
GROUPS = 4
UP_STEPS = 7
UP_BUFS = 4
EARLY = 20
AHEAD = 3
LATE_BUFS = 6
UP_LAG = 2
DOWN_STEPS = 14
DOWN_BUFS = 4
DOWN_LAG = 2
TIERS = ((64, 160, 112), (64, 176, 112), (80, 176, 128), (96, 224, 128), (128, 256, 128))
DOWN_VMEM = (46 * 1024 * 1024, 46 * 1024 * 1024, 48 * 1024 * 1024, 52 * 1024 * 1024, 56 * 1024 * 1024)
VMEM_LIMIT = 60 * 1024 * 1024


def remote(src, dst, send_sem, recv_sem, device):
    return pltpu.make_async_remote_copy(src_ref=src, dst_ref=dst, send_sem=send_sem, recv_sem=recv_sem, device_id=device, device_id_type=MESH)


def place():
    dp, tp, ep = lax.axis_index('dp'), lax.axis_index('tp'), lax.axis_index('ep')
    return dp, tp, ep, ep // 2, ep % 2


def column(row):
    n = row.shape[1]
    eye = lax.broadcasted_iota(jnp.int32, (n, n), 0) == lax.broadcasted_iota(jnp.int32, (n, n), 1)
    return jnp.sum(jnp.where(eye, row.astype(F32), 0.0), axis=1, keepdims=True).astype(jnp.int32)


def up_kernel(x_ref, g_ref, wr_hbm, wg_hbm, wu_hbm, choice_ref, hid_ref, late_hbm, gate_ref, tab_ref, act_ref, flag_ref,
              u_ref, xs_ref, pick_ref, acc_ref, wbuf, logit_ref, ch_ref, wr_ref, stage_ref,
              w_sem, wr_sem, l_sem, c_s, c_r, own_s, own_r, x_s, x_r, y_s, y_r, dx_s, dx_r, dy_s, dy_r):
    dp, tp, ep, cx, core = place()
    tok, d_model = x_ref.shape
    half = d_model // 2
    steps = UP_STEPS
    cw = half // steps
    twin = (dp, tp, cx * 2 + (1 - core))
    across = (dp, tp, (1 - cx) * 2 + core)
    far_twin = (dp, tp, (1 - cx) * 2 + (1 - core))
    other_tp = (dp, 1 - tp, ep)
    far = (1 - cx) * 2 + core

    barrier = pltpu.get_barrier_semaphore()
    for peer in (twin, across, far_twin, other_tp):
        pl.semaphore_signal(barrier, inc=1, device_id=peer, device_id_type=MESH)

    def weight_copies(step, slot):
        out = []
        for h in range(2):
            rows = pl.ds(pl.multiple_of(h * half + step * cw, cw), cw)
            for m, w in enumerate((wg_hbm, wu_hbm)):
                out.append(pltpu.make_async_copy(w.at[0:EARLY, rows, :], wbuf.at[slot, :, h * cw:(h + 1) * cw, m * 128:(m + 1) * 128], w_sem.at[slot, h * 2 + m]))
        return out

    for b in range(2):
        for c in weight_copies(b, b):
            c.start()

    scale = g_ref[...].astype(F32).reshape(1, d_model)

    def norm_rows(r, carry):
        rows = pl.ds(pl.multiple_of(r * 16, 16), 16)
        xb = x_ref[rows, :].astype(F32)
        cen = xb - jnp.mean(xb, axis=-1, keepdims=True)
        var = jnp.mean(cen * cen, axis=-1, keepdims=True)
        u = (cen * lax.rsqrt(var + NORM_EPS) * scale).astype(BF16)
        for j in range(steps):
            for h in range(2):
                u_ref[j, h, ep, rows, :] = u[:, h * half + j * cw:h * half + (j + 1) * cw]
        return carry

    lax.fori_loop(0, tok // 16, norm_rows, 0)
    pl.semaphore_wait(barrier, 4)

    def choice_copy(n):
        peer = (across, far_twin, twin)[n]
        return remote(choice_ref, ch_ref.at[ep], c_s.at[n], c_r.at[n], peer)

    for n in range(3):
        choice_copy(n).start()

    own_copy = remote(u_ref.at[:, :, ep], u_ref.at[:, :, ep], own_s, own_r, twin)

    def x_copy(j):
        return remote(u_ref.at[j, tp, ep], u_ref.at[j, tp, ep], x_s.at[j], x_r.at[j], across)

    def y_copy(j):
        return remote(u_ref.at[j, tp, far], u_ref.at[j, tp, far], y_s.at[j], y_r.at[j], other_tp)

    def dx_copy(j):
        return remote(u_ref.at[j, tp, far], u_ref.at[j, tp, far], dx_s.at[j], dx_r.at[j], twin)

    def dy_copy(j):
        return remote(u_ref.at[j, 1 - tp, far], u_ref.at[j, 1 - tp, far], dy_s.at[j], dy_r.at[j], twin)

    def first_sends(j, carry):
        x_copy(j).start()
        return carry

    lax.fori_loop(0, AHEAD, first_sends, 0)
    own_copy.start()
    wr_copy = pltpu.make_async_copy(wr_hbm, wr_ref, wr_sem)
    wr_copy.start()
    for b in range(2, UP_BUFS):
        for c in weight_copies(b, b):
            c.start()
    ch_ref[ep] = choice_ref[...]
    acc_ref[...] = jnp.zeros_like(acc_ref)
    logit_ref[...] = jnp.zeros_like(logit_ref)
    for n in range(3):
        choice_copy(n).wait_recv()

    slots = pick_ref.shape[0]
    upper = jnp.where(lax.broadcasted_iota(jnp.int32, (tok, tok), 0) < lax.broadcasted_iota(jnp.int32, (tok, tok), 1), 1.0, 0.0).astype(BF16)
    ids = lax.broadcasted_iota(jnp.int32, (tok, tok), 0)
    lane16 = lax.broadcasted_iota(jnp.int32, (16, tok), 0)
    slot_iota = lax.broadcasted_iota(jnp.int32, (slots, tok), 0)
    most = jnp.zeros((16, 1), F32)
    load = jnp.zeros((tok, 1), F32)
    for g in range(GROUPS):
        c = [ch_ref[g, j:j + 1, :] for j in range(2)]
        hot = [jnp.where(ids == c[j], 1.0, 0.0) for j in range(2)]
        earlier = jnp.dot((hot[0] + hot[1]).astype(BF16), upper, preferred_element_type=F32)
        pos = [jnp.sum(earlier * hot[j], axis=0, keepdims=True).astype(jnp.int32) for j in range(2)]
        kept = [pos[j] < CAP for j in range(2)]
        keptf = [jnp.where(kept[j], 1.0, 0.0) for j in range(2)]
        owner = [c[j] // 32 for j in range(2)]
        mine = [jnp.where(lane16 == owner[j], keptf[j], 0.0) for j in range(2)]
        every = [jnp.where(lane16 == GROUPS, keptf[j], 0.0) for j in range(2)]
        some = jnp.maximum(keptf[0], keptf[1])
        tally = mine[0] + mine[1] + every[0] + every[1] + jnp.where(lane16 == GROUPS + 1, some, 0.0)
        before = jnp.dot(tally.astype(BF16), upper, preferred_element_type=F32)
        load = load + jnp.sum(hot[0] + hot[1], axis=1, keepdims=True)
        most = jnp.maximum(most, jnp.sum(tally, axis=1, keepdims=True))
        rank = [jnp.sum(before * mine[j], axis=0, keepdims=True) for j in range(2)]
        rank[1] = rank[1] + jnp.where(owner[0] == owner[1], keptf[0], 0.0)
        nrank = [before[GROUPS:GROUPS + 1, :], before[GROUPS:GROUPS + 1, :] + keptf[0]]
        for j in range(2):
            slot = jnp.where(kept[j] & (owner[j] == ep), (c[j] - ep * 32) * 16 + g * CAP + pos[j], -1)
            tab_ref[g, j:j + 1, :] = slot
            tab_ref[g, 2 + j:3 + j, :] = jnp.where(kept[j], owner[j] * 128 + rank[j].astype(jnp.int32), -1)
            tab_ref[g, 4 + j:5 + j, :] = jnp.where(kept[j], nrank[j].astype(jnp.int32), -1)
        tab_ref[g, 6:7, :] = jnp.where(some > 0.0, before[GROUPS + 1:GROUPS + 2, :].astype(jnp.int32), -1)
        tab_ref[g, 7:8, :] = jnp.zeros((1, tok), jnp.int32)
        pick_ref[:, g * tok:(g + 1) * tok] = jnp.where((slot_iota == tab_ref[g, 0:1, :]) | (slot_iota == tab_ref[g, 1:2, :]), 1.0, 0.0).astype(BF16)
    sub16 = lax.broadcasted_iota(jnp.int32, (16, 1), 0)
    fits = [jnp.where(sub16 < GROUPS, rows_c, jnp.where(sub16 == GROUPS, rows_n, jnp.where(sub16 == GROUPS + 1, rows_t, 0))).astype(F32) for rows_c, rows_n, rows_t in TIERS[:-1]]
    level = jnp.zeros((1, 1), F32)
    for f in fits:
        level = level + jnp.max(jnp.where(most > f, 1.0, 0.0), axis=0, keepdims=True)
    diag = ids == lax.broadcasted_iota(jnp.int32, (tok, tok), 1)
    act_ref[...] = jnp.sum(jnp.where(diag, load, 0.0), axis=0, keepdims=True).astype(jnp.int32)
    flag_ref[0] = jnp.max(level).astype(jnp.int32)

    wr_copy.wait()

    def late_copies(j):
        out = []
        for h in range(2):
            cols = pl.ds(pl.multiple_of(h * half + j * cw, cw), cw)
            out.append(pltpu.make_async_copy(stage_ref.at[j, h], late_hbm.at[:, cols], l_sem.at[j, h]))
        return out

    def main(i, carry):
        @pl.when(i < steps)
        def _():
            x_copy(i).wait_recv()
            y_copy(i).start()
            dx_copy(i).start()

        @pl.when(i + AHEAD < steps)
        def _():
            first_sends(i + AHEAD, 0)

        @pl.when((i >= UP_LAG) & (i < steps + UP_LAG))
        def _():
            j = i - UP_LAG
            y_copy(j).wait_recv()
            dy_copy(j).start()

        @pl.when(i >= UP_LAG + 1)
        def _():
            j = i - UP_LAG - 1
            slot = lax.rem(j, UP_BUFS)
            for h in range(2):
                kr = pl.ds(pl.multiple_of(h * half + j * cw, cw), cw)
                logit_ref[...] += jnp.dot(u_ref[j, h, ep], wr_ref[kr, :], preferred_element_type=F32)
            @pl.when(j == 0)
            def _():
                own_copy.wait_recv()
            dx_copy(j).wait_recv()
            dy_copy(j).wait_recv()
            for h in range(2):
                block = u_ref[j, h].reshape(GROUPS * tok, cw)
                rows_u = jnp.dot(pick_ref[...], block, preferred_element_type=F32).astype(BF16)
                xs_ref[:, h * cw:(h + 1) * cw] = rows_u[0:EARLY * 16]
                stage_ref[j, h] = rows_u[EARLY * 16:]
            for c in weight_copies(j, slot):
                c.wait()
            for c in late_copies(j):
                c.start()

            def experts(t, carry2):
                for z in range(4):
                    e = t * 4 + z
                    rows = pl.ds(pl.multiple_of(e * 16, 16), 16)
                    acc_ref[rows, :] += jnp.dot(xs_ref[rows, :], wbuf[slot, e], preferred_element_type=F32)
                return carry2

            lax.fori_loop(0, EARLY // 4, experts, 0)

            @pl.when(j + UP_BUFS < steps)
            def _():
                for c in weight_copies(j + UP_BUFS, slot):
                    c.start()
        return carry

    lax.fori_loop(0, steps + UP_LAG + 1, main, 0)

    gate_act = acc_ref[:, :128]
    hid_ref[...] = (gate_act * jax.nn.sigmoid(gate_act) * acc_ref[:, 128:]).astype(BF16)
    logits = logit_ref[...]
    ex = jnp.exp(logits - jnp.max(logits, axis=-1, keepdims=True))
    probs = ex / jnp.sum(ex, axis=-1, keepdims=True)
    lanes = lax.broadcasted_iota(jnp.int32, probs.shape, 1)
    picked = [jnp.sum(jnp.where(column(ch_ref[ep, j:j + 1, :]) == lanes, probs, 0.0), axis=-1, keepdims=True) for j in range(2)]
    for j in range(2):
        gate_ref[:, j:j + 1] = picked[j] / (picked[0] + picked[1])

    def last_waits(j, carry):
        for c in late_copies(j):
            c.wait()
        x_copy(j).wait_send()
        y_copy(j).wait_send()
        dx_copy(j).wait_send()
        dy_copy(j).wait_send()
        return carry

    lax.fori_loop(0, steps, last_waits, 0)
    own_copy.wait_send()
    for n in range(3):
        choice_copy(n).wait_send()


def late_kernel(act_ref, late_hbm, wg_hbm, wu_hbm, hid_ref, list_ref, late_ref, wbuf, w_sem, l_sem):
    ep = lax.axis_index('ep')
    local = wg_hbm.shape[0]
    hid_ref[...] = jnp.zeros_like(hid_ref)

    def scan(e, n):
        busy = act_ref[0, ep * local + e] > 0

        @pl.when(busy)
        def _():
            list_ref[n] = e
        return n + busy.astype(jnp.int32)

    count = lax.fori_loop(EARLY, local, scan, 0)

    def weight_copies(n):
        slot = lax.rem(n, LATE_BUFS)
        e = list_ref[n]
        return [pltpu.make_async_copy(w.at[e], wbuf.at[slot, :, m * 128:(m + 1) * 128], w_sem.at[slot, m]) for m, w in enumerate((wg_hbm, wu_hbm))]

    def start(n):
        @pl.when(n < count)
        def _():
            for c in weight_copies(n):
                c.start()

    rows_copy = pltpu.make_async_copy(late_hbm, late_ref, l_sem)
    rows_copy.start()
    for n in range(LATE_BUFS):
        start(n)
    rows_copy.wait()

    def step(n, carry):
        for c in weight_copies(n):
            c.wait()
        rows = pl.ds(pl.multiple_of((list_ref[n] - EARLY) * 16, 16), 16)
        both = jnp.dot(late_ref[rows, :], wbuf[lax.rem(n, LATE_BUFS)], preferred_element_type=F32)
        gate_act = both[:, :128]
        hid_ref[rows, :] = (gate_act * jax.nn.sigmoid(gate_act) * both[:, 128:]).astype(BF16)
        start(n + LATE_BUFS)
        return carry

    lax.fori_loop(0, count, step, 0)


def down_kernel(rows_c, rows_n, rows_t, early_ref, late_ref, x_ref, gate_ref, tab_ref, wd_hbm, out_ref,
                hid_ref, send_ref, land_ref, fwd_ref, yland_ref, done_ref, theirs_ref, qs_ref, w2buf, p_ref, s_ref, a_ref, b_ref, t_ref, e_ref,
                w_sem, q_s, q_r, f_s, f_r, o_s, o_r):
    dp, tp, ep, cx, core = place()
    local = wd_hbm.shape[0]
    tok, d_model = x_ref.shape
    half = d_model // 2
    steps = DOWN_STEPS
    cw = half // steps
    peers = [(1 - cx) * 2 + core, (1 - cx) * 2 + (1 - core), cx * 2 + (1 - core)]
    other_tp = (dp, 1 - tp, ep)

    barrier = pltpu.get_barrier_semaphore()
    for g in peers:
        pl.semaphore_signal(barrier, inc=1, device_id=(dp, tp, g), device_id_type=MESH)
    pl.semaphore_signal(barrier, inc=1, device_id=other_tp, device_id_type=MESH)

    def weight_copies(step, slot):
        out = []
        for h in range(2):
            cols = pl.ds(pl.multiple_of(h * half + step * cw, 128), cw)
            out.append(pltpu.make_async_copy(wd_hbm.at[:, :, cols], w2buf.at[slot, :, :, h * cw:(h + 1) * cw], w_sem.at[slot, h]))
        return out

    for c in weight_copies(0, 0):
        c.start()

    hid_ref[0:EARLY * 16, :] = early_ref[...]
    hid_ref[EARLY * 16:, :] = late_ref[...]
    all_rows = GROUPS * rows_c
    slots = qs_ref.shape[0]
    gap = 128 - rows_c
    slot_iota = lax.broadcasted_iota(jnp.int32, (slots, tok), 0)
    c_iota = lax.broadcasted_iota(jnp.int32, (rows_c, tok), 0)

    def key_of(r):
        for n in range(1, GROUPS):
            r = r + jnp.where(r >= n * rows_c + (n - 1) * gap, gap, 0)
        return r

    def onehot(rows, values):
        return jnp.where(rows == values, 1.0, 0.0).astype(BF16)

    def times_t(a, b):
        return lax.dot_general(a, b, (((1,), (1,)), ((), ())), preferred_element_type=F32)

    for g in range(GROUPS):
        total = jnp.zeros((rows_c, slots), F32)
        for j in range(2):
            total += times_t(onehot(c_iota + ep * 128, tab_ref[g, 2 + j:3 + j, :]), onehot(slot_iota, tab_ref[g, j:j + 1, :]))
        p_ref[g * rows_c:(g + 1) * rows_c, :] = total.astype(BF16)
    key_iota = key_of(lax.broadcasted_iota(jnp.int32, (all_rows, tok), 0))
    n_iota = lax.broadcasted_iota(jnp.int32, (rows_n, tok), 0)
    my_key = [tab_ref[ep, 2 + j:3 + j, :] for j in range(2)]
    my_n = [tab_ref[ep, 4 + j:5 + j, :] for j in range(2)]
    total = jnp.zeros((rows_n, all_rows), F32)
    for j in range(2):
        total += times_t(onehot(n_iota, my_n[j]), onehot(key_iota, my_key[j]))
    s_ref[...] = total.astype(BF16)

    def split_gates(keys, pos, dst):
        mat = jnp.where(pos[0] == keys, gate_ref[:, 0:1], 0.0) + jnp.where(pos[1] == keys, gate_ref[:, 1:2], 0.0)
        for z in range(3):
            part = mat.astype(BF16)
            dst[z] = part
            mat = mat - part.astype(F32)

    split_gates(key_of(lax.broadcasted_iota(jnp.int32, (tok, all_rows), 1)), [column(v) for v in my_key], a_ref)
    split_gates(lax.broadcasted_iota(jnp.int32, (tok, rows_n), 1), [column(v) for v in my_n], b_ref)
    my_t = tab_ref[ep, 6:7, :]
    t_ref[...] = onehot(lax.broadcasted_iota(jnp.int32, (rows_t, tok), 0), my_t)
    e_ref[...] = onehot(lax.broadcasted_iota(jnp.int32, (tok, rows_t), 1), column(my_t))
    some = column(my_t) >= 0
    for c in weight_copies(1, 1):
        c.start()
    pl.semaphore_wait(barrier, 4)

    def q_copy(k, n):
        return remote(send_ref.at[k, :, peers[n]], land_ref.at[k, :, ep], q_s.at[k, n], q_r.at[k, n], (dp, tp, peers[n]))

    def f_copy(k):
        return remote(fwd_ref.at[k], yland_ref.at[k], f_s.at[k], f_r.at[k], other_tp)

    def o_copy(k):
        return remote(done_ref.at[k], theirs_ref.at[k], o_s.at[k], o_r.at[k], other_tp)

    def main(i, carry):
        @pl.when((i >= DOWN_LAG) & (i < steps + DOWN_LAG))
        def _():
            k = i - DOWN_LAG
            for n in range(3):
                q_copy(k, n).wait_recv()
            block = land_ref[k, 1 - tp].reshape(GROUPS * rows_c, cw)
            fwd_ref[k] = jnp.dot(s_ref[...], block, preferred_element_type=F32).astype(BF16)
            f_copy(k).start()

        @pl.when(i < steps)
        def _():
            slot = lax.rem(i, DOWN_BUFS)
            for c in weight_copies(i, slot):
                c.wait()

            def experts(t, carry2):
                for z in range(4):
                    e = t * 4 + z
                    rows = pl.ds(pl.multiple_of(e * 16, 16), 16)
                    qs_ref[rows, :] = jnp.dot(hid_ref[rows, :], w2buf[slot, e], preferred_element_type=F32).astype(BF16)
                return carry2

            lax.fori_loop(0, local // 4, experts, 0)
            for h in range(2):
                send_ref[i, h] = jnp.dot(p_ref[...], qs_ref[:, h * cw:(h + 1) * cw], preferred_element_type=F32).astype(BF16).reshape(GROUPS, rows_c, cw)
            land_ref[i, :, ep] = send_ref[i, :, ep]

            for n in range(3):
                q_copy(i, n).start()

            @pl.when(i + DOWN_BUFS - 2 < steps)
            def _():
                for c in weight_copies(i + DOWN_BUFS - 2, lax.rem(i + DOWN_BUFS - 2, DOWN_BUFS)):
                    c.start()

        @pl.when((i >= 2 * DOWN_LAG) & (i < steps + 2 * DOWN_LAG))
        def _():
            k = i - 2 * DOWN_LAG
            mine = land_ref[k, tp].reshape(GROUPS * rows_c, cw)
            mix = jnp.dot(a_ref[2], mine, preferred_element_type=F32)
            mix += jnp.dot(a_ref[1], mine, preferred_element_type=F32)
            mix += jnp.dot(a_ref[0], mine, preferred_element_type=F32)
            f_copy(k).wait_recv()
            theirs = yland_ref[k]
            for z in (2, 1, 0):
                mix += jnp.dot(b_ref[z], theirs, preferred_element_type=F32)
            cols = pl.ds(pl.multiple_of(tp * half + k * cw, 128), cw)
            rows = (x_ref[:, cols].astype(F32) + mix).astype(BF16)
            done_ref[k] = jnp.dot(t_ref[...], rows, preferred_element_type=F32).astype(BF16)
            o_copy(k).start()
            out_ref[:, cols] = rows

        @pl.when(i >= 3 * DOWN_LAG)
        def _():
            k = i - 3 * DOWN_LAG
            cols = pl.ds(pl.multiple_of((1 - tp) * half + k * cw, 128), cw)
            o_copy(k).wait_recv()
            rows = jnp.dot(e_ref[...], theirs_ref[k], preferred_element_type=F32)
            out_ref[:, cols] = jnp.where(some, rows, x_ref[:, cols].astype(F32)).astype(BF16)
        return carry

    lax.fori_loop(0, steps + 3 * DOWN_LAG, main, 0)

    def last_waits(k, carry):
        for n in range(3):
            q_copy(k, n).wait_send()
        f_copy(k).wait_send()
        o_copy(k).wait_send()
        return carry

    lax.fori_loop(0, steps, last_waits, 0)


def run_up(x, g, wr, wg, wu, choice_t):
    tok, d_model = x.shape
    local = wg.shape[0]
    cw = d_model // 2 // UP_STEPS
    slots = local * GROUPS * CAP
    vm = pl.BlockSpec(memory_space=pltpu.VMEM)
    hbm = pl.BlockSpec(memory_space=pltpu.HBM)
    sem = pltpu.SemaphoreType.DMA
    return pl.pallas_call(
        up_kernel,
        out_shape=(
            jax.ShapeDtypeStruct((EARLY * 16, 128), BF16),
            jax.ShapeDtypeStruct((slots - EARLY * 16, d_model), BF16),
            jax.ShapeDtypeStruct((tok, 2), F32),
            jax.ShapeDtypeStruct((GROUPS, 8, tok), jnp.int32),
            jax.ShapeDtypeStruct((1, 128), jnp.int32),
            jax.ShapeDtypeStruct((1,), jnp.int32),
        ),
        in_specs=[vm, vm, hbm, hbm, hbm, vm],
        out_specs=(vm, hbm, vm, vm, vm, pl.BlockSpec(memory_space=pltpu.SMEM)),
        scratch_shapes=[
            pltpu.VMEM((UP_STEPS, 2, GROUPS, tok, cw), BF16),
            pltpu.VMEM((EARLY * 16, 2 * cw), BF16),
            pltpu.VMEM((slots, GROUPS * tok), BF16),
            pltpu.VMEM((EARLY * 16, 256), F32),
            pltpu.VMEM((UP_BUFS, EARLY, 2 * cw, 256), BF16),
            pltpu.VMEM((tok, 128), F32),
            pltpu.VMEM((GROUPS, 2, tok), jnp.int32),
            pltpu.VMEM(wr.shape, BF16),
            pltpu.VMEM((UP_STEPS, 2, slots - EARLY * 16, cw), BF16),
            sem((UP_BUFS, 4)), sem, sem((UP_STEPS, 2)), sem((3,)), sem((3,)), sem, sem,
        ] + [sem((UP_STEPS,))] * 8,
        compiler_params=pltpu.CompilerParams(collective_id=0, has_side_effects=True, vmem_limit_bytes=VMEM_LIMIT),
        name='up',
    )(x, g, wr, wg, wu, choice_t)


def run_late(act, late, wg, wu):
    d_model = late.shape[1]
    vm = pl.BlockSpec(memory_space=pltpu.VMEM)
    hbm = pl.BlockSpec(memory_space=pltpu.HBM)
    return pl.pallas_call(
        late_kernel,
        out_shape=jax.ShapeDtypeStruct((late.shape[0], 128), BF16),
        in_specs=[pl.BlockSpec(memory_space=pltpu.SMEM), hbm, hbm, hbm],
        out_specs=vm,
        scratch_shapes=[
            pltpu.SMEM((64,), jnp.int32),
            pltpu.VMEM(late.shape, BF16),
            pltpu.VMEM((LATE_BUFS, d_model, 256), BF16),
            pltpu.SemaphoreType.DMA((LATE_BUFS, 2)),
            pltpu.SemaphoreType.DMA,
        ],
        compiler_params=pltpu.CompilerParams(vmem_limit_bytes=60 * 1024 * 1024),
        name='late',
    )(act, late, wg, wu)


def run_down(tier, early, late, x, gate, tab, wd):
    rows_c, rows_n, rows_t = TIERS[tier]
    tok, d_model = x.shape
    local = wd.shape[0]
    cw = d_model // 2 // DOWN_STEPS
    slots = local * GROUPS * CAP
    vm = pl.BlockSpec(memory_space=pltpu.VMEM)
    hbm = pl.BlockSpec(memory_space=pltpu.HBM)
    sem = pltpu.SemaphoreType.DMA
    return pl.pallas_call(
        functools.partial(down_kernel, rows_c, rows_n, rows_t),
        out_shape=jax.ShapeDtypeStruct(x.shape, BF16),
        in_specs=[vm] * 5 + [hbm],
        out_specs=vm,
        scratch_shapes=[
            pltpu.VMEM((slots, 128), BF16),
            pltpu.VMEM((DOWN_STEPS, 2, GROUPS, rows_c, cw), BF16),
            pltpu.VMEM((DOWN_STEPS, 2, GROUPS, rows_c, cw), BF16),
            pltpu.VMEM((DOWN_STEPS, rows_n, cw), BF16),
            pltpu.VMEM((DOWN_STEPS, rows_n, cw), BF16),
            pltpu.VMEM((DOWN_STEPS, rows_t, cw), BF16),
            pltpu.VMEM((DOWN_STEPS, rows_t, cw), BF16),
            pltpu.VMEM((slots, 2 * cw), BF16),
            pltpu.VMEM((DOWN_BUFS, local, 128, 2 * cw), BF16),
            pltpu.VMEM((GROUPS * rows_c, slots), BF16),
            pltpu.VMEM((rows_n, GROUPS * rows_c), BF16),
            pltpu.VMEM((3, tok, GROUPS * rows_c), BF16),
            pltpu.VMEM((3, tok, rows_n), BF16),
            pltpu.VMEM((rows_t, tok), BF16),
            pltpu.VMEM((tok, rows_t), BF16),
            sem((DOWN_BUFS, 2)), sem((DOWN_STEPS, 3)), sem((DOWN_STEPS, 3)),
            sem((DOWN_STEPS,)), sem((DOWN_STEPS,)), sem((DOWN_STEPS,)), sem((DOWN_STEPS,)),
        ],
        compiler_params=pltpu.CompilerParams(collective_id=1 + tier, has_side_effects=True, vmem_limit_bytes=DOWN_VMEM[tier]),
        name='down%d_%d' % (rows_c, rows_n),
    )(early, late, x, gate, tab, wd)


def solution(mesh):
    row_spec = P(('dp', 'ep'), None)

    def device_step(resid_in, norm_scale, w_router, w_gate, w_up, w_down, choice):
        early, rows_late, gate, tab, act, flag = run_up(resid_in, norm_scale, w_router, w_gate, w_up, choice.T)
        late = run_late(act, rows_late, w_gate, w_up)
        return lax.switch(flag[0], [functools.partial(run_down, t) for t in range(len(TIERS))], early, late, resid_in, gate, tab, w_down)

    return jax.shard_map(device_step, mesh=mesh, in_specs=(row_spec, P(None), P(None, None), P('ep', None, 'tp'), P('ep', None, 'tp'), P('ep', 'tp', None), row_spec), out_specs=row_spec, check_vma=False)
```

```python
import functools

import jax
import jax.numpy as jnp
from jax import lax
from jax.experimental import pallas as pl
from jax.experimental.pallas import tpu as pltpu
from jax.sharding import PartitionSpec as P

NORM_EPS = 1e-5
MESH = pl.DeviceIdType.MESH
F32 = jnp.float32
BF16 = jnp.bfloat16
CAP = 4
GROUPS = 4
UP_STEPS = 7
UP_BUFS = 4
EARLY = 20
AHEAD = 3
LATE_BUFS = 6
UP_LAG = 2
DOWN_STEPS = 14
DOWN_BUFS = 4
DOWN_LAG = 2
TIERS = ((64, 160, 112), (64, 176, 112), (80, 176, 128), (96, 224, 128), (128, 256, 128))
DOWN_VMEM = (46 * 1024 * 1024, 46 * 1024 * 1024, 48 * 1024 * 1024, 52 * 1024 * 1024, 56 * 1024 * 1024)
VMEM_LIMIT = 60 * 1024 * 1024


def remote(src, dst, send_sem, recv_sem, device):
    return pltpu.make_async_remote_copy(src_ref=src, dst_ref=dst, send_sem=send_sem, recv_sem=recv_sem, device_id=device, device_id_type=MESH)


def place():
    dp, tp, ep = lax.axis_index('dp'), lax.axis_index('tp'), lax.axis_index('ep')
    return dp, tp, ep, ep // 2, ep % 2


def column(row):
    n = row.shape[1]
    eye = lax.broadcasted_iota(jnp.int32, (n, n), 0) == lax.broadcasted_iota(jnp.int32, (n, n), 1)
    return jnp.sum(jnp.where(eye, row.astype(F32), 0.0), axis=1, keepdims=True).astype(jnp.int32)


def up_kernel(x_ref, g_ref, wr_hbm, wg_hbm, wu_hbm, choice_ref, hid_ref, late_hbm, gate_ref, tab_ref, act_ref, flag_ref,
              u_ref, xs_ref, pick_ref, acc_ref, wbuf, logit_ref, ch_ref, wr_ref, stage_ref,
              w_sem, wr_sem, l_sem, c_s, c_r, own_s, own_r, x_s, x_r, y_s, y_r, dx_s, dx_r, dy_s, dy_r):
    dp, tp, ep, cx, core = place()
    tok, d_model = x_ref.shape
    half = d_model // 2
    steps = UP_STEPS
    cw = half // steps
    twin = (dp, tp, cx * 2 + (1 - core))
    across = (dp, tp, (1 - cx) * 2 + core)
    far_twin = (dp, tp, (1 - cx) * 2 + (1 - core))
    other_tp = (dp, 1 - tp, ep)
    far = (1 - cx) * 2 + core

    barrier = pltpu.get_barrier_semaphore()
    for peer in (twin, across, far_twin, other_tp):
        pl.semaphore_signal(barrier, inc=1, device_id=peer, device_id_type=MESH)

    def weight_copies(step, slot):
        out = []
        for h in range(2):
            rows = pl.ds(pl.multiple_of(h * half + step * cw, cw), cw)
            for m, w in enumerate((wg_hbm, wu_hbm)):
                out.append(pltpu.make_async_copy(w.at[0:EARLY, rows, :], wbuf.at[slot, :, h * cw:(h + 1) * cw, m * 128:(m + 1) * 128], w_sem.at[slot, h * 2 + m]))
        return out

    for b in range(2):
        for c in weight_copies(b, b):
            c.start()

    scale = g_ref[...].astype(F32).reshape(1, d_model)

    def norm_rows(r, carry):
        rows = pl.ds(pl.multiple_of(r * 16, 16), 16)
        xb = x_ref[rows, :].astype(F32)
        cen = xb - jnp.mean(xb, axis=-1, keepdims=True)
        var = jnp.mean(cen * cen, axis=-1, keepdims=True)
        u = (cen * lax.rsqrt(var + NORM_EPS) * scale).astype(BF16)
        for j in range(steps):
            for h in range(2):
                u_ref[j, h, ep, rows, :] = u[:, h * half + j * cw:h * half + (j + 1) * cw]
        return carry

    lax.fori_loop(0, tok // 16, norm_rows, 0)
    pl.semaphore_wait(barrier, 4)

    def choice_copy(n):
        peer = (across, far_twin, twin)[n]
        return remote(choice_ref, ch_ref.at[ep], c_s.at[n], c_r.at[n], peer)

    for n in range(3):
        choice_copy(n).start()

    own_copy = remote(u_ref.at[:, :, ep], u_ref.at[:, :, ep], own_s, own_r, twin)

    def x_copy(j):
        return remote(u_ref.at[j, tp, ep], u_ref.at[j, tp, ep], x_s.at[j], x_r.at[j], across)

    def y_copy(j):
        return remote(u_ref.at[j, tp, far], u_ref.at[j, tp, far], y_s.at[j], y_r.at[j], other_tp)

    def dx_copy(j):
        return remote(u_ref.at[j, tp, far], u_ref.at[j, tp, far], dx_s.at[j], dx_r.at[j], twin)

    def dy_copy(j):
        return remote(u_ref.at[j, 1 - tp, far], u_ref.at[j, 1 - tp, far], dy_s.at[j], dy_r.at[j], twin)

    def first_sends(j, carry):
        x_copy(j).start()
        return carry

    lax.fori_loop(0, AHEAD, first_sends, 0)
    own_copy.start()
    wr_copy = pltpu.make_async_copy(wr_hbm, wr_ref, wr_sem)
    wr_copy.start()
    for b in range(2, UP_BUFS):
        for c in weight_copies(b, b):
            c.start()
    ch_ref[ep] = choice_ref[...]
    acc_ref[...] = jnp.zeros_like(acc_ref)
    logit_ref[...] = jnp.zeros_like(logit_ref)
    for n in range(3):
        choice_copy(n).wait_recv()

    slots = pick_ref.shape[0]
    upper = jnp.where(lax.broadcasted_iota(jnp.int32, (tok, tok), 0) < lax.broadcasted_iota(jnp.int32, (tok, tok), 1), 1.0, 0.0).astype(BF16)
    ids = lax.broadcasted_iota(jnp.int32, (tok, tok), 0)
    lane16 = lax.broadcasted_iota(jnp.int32, (16, tok), 0)
    slot_iota = lax.broadcasted_iota(jnp.int32, (slots, tok), 0)
    most = jnp.zeros((16, 1), F32)
    load = jnp.zeros((tok, 1), F32)
    for g in range(GROUPS):
        c = [ch_ref[g, j:j + 1, :] for j in range(2)]
        hot = [jnp.where(ids == c[j], 1.0, 0.0) for j in range(2)]
        earlier = jnp.dot((hot[0] + hot[1]).astype(BF16), upper, preferred_element_type=F32)
        pos = [jnp.sum(earlier * hot[j], axis=0, keepdims=True).astype(jnp.int32) for j in range(2)]
        kept = [pos[j] < CAP for j in range(2)]
        keptf = [jnp.where(kept[j], 1.0, 0.0) for j in range(2)]
        owner = [c[j] // 32 for j in range(2)]
        mine = [jnp.where(lane16 == owner[j], keptf[j], 0.0) for j in range(2)]
        every = [jnp.where(lane16 == GROUPS, keptf[j], 0.0) for j in range(2)]
        some = jnp.maximum(keptf[0], keptf[1])
        tally = mine[0] + mine[1] + every[0] + every[1] + jnp.where(lane16 == GROUPS + 1, some, 0.0)
        before = jnp.dot(tally.astype(BF16), upper, preferred_element_type=F32)
        load = load + jnp.sum(hot[0] + hot[1], axis=1, keepdims=True)
        most = jnp.maximum(most, jnp.sum(tally, axis=1, keepdims=True))
        rank = [jnp.sum(before * mine[j], axis=0, keepdims=True) for j in range(2)]
        rank[1] = rank[1] + jnp.where(owner[0] == owner[1], keptf[0], 0.0)
        nrank = [before[GROUPS:GROUPS + 1, :], before[GROUPS:GROUPS + 1, :] + keptf[0]]
        for j in range(2):
            slot = jnp.where(kept[j] & (owner[j] == ep), (c[j] - ep * 32) * 16 + g * CAP + pos[j], -1)
            tab_ref[g, j:j + 1, :] = slot
            tab_ref[g, 2 + j:3 + j, :] = jnp.where(kept[j], owner[j] * 128 + rank[j].astype(jnp.int32), -1)
            tab_ref[g, 4 + j:5 + j, :] = jnp.where(kept[j], nrank[j].astype(jnp.int32), -1)
        tab_ref[g, 6:7, :] = jnp.where(some > 0.0, before[GROUPS + 1:GROUPS + 2, :].astype(jnp.int32), -1)
        tab_ref[g, 7:8, :] = jnp.zeros((1, tok), jnp.int32)
        pick_ref[:, g * tok:(g + 1) * tok] = jnp.where((slot_iota == tab_ref[g, 0:1, :]) | (slot_iota == tab_ref[g, 1:2, :]), 1.0, 0.0).astype(BF16)
    sub16 = lax.broadcasted_iota(jnp.int32, (16, 1), 0)
    fits = [jnp.where(sub16 < GROUPS, rows_c, jnp.where(sub16 == GROUPS, rows_n, jnp.where(sub16 == GROUPS + 1, rows_t, 0))).astype(F32) for rows_c, rows_n, rows_t in TIERS[:-1]]
    level = jnp.zeros((1, 1), F32)
    for f in fits:
        level = level + jnp.max(jnp.where(most > f, 1.0, 0.0), axis=0, keepdims=True)
    diag = ids == lax.broadcasted_iota(jnp.int32, (tok, tok), 1)
    act_ref[...] = jnp.sum(jnp.where(diag, load, 0.0), axis=0, keepdims=True).astype(jnp.int32)
    flag_ref[0] = jnp.max(level).astype(jnp.int32)

    wr_copy.wait()

    def late_copies(j):
        out = []
        for h in range(2):
            cols = pl.ds(pl.multiple_of(h * half + j * cw, cw), cw)
            out.append(pltpu.make_async_copy(stage_ref.at[j, h], late_hbm.at[:, cols], l_sem.at[j, h]))
        return out

    def main(i, carry):
        @pl.when(i < steps)
        def _():
            x_copy(i).wait_recv()
            y_copy(i).start()
            dx_copy(i).start()

        @pl.when(i + AHEAD < steps)
        def _():
            first_sends(i + AHEAD, 0)

        @pl.when((i >= UP_LAG) & (i < steps + UP_LAG))
        def _():
            j = i - UP_LAG
            y_copy(j).wait_recv()
            dy_copy(j).start()

        @pl.when(i >= UP_LAG + 1)
        def _():
            j = i - UP_LAG - 1
            slot = lax.rem(j, UP_BUFS)
            for h in range(2):
                kr = pl.ds(pl.multiple_of(h * half + j * cw, cw), cw)
                logit_ref[...] += jnp.dot(u_ref[j, h, ep], wr_ref[kr, :], preferred_element_type=F32)
            @pl.when(j == 0)
            def _():
                own_copy.wait_recv()
            dx_copy(j).wait_recv()
            dy_copy(j).wait_recv()
            for h in range(2):
                block = u_ref[j, h].reshape(GROUPS * tok, cw)
                rows_u = jnp.dot(pick_ref[...], block, preferred_element_type=F32).astype(BF16)
                xs_ref[:, h * cw:(h + 1) * cw] = rows_u[0:EARLY * 16]
                stage_ref[j, h] = rows_u[EARLY * 16:]
            for c in weight_copies(j, slot):
                c.wait()
            for c in late_copies(j):
                c.start()

            def experts(t, carry2):
                for z in range(4):
                    e = t * 4 + z
                    rows = pl.ds(pl.multiple_of(e * 16, 16), 16)
                    acc_ref[rows, :] += jnp.dot(xs_ref[rows, :], wbuf[slot, e], preferred_element_type=F32)
                return carry2

            lax.fori_loop(0, EARLY // 4, experts, 0)

            @pl.when(j + UP_BUFS < steps)
            def _():
                for c in weight_copies(j + UP_BUFS, slot):
                    c.start()
        return carry

    lax.fori_loop(0, steps + UP_LAG + 1, main, 0)

    gate_act = acc_ref[:, :128]
    hid_ref[...] = (gate_act * jax.nn.sigmoid(gate_act) * acc_ref[:, 128:]).astype(BF16)
    logits = logit_ref[...]
    ex = jnp.exp(logits - jnp.max(logits, axis=-1, keepdims=True))
    probs = ex / jnp.sum(ex, axis=-1, keepdims=True)
    lanes = lax.broadcasted_iota(jnp.int32, probs.shape, 1)
    picked = [jnp.sum(jnp.where(column(ch_ref[ep, j:j + 1, :]) == lanes, probs, 0.0), axis=-1, keepdims=True) for j in range(2)]
    for j in range(2):
        gate_ref[:, j:j + 1] = picked[j] / (picked[0] + picked[1])

    def last_waits(j, carry):
        for c in late_copies(j):
            c.wait()
        x_copy(j).wait_send()
        y_copy(j).wait_send()
        dx_copy(j).wait_send()
        dy_copy(j).wait_send()
        return carry

    lax.fori_loop(0, steps, last_waits, 0)
    own_copy.wait_send()
    for n in range(3):
        choice_copy(n).wait_send()


def late_kernel(act_ref, late_hbm, wg_hbm, wu_hbm, hid_ref, list_ref, late_ref, wbuf, w_sem, l_sem):
    ep = lax.axis_index('ep')
    local = wg_hbm.shape[0]
    hid_ref[...] = jnp.zeros_like(hid_ref)

    def scan(e, n):
        busy = act_ref[0, ep * local + e] > 0

        @pl.when(busy)
        def _():
            list_ref[n] = e
        return n + busy.astype(jnp.int32)

    count = lax.fori_loop(EARLY, local, scan, 0)

    def weight_copies(n):
        slot = lax.rem(n, LATE_BUFS)
        e = list_ref[n]
        return [pltpu.make_async_copy(w.at[e], wbuf.at[slot, :, m * 128:(m + 1) * 128], w_sem.at[slot, m]) for m, w in enumerate((wg_hbm, wu_hbm))]

    def start(n):
        @pl.when(n < count)
        def _():
            for c in weight_copies(n):
                c.start()

    rows_copy = pltpu.make_async_copy(late_hbm, late_ref, l_sem)
    rows_copy.start()
    for n in range(LATE_BUFS):
        start(n)
    rows_copy.wait()

    def step(n, carry):
        for c in weight_copies(n):
            c.wait()
        rows = pl.ds(pl.multiple_of((list_ref[n] - EARLY) * 16, 16), 16)
        both = jnp.dot(late_ref[rows, :], wbuf[lax.rem(n, LATE_BUFS)], preferred_element_type=F32)
        gate_act = both[:, :128]
        hid_ref[rows, :] = (gate_act * jax.nn.sigmoid(gate_act) * both[:, 128:]).astype(BF16)
        start(n + LATE_BUFS)
        return carry

    lax.fori_loop(0, count, step, 0)


def down_kernel(rows_c, rows_n, rows_t, early_ref, late_ref, x_ref, gate_ref, tab_ref, wd_hbm, out_ref,
                hid_ref, send_ref, land_ref, fwd_ref, yland_ref, done_ref, theirs_ref, qs_ref, w2buf, p_ref, s_ref, a_ref, b_ref, t_ref, e_ref,
                w_sem, q_s, q_r, f_s, f_r, o_s, o_r):
    dp, tp, ep, cx, core = place()
    local = wd_hbm.shape[0]
    tok, d_model = x_ref.shape
    half = d_model // 2
    steps = DOWN_STEPS
    cw = half // steps
    peers = [(1 - cx) * 2 + core, (1 - cx) * 2 + (1 - core), cx * 2 + (1 - core)]
    other_tp = (dp, 1 - tp, ep)

    barrier = pltpu.get_barrier_semaphore()
    for g in peers:
        pl.semaphore_signal(barrier, inc=1, device_id=(dp, tp, g), device_id_type=MESH)
    pl.semaphore_signal(barrier, inc=1, device_id=other_tp, device_id_type=MESH)

    def weight_copies(step, slot):
        out = []
        for h in range(2):
            cols = pl.ds(pl.multiple_of(h * half + step * cw, 128), cw)
            out.append(pltpu.make_async_copy(wd_hbm.at[:, :, cols], w2buf.at[slot, :, :, h * cw:(h + 1) * cw], w_sem.at[slot, h]))
        return out

    for c in weight_copies(0, 0):
        c.start()

    hid_ref[0:EARLY * 16, :] = early_ref[...]
    hid_ref[EARLY * 16:, :] = late_ref[...]
    all_rows = GROUPS * rows_c
    slots = qs_ref.shape[0]
    gap = 128 - rows_c
    slot_iota = lax.broadcasted_iota(jnp.int32, (slots, tok), 0)
    c_iota = lax.broadcasted_iota(jnp.int32, (rows_c, tok), 0)

    def key_of(r):
        for n in range(1, GROUPS):
            r = r + jnp.where(r >= n * rows_c + (n - 1) * gap, gap, 0)
        return r

    def onehot(rows, values):
        return jnp.where(rows == values, 1.0, 0.0).astype(BF16)

    def times_t(a, b):
        return lax.dot_general(a, b, (((1,), (1,)), ((), ())), preferred_element_type=F32)

    for g in range(GROUPS):
        total = jnp.zeros((rows_c, slots), F32)
        for j in range(2):
            total += times_t(onehot(c_iota + ep * 128, tab_ref[g, 2 + j:3 + j, :]), onehot(slot_iota, tab_ref[g, j:j + 1, :]))
        p_ref[g * rows_c:(g + 1) * rows_c, :] = total.astype(BF16)
    key_iota = key_of(lax.broadcasted_iota(jnp.int32, (all_rows, tok), 0))
    n_iota = lax.broadcasted_iota(jnp.int32, (rows_n, tok), 0)
    my_key = [tab_ref[ep, 2 + j:3 + j, :] for j in range(2)]
    my_n = [tab_ref[ep, 4 + j:5 + j, :] for j in range(2)]
    total = jnp.zeros((rows_n, all_rows), F32)
    for j in range(2):
        total += times_t(onehot(n_iota, my_n[j]), onehot(key_iota, my_key[j]))
    s_ref[...] = total.astype(BF16)

    def split_gates(keys, pos, dst):
        mat = jnp.where(pos[0] == keys, gate_ref[:, 0:1], 0.0) + jnp.where(pos[1] == keys, gate_ref[:, 1:2], 0.0)
        for z in range(3):
            part = mat.astype(BF16)
            dst[z] = part
            mat = mat - part.astype(F32)

    split_gates(key_of(lax.broadcasted_iota(jnp.int32, (tok, all_rows), 1)), [column(v) for v in my_key], a_ref)
    split_gates(lax.broadcasted_iota(jnp.int32, (tok, rows_n), 1), [column(v) for v in my_n], b_ref)
    my_t = tab_ref[ep, 6:7, :]
    t_ref[...] = onehot(lax.broadcasted_iota(jnp.int32, (rows_t, tok), 0), my_t)
    e_ref[...] = onehot(lax.broadcasted_iota(jnp.int32, (tok, rows_t), 1), column(my_t))
    some = column(my_t) >= 0
    for c in weight_copies(1, 1):
        c.start()
    pl.semaphore_wait(barrier, 4)

    def q_copy(k, n):
        return remote(send_ref.at[k, :, peers[n]], land_ref.at[k, :, ep], q_s.at[k, n], q_r.at[k, n], (dp, tp, peers[n]))

    def f_copy(k):
        return remote(fwd_ref.at[k], yland_ref.at[k], f_s.at[k], f_r.at[k], other_tp)

    def o_copy(k):
        return remote(done_ref.at[k], theirs_ref.at[k], o_s.at[k], o_r.at[k], other_tp)

    def main(i, carry):
        @pl.when(i < steps)
        def _():
            slot = lax.rem(i, DOWN_BUFS)
            for c in weight_copies(i, slot):
                c.wait()

            def experts(t, carry2):
                for z in range(4):
                    e = t * 4 + z
                    rows = pl.ds(pl.multiple_of(e * 16, 16), 16)
                    qs_ref[rows, :] = jnp.dot(hid_ref[rows, :], w2buf[slot, e], preferred_element_type=F32).astype(BF16)
                return carry2

            lax.fori_loop(0, local // 4, experts, 0)
            for h in range(2):
                send_ref[i, h] = jnp.dot(p_ref[...], qs_ref[:, h * cw:(h + 1) * cw], preferred_element_type=F32).astype(BF16).reshape(GROUPS, rows_c, cw)
            land_ref[i, :, ep] = send_ref[i, :, ep]

            for n in range(3):
                q_copy(i, n).start()

            @pl.when(i + DOWN_BUFS - 2 < steps)
            def _():
                for c in weight_copies(i + DOWN_BUFS - 2, lax.rem(i + DOWN_BUFS - 2, DOWN_BUFS)):
                    c.start()

        @pl.when((i >= DOWN_LAG) & (i < steps + DOWN_LAG))
        def _():
            k = i - DOWN_LAG
            for n in range(3):
                q_copy(k, n).wait_recv()
            block = land_ref[k, 1 - tp].reshape(GROUPS * rows_c, cw)
            fwd_ref[k] = jnp.dot(s_ref[...], block, preferred_element_type=F32).astype(BF16)
            f_copy(k).start()

        @pl.when((i >= 2 * DOWN_LAG) & (i < steps + 2 * DOWN_LAG))
        def _():
            k = i - 2 * DOWN_LAG
            mine = land_ref[k, tp].reshape(GROUPS * rows_c, cw)
            mix = jnp.dot(a_ref[2], mine, preferred_element_type=F32)
            mix += jnp.dot(a_ref[1], mine, preferred_element_type=F32)
            mix += jnp.dot(a_ref[0], mine, preferred_element_type=F32)
            f_copy(k).wait_recv()
            theirs = yland_ref[k]
            for z in (2, 1, 0):
                mix += jnp.dot(b_ref[z], theirs, preferred_element_type=F32)
            cols = pl.ds(pl.multiple_of(tp * half + k * cw, 128), cw)
            rows = (x_ref[:, cols].astype(F32) + mix).astype(BF16)
            done_ref[k] = jnp.dot(t_ref[...], rows, preferred_element_type=F32).astype(BF16)
            o_copy(k).start()
            out_ref[:, cols] = rows

        @pl.when(i >= 3 * DOWN_LAG)
        def _():
            k = i - 3 * DOWN_LAG
            cols = pl.ds(pl.multiple_of((1 - tp) * half + k * cw, 128), cw)
            o_copy(k).wait_recv()
            rows = jnp.dot(e_ref[...], theirs_ref[k], preferred_element_type=F32)
            out_ref[:, cols] = jnp.where(some, rows, x_ref[:, cols].astype(F32)).astype(BF16)
        return carry

    lax.fori_loop(0, steps + 3 * DOWN_LAG, main, 0)

    def last_waits(k, carry):
        for n in range(3):
            q_copy(k, n).wait_send()
        f_copy(k).wait_send()
        o_copy(k).wait_send()
        return carry

    lax.fori_loop(0, steps, last_waits, 0)


def run_up(x, g, wr, wg, wu, choice_t):
    tok, d_model = x.shape
    local = wg.shape[0]
    cw = d_model // 2 // UP_STEPS
    slots = local * GROUPS * CAP
    vm = pl.BlockSpec(memory_space=pltpu.VMEM)
    hbm = pl.BlockSpec(memory_space=pltpu.HBM)
    sem = pltpu.SemaphoreType.DMA
    return pl.pallas_call(
        up_kernel,
        out_shape=(
            jax.ShapeDtypeStruct((EARLY * 16, 128), BF16),
            jax.ShapeDtypeStruct((slots - EARLY * 16, d_model), BF16),
            jax.ShapeDtypeStruct((tok, 2), F32),
            jax.ShapeDtypeStruct((GROUPS, 8, tok), jnp.int32),
            jax.ShapeDtypeStruct((1, 128), jnp.int32),
            jax.ShapeDtypeStruct((1,), jnp.int32),
        ),
        in_specs=[vm, vm, hbm, hbm, hbm, vm],
        out_specs=(vm, hbm, vm, vm, vm, pl.BlockSpec(memory_space=pltpu.SMEM)),
        scratch_shapes=[
            pltpu.VMEM((UP_STEPS, 2, GROUPS, tok, cw), BF16),
            pltpu.VMEM((EARLY * 16, 2 * cw), BF16),
            pltpu.VMEM((slots, GROUPS * tok), BF16),
            pltpu.VMEM((EARLY * 16, 256), F32),
            pltpu.VMEM((UP_BUFS, EARLY, 2 * cw, 256), BF16),
            pltpu.VMEM((tok, 128), F32),
            pltpu.VMEM((GROUPS, 2, tok), jnp.int32),
            pltpu.VMEM(wr.shape, BF16),
            pltpu.VMEM((UP_STEPS, 2, slots - EARLY * 16, cw), BF16),
            sem((UP_BUFS, 4)), sem, sem((UP_STEPS, 2)), sem((3,)), sem((3,)), sem, sem,
        ] + [sem((UP_STEPS,))] * 8,
        compiler_params=pltpu.CompilerParams(collective_id=0, has_side_effects=True, vmem_limit_bytes=VMEM_LIMIT),
        name='up',
    )(x, g, wr, wg, wu, choice_t)


def run_late(act, late, wg, wu):
    d_model = late.shape[1]
    vm = pl.BlockSpec(memory_space=pltpu.VMEM)
    hbm = pl.BlockSpec(memory_space=pltpu.HBM)
    return pl.pallas_call(
        late_kernel,
        out_shape=jax.ShapeDtypeStruct((late.shape[0], 128), BF16),
        in_specs=[pl.BlockSpec(memory_space=pltpu.SMEM), hbm, hbm, hbm],
        out_specs=vm,
        scratch_shapes=[
            pltpu.SMEM((64,), jnp.int32),
            pltpu.VMEM(late.shape, BF16),
            pltpu.VMEM((LATE_BUFS, d_model, 256), BF16),
            pltpu.SemaphoreType.DMA((LATE_BUFS, 2)),
            pltpu.SemaphoreType.DMA,
        ],
        compiler_params=pltpu.CompilerParams(vmem_limit_bytes=60 * 1024 * 1024),
        name='late',
    )(act, late, wg, wu)


def run_down(tier, early, late, x, gate, tab, wd):
    rows_c, rows_n, rows_t = TIERS[tier]
    tok, d_model = x.shape
    local = wd.shape[0]
    cw = d_model // 2 // DOWN_STEPS
    slots = local * GROUPS * CAP
    vm = pl.BlockSpec(memory_space=pltpu.VMEM)
    hbm = pl.BlockSpec(memory_space=pltpu.HBM)
    sem = pltpu.SemaphoreType.DMA
    return pl.pallas_call(
        functools.partial(down_kernel, rows_c, rows_n, rows_t),
        out_shape=jax.ShapeDtypeStruct(x.shape, BF16),
        in_specs=[vm] * 5 + [hbm],
        out_specs=vm,
        scratch_shapes=[
            pltpu.VMEM((slots, 128), BF16),
            pltpu.VMEM((DOWN_STEPS, 2, GROUPS, rows_c, cw), BF16),
            pltpu.VMEM((DOWN_STEPS, 2, GROUPS, rows_c, cw), BF16),
            pltpu.VMEM((DOWN_STEPS, rows_n, cw), BF16),
            pltpu.VMEM((DOWN_STEPS, rows_n, cw), BF16),
            pltpu.VMEM((DOWN_STEPS, rows_t, cw), BF16),
            pltpu.VMEM((DOWN_STEPS, rows_t, cw), BF16),
            pltpu.VMEM((slots, 2 * cw), BF16),
            pltpu.VMEM((DOWN_BUFS, local, 128, 2 * cw), BF16),
            pltpu.VMEM((GROUPS * rows_c, slots), BF16),
            pltpu.VMEM((rows_n, GROUPS * rows_c), BF16),
            pltpu.VMEM((3, tok, GROUPS * rows_c), BF16),
            pltpu.VMEM((3, tok, rows_n), BF16),
            pltpu.VMEM((rows_t, tok), BF16),
            pltpu.VMEM((tok, rows_t), BF16),
            sem((DOWN_BUFS, 2)), sem((DOWN_STEPS, 3)), sem((DOWN_STEPS, 3)),
            sem((DOWN_STEPS,)), sem((DOWN_STEPS,)), sem((DOWN_STEPS,)), sem((DOWN_STEPS,)),
        ],
        compiler_params=pltpu.CompilerParams(collective_id=1 + tier, has_side_effects=True, vmem_limit_bytes=DOWN_VMEM[tier]),
        name='down%d_%d' % (rows_c, rows_n),
    )(early, late, x, gate, tab, wd)


def solution(mesh):
    row_spec = P(('dp', 'ep'), None)

    def device_step(resid_in, norm_scale, w_router, w_gate, w_up, w_down, choice):
        early, rows_late, gate, tab, act, flag = run_up(resid_in, norm_scale, w_router, w_gate, w_up, choice.T)
        late = run_late(act, rows_late, w_gate, w_up)
        return lax.switch(flag[0], [functools.partial(run_down, t) for t in range(len(TIERS))], early, late, resid_in, gate, tab, w_down)

    return jax.shard_map(device_step, mesh=mesh, in_specs=(row_spec, P(None), P(None, None), P('ep', None, 'tp'), P('ep', None, 'tp'), P('ep', 'tp', None), row_spec), out_specs=row_spec, check_vma=False)
```
